8 devices in a mesh: dp: 8 (over z, y, x, core).
Axes of the slice: x: 2, y: 2, z: 1, core: 2. Of those that a mesh axis runs over, the one named last changes fastest.
Arguments:
- grad_embed: bfloat16 [8, 4096, 3840], P('dp')
- grad_q: bfloat16 [8, 6, 3840, 64], P('dp')
- grad_k: bfloat16 [8, 6, 3840, 32], P('dp')
- grad_v: bfloat16 [8, 6, 3840, 32], P('dp')
- grad_out: bfloat16 [8, 6, 64, 3840], P('dp')
- grad_gate: bfloat16 [8, 6, 3840, 240], P('dp')
- grad_up: bfloat16 [8, 6, 3840, 240], P('dp')
- grad_down: bfloat16 [8, 6, 240, 3840], P('dp')
- grad_norms: bfloat16 [8, 6, 4, 3840], P('dp')
- grad_qk_norms: bfloat16 [8, 6, 2, 256], P('dp')
- first_moment: float32 [36836352], P('dp')
- second_moment: float32 [36836352], P('dp')
- master_param: float32 [36836352], P('dp')
- hyper_params: float32 [5], replicated
Outputs:
- output 1: bfloat16 [4096, 3840], replicated
- output 2: bfloat16 [6, 3840, 64], replicated
- output 3: bfloat16 [6, 3840, 32], replicated
- output 4: bfloat16 [6, 3840, 32], replicated
- output 5: bfloat16 [6, 64, 3840], replicated
- output 6: bfloat16 [6, 3840, 240], replicated
- output 7: bfloat16 [6, 3840, 240], replicated
- output 8: bfloat16 [6, 240, 3840], replicated
- output 9: bfloat16 [6, 4, 3840], replicated
- output 10: bfloat16 [6, 2, 256], replicated
- output 11: float32 [36836352], P('dp')
- output 12: float32 [36836352], P('dp')
- output 13: float32 [36836352], P('dp')
All inputs are finite; a program needn't handle non-finite values.
Results may differ from the reference program's by a relative error of at most 0.001.
Values are sent between devices in bfloat16 or wider.
A program may use at most 1 GiB of HBM per device.

```python
import math
import jax
import jax.numpy as jnp

D_MODEL = 3840
FF_WIDTH = 15360
Q_HEADS = 16
KV_HEADS = 8
HEAD_DIM = 256
VOCAB_SIZE = 262144
TP_RANKS = 64
NUM_LAYERS = 6
DATA_PAR = 8
ADAM_STEP = 7

ADAM_EPS = 1e-8
CLIP_EPS = 1e-6
Q_COLS = Q_HEADS * HEAD_DIM // TP_RANKS
KV_COLS = KV_HEADS * HEAD_DIM // TP_RANKS
FF_COLS = FF_WIDTH // TP_RANKS
VOCAB_ROWS = VOCAB_SIZE // TP_RANKS
PARAM_SHAPES = ((VOCAB_ROWS, D_MODEL), (NUM_LAYERS, D_MODEL, Q_COLS), (NUM_LAYERS, D_MODEL, KV_COLS), (NUM_LAYERS, D_MODEL, KV_COLS), (NUM_LAYERS, Q_COLS, D_MODEL), (NUM_LAYERS, D_MODEL, FF_COLS), (NUM_LAYERS, D_MODEL, FF_COLS), (NUM_LAYERS, FF_COLS, D_MODEL), (NUM_LAYERS, 4, D_MODEL), (NUM_LAYERS, 2, HEAD_DIM))
PARAM_SIZES = tuple(math.prod(tensor_dims) for tensor_dims in PARAM_SHAPES)
PARAMS_TOTAL = sum(PARAM_SIZES)
DECAY_LEN = PARAMS_TOTAL - PARAM_SIZES[8] - PARAM_SIZES[9]
GRAD_NAMES = ("grad_embed", "grad_q", "grad_k", "grad_v", "grad_out", "grad_gate", "grad_up", "grad_down", "grad_norms", "grad_qk_norms")


def setup_inputs(seed: int = 0) -> dict:
    key_list = jax.random.split(jax.random.key(seed), 16)
    grad_scale = math.sqrt(DATA_PAR)
    inputs = {}
    square_sum = jnp.float32(0.0)
    for tensor_index, tensor_dims in enumerate(PARAM_SHAPES):
        noise_draw = jax.random.normal(key_list[tensor_index], (DATA_PAR,) + tensor_dims, jnp.float32)
        grad_arr = (grad_scale * noise_draw).astype(jnp.bfloat16)
        mean_grad = jnp.sum(grad_arr, axis=0, dtype=jnp.float32) / DATA_PAR
        square_sum = square_sum + jnp.sum(mean_grad * mean_grad)
        inputs[GRAD_NAMES[tensor_index]] = grad_arr
    inputs["first_moment"] = 0.1 * jax.random.normal(key_list[10], (PARAMS_TOTAL,), jnp.float32)
    inputs["second_moment"] = 0.015 * jnp.exp(0.5 * jax.random.normal(key_list[11], (PARAMS_TOTAL,), jnp.float32))
    inputs["master_param"] = 0.5 * jax.random.normal(key_list[12], (PARAMS_TOTAL,), jnp.float32)
    hyper_draw = jax.random.uniform(key_list[13], (5,), jnp.float32)
    inputs["hyper_params"] = jnp.stack([0.05 + 0.1 * hyper_draw[0], 0.8 + 0.15 * hyper_draw[1], 0.9 + 0.09 * hyper_draw[2], 0.3 + 1.2 * hyper_draw[3], (0.3 + 0.4 * hyper_draw[4]) * jnp.sqrt(square_sum)])
    return inputs


def reference(grad_embed, grad_q, grad_k, grad_v, grad_out, grad_gate, grad_up, grad_down, grad_norms, grad_qk_norms, first_moment, second_moment, master_param, hyper_params):
    grads = (grad_embed, grad_q, grad_k, grad_v, grad_out, grad_gate, grad_up, grad_down, grad_norms, grad_qk_norms)
    mean_grad = jnp.concatenate([jnp.sum(grad_arr, axis=0, dtype=jnp.float32).reshape(-1) for grad_arr in grads]) / DATA_PAR
    learn_rate = hyper_params[0]
    beta_one = hyper_params[1]
    beta_two = hyper_params[2]
    weight_decay = hyper_params[3]
    grad_norm = jnp.sqrt(jnp.sum(mean_grad * mean_grad))
    clip_scale = jnp.minimum(1.0, hyper_params[4] / (grad_norm + CLIP_EPS))
    clipped = mean_grad * clip_scale
    moment_one = beta_one * first_moment + (1.0 - beta_one) * clipped
    moment_two = beta_two * second_moment + (1.0 - beta_two) * (clipped * clipped)
    m_hat = moment_one / (1.0 - beta_one ** ADAM_STEP)
    v_hat = moment_two / (1.0 - beta_two ** ADAM_STEP)
    keep_decay = jnp.arange(PARAMS_TOTAL) < DECAY_LEN
    direction = m_hat / (jnp.sqrt(v_hat) + ADAM_EPS) + jnp.where(keep_decay, weight_decay * master_param, 0.0)
    new_master = master_param - learn_rate * direction
    new_params = new_master.astype(jnp.bfloat16)
    out_list = []
    start_pos = 0
    for tensor_dims, tensor_size in zip(PARAM_SHAPES, PARAM_SIZES):
        out_list.append(new_params[start_pos:start_pos + tensor_size].reshape(tensor_dims))
        start_pos = start_pos + tensor_size
    return (out_list[0], out_list[1], out_list[2], out_list[3], out_list[4], out_list[5], out_list[6], out_list[7], out_list[8], out_list[9], moment_one, moment_two, new_master)
```

```python
import functools
import math

import jax
import jax.numpy as jnp
import numpy as np
from jax import lax
from jax.experimental import pallas as pl
from jax.experimental.pallas import tpu as pltpu
from jax.sharding import PartitionSpec as P

ADAM_STEP = 7
ADAM_EPS = 1e-8
CLIP_EPS = 1e-6
D = 3840
BLK = D // 128
LAYERS = 6
DEV = 8
TENSORS = (("R", 4096, 1), ("C", 64, LAYERS), ("C", 32, LAYERS), ("C", 32, LAYERS), ("R", 64 * LAYERS, 1),
           ("C", 240, LAYERS), ("C", 240, LAYERS), ("R", 240 * LAYERS, 1))
SIZES = tuple(rows * layers * D for _, rows, layers in TENSORS)
STARTS = tuple(sum(SIZES[:i]) for i in range(len(SIZES)))
DECAY = sum(SIZES)
TAIL = LAYERS * 4 * D + LAYERS * 2 * 256
TOTAL = DECAY + TAIL
SHARE = TOTAL // DEV
SROWS = SHARE // 128
NT = 4536
NR = NT * 8
GUARD = 240
NCH = 9
CR = NR // 2 // NCH
MESH = pl.DeviceIdType.MESH


def plan():
    pieces, units = [], []
    for r in range(DEV):
        lo, hi = r * SHARE, (r + 1) * SHARE
        off, plist, ulist = 0, [], []
        for t, (kind, rows, layers) in enumerate(TENSORS):
            if kind == "R":
                a, b = max(lo, STARTS[t]), min(hi, STARTS[t] + SIZES[t])
                if a >= b:
                    continue
                g0, g1 = (a - STARTS[t]) // (8 * D), -((STARTS[t] - b) // (8 * D))
                plist.append((t, 0, g0, g1, off))
                for g in range(g0, g1):
                    ulist.append(("R", off + (g - g0) * BLK, 1, (STARTS[t] + g * 8 * D - lo) // 128))
                off += (g1 - g0) * BLK
                continue
            for l in range(layers):
                s = STARTS[t] + l * rows * D
                a, b = max(lo, s), min(hi, s + rows * D)
                if a >= b:
                    continue
                j0, j1 = (a - s) // (128 * rows), -((s - b) // (128 * rows))
                plist.append((t, l, j0, j1, off))
                for j in range(j0, j1):
                    ulist.append((rows, off + j - j0, j1 - j0, (s + j * 128 * rows - lo) // 128))
                off += (j1 - j0) * rows // 8
        if hi > DECAY:
            for i in range(TAIL // 1024):
                ulist.append(("T", off + i, 1, (DECAY - lo) // 128 + 8 * i))
            plist.append((len(TENSORS), 0, 0, TAIL // 1024, off))
            off += TAIL // 1024
        assert off <= NT
        pieces.append((plist, off))
        units.append(ulist)
    return pieces, units


PIECES, UNITS = plan()


def flip(dev, bit):
    return dev + bit - 2 * bit * (lax.rem(lax.div(dev, bit), 2))


def barrier_all(me):
    sem = pltpu.get_barrier_semaphore()
    for step in range(1, DEV):
        pl.semaphore_signal(sem, inc=1, device_id=(lax.rem(me + step, DEV),), device_id_type=MESH)
    pl.semaphore_wait(sem, DEV - 1)


def rs_kernel(s_ref, g_ref, sq_ref, r_ref, part, land, loads, outs, accum, sq_all,
              send1, recv1, send2, recv2, load_sem, out_sem, sq_send, sq_recv):
    me = lax.axis_index("dp")
    barrier_all(me)
    half = NR // 2

    def hop(d, q, slot, k):
        first, second = (2, 4) if d == 0 else (4, 2)
        target = flip(me, 1) if slot == 0 else flip(me, first) if slot == 1 else flip(flip(me, first), 1)
        owner = flip(target, second) if q == 0 else target
        return pltpu.make_async_remote_copy(
            src_ref=s_ref.at[pl.ds(owner * NR + d * half + k * CR, CR)],
            dst_ref=r_ref.at[pl.ds(((d * 2 + q) * 3 + slot) * half + k * CR, CR)],
            send_sem=send1.at[d, q, slot, k], recv_sem=recv1.at[d, q, slot, k],
            device_id=(target,), device_id_type=MESH)

    def pass_on(d, k):
        second = 4 if d == 0 else 2
        return pltpu.make_async_remote_copy(
            src_ref=part.at[pl.ds(d * half + k * CR, CR)], dst_ref=land.at[pl.ds(d * half + k * CR, CR)],
            send_sem=send2.at[d, k], recv_sem=recv2.at[d, k],
            device_id=(flip(me, second),), device_id_type=MESH)

    for q in range(2):
        @pl.loop(0, NCH)
        def _(k):
            for slot in (1, 2, 0):
                for d in range(2):
                    hop(d, q, slot, k).start()

    def load(d, q, slot, k, buf):
        second = 4 if d == 0 else 2
        if slot == 3:
            owner = flip(me, second) if q == 0 else me
            src = s_ref.at[pl.ds(owner * NR + d * half + k * CR, CR)]
        else:
            src = r_ref.at[pl.ds(((d * 2 + q) * 3 + slot) * half + k * CR, CR)]
        return pltpu.make_async_copy(src, loads.at[buf, slot], load_sem.at[buf, slot])

    def fetch(d, q, k, buf):
        for slot in range(3):
            hop(d, q, slot, k).wait_recv()
        for slot in range(4):
            load(d, q, slot, k, buf).start()

    def ready(d, q, k, buf):
        for slot in range(4):
            load(d, q, slot, k, buf).wait()

    def total(buf, rows):
        acc = loads[buf, 3, rows, :].astype(jnp.float32)
        for slot in range(3):
            acc = acc + loads[buf, slot, rows, :].astype(jnp.float32)
        return acc

    STEP = 112

    for d in range(2):
        fetch(d, 0, 0, d)

    @pl.loop(0, NCH)
    def _(k):
        for d in range(2):
            ready(d, 0, k, d)

            @pl.loop(0, CR // STEP)
            def _(i):
                rows = pl.ds(i * STEP, STEP)
                part[pl.ds(d * half + k * CR + i * STEP, STEP), :] = total(d, rows)

            @pl.when(k + 1 < NCH)
            def _():
                fetch(d, 0, k + 1, d)

            pass_on(d, k).start()

    accum[...] = jnp.zeros_like(accum)
    skip_rows = me * 0

    def out_copy(d, k):
        return pltpu.make_async_copy(outs.at[d], g_ref.at[pl.ds(d * half + k * CR, CR)], out_sem.at[d])

    for d in range(2):
        fetch(d, 1, 0, d)

    @pl.loop(0, NCH)
    def _(k):
        for d in range(2):
            ready(d, 1, k, d)
            pass_on(d, k).wait_recv()

            @pl.when(k > 0)
            def _():
                out_copy(d, k - 1).wait()

            @pl.loop(0, CR // STEP)
            def _(i):
                base = d * half + k * CR + i * STEP
                g = (total(d, pl.ds(i * STEP, STEP)) + land[pl.ds(base, STEP), :]) * (1.0 / DEV)
                outs[d, pl.ds(i * STEP, STEP), :] = g
                tile = lax.div(base, 8) + lax.broadcasted_iota(jnp.int32, (STEP // 8, 8, 128), 0)
                g3 = g.reshape(STEP // 8, 8, 128)
                accum[...] += jnp.sum(jnp.where(counted(me, tile), g3 * g3, 0.0), axis=0)

            @pl.when(k + 1 < NCH)
            def _():
                fetch(d, 1, k + 1, d)

            out_copy(d, k).start()

    sq_all[pl.ds(me * 8, 8), :] = accum[...]
    for d in range(2):
        out_copy(d, NCH - 1).wait()
    for d in range(2):
        @pl.loop(0, NCH)
        def _(k):
            for q in range(2):
                for slot in range(3):
                    hop(d, q, slot, k).wait_send()
            pass_on(d, k).wait_send()

    def tell(step):
        return pltpu.make_async_remote_copy(
            src_ref=accum, dst_ref=sq_all.at[pl.ds(me * 8, 8)],
            send_sem=sq_send.at[step], recv_sem=sq_recv.at[step],
            device_id=(lax.rem(me + step + 1, DEV),), device_id_type=MESH)

    for step in range(DEV - 1):
        tell(step).start()
    for step in range(DEV - 1):
        tell(step).wait()
    whole = sq_all[pl.ds(0, 8), :]
    for i in range(1, DEV):
        whole = whole + sq_all[pl.ds(8 * i, 8), :]
    sq_ref[...] = jnp.broadcast_to(jnp.sum(whole, keepdims=True), (8, 128))


def shared_first():
    found = []
    for r in range(1, DEV):
        kind, tile, stride, row = UNITS[r][0]
        if row >= 0:
            continue
        found.append((r, BLK, 1) if kind == "R" else (r, stride * kind // 8, stride))
    return found


def counted(me, tile):
    keep = tile >= 0
    for r, tiles, period in shared_first():
        skip = (tile < tiles) & (lax.rem(tile, period) == 0)
        keep = keep & jnp.logical_not(skip & (me == r))
    return keep


def reduce_scatter(send):
    half = NR // 2
    return pl.pallas_call(
        rs_kernel,
        name="reduce_scatter",
        out_shape=(jax.ShapeDtypeStruct((NR, 128), jnp.float32), jax.ShapeDtypeStruct((8, 128), jnp.float32),
                   jax.ShapeDtypeStruct((12 * half, 128), jnp.bfloat16)),
        in_specs=[pl.BlockSpec(memory_space=pl.ANY)],
        out_specs=(pl.BlockSpec(memory_space=pl.ANY), pl.BlockSpec(memory_space=pltpu.VMEM),
                   pl.BlockSpec(memory_space=pl.ANY)),
        scratch_shapes=[
            pltpu.VMEM((NR, 128), jnp.float32), pltpu.VMEM((NR, 128), jnp.float32),
            pltpu.VMEM((2, 4, CR, 128), jnp.bfloat16), pltpu.VMEM((2, CR, 128), jnp.float32),
            pltpu.VMEM((8, 128), jnp.float32), pltpu.VMEM((8 * DEV, 128), jnp.float32),
            pltpu.SemaphoreType.DMA((2, 2, 3, NCH)), pltpu.SemaphoreType.DMA((2, 2, 3, NCH)),
            pltpu.SemaphoreType.DMA((2, NCH)), pltpu.SemaphoreType.DMA((2, NCH)),
            pltpu.SemaphoreType.DMA((2, 4)), pltpu.SemaphoreType.DMA((2,)),
            pltpu.SemaphoreType.DMA((DEV - 1,)), pltpu.SemaphoreType.DMA((DEV - 1,))],
        compiler_params=pltpu.CompilerParams(collective_id=0, has_side_effects=True, vmem_limit_bytes=60 << 20),
    )(send)


BR = 1128
NB = -(-SROWS // BR)
KINDS = ("R", 240, 64, 32, "T")


def unit_tables():
    depth = max(len([u for u in ulist if u[0] == kind]) for ulist in UNITS for kind in KINDS)
    entry = np.zeros((DEV, len(KINDS), 3, depth), np.int32)
    span = np.zeros((DEV, len(KINDS), 2, NB + 1), np.int32)
    for r, ulist in enumerate(UNITS):
        for n, kind in enumerate(KINDS):
            mine = [u for u in ulist if u[0] == kind]
            length = 8 if kind == "T" else 240 if kind == "R" else kind
            for i, u in enumerate(mine):
                entry[r, n, :, i] = (u[1] * 8, u[2] * 8, u[3] + GUARD)
            for b in range(NB):
                span[r, n, 0, b + 1] = sum(u[3] < (b + 1) * BR for u in mine)
                span[r, n, 1, b + 1] = sum(u[3] + length <= (b + 1) * BR for u in mine) if b < NB - 1 else len(mine)
    return entry, span, depth


ENTRY, SPAN, DEPTH = unit_tables()


def lanes(rows):
    return lax.broadcasted_iota(jnp.int32, (rows, 128), 1)


def roll(x, shift):
    shift = shift % 128
    return x if shift == 0 else pltpu.roll(x, shift, 1)


def to_flat(kind, tiles, flat, ta, tb, base, stride, row):
    def tile(i):
        return tiles[pl.ds(pl.multiple_of(base + i * stride, 8), 8), :]

    if kind == "T":
        flat[pl.ds(row, 8), :] = tile(0)
        return
    if kind == "R":
        for c in range(BLK):
            flat[pl.ds(row + c, 8, stride=BLK), :] = tile(c)
        return
    count = kind // 8
    grid = jnp.concatenate([tile(i) for i in range(min(count, 16))], axis=0)
    if count < 16:
        grid = jnp.concatenate([grid, jnp.zeros((128 - kind, 128), jnp.float32)], axis=0)
    ta[...] = grid.T
    if kind == 240:
        grid = jnp.concatenate([tile(i) for i in range(16, 30)] + [jnp.zeros((16, 128), jnp.float32)], axis=0)
        tb[...] = grid.T
        lane = lanes(16)
        for k in range(15):
            r, o = divmod(128 * k, 240)
            if o < 128:
                x = ta[pl.ds(r, 16, stride=8), :]
                if o > 0:
                    x = jnp.where(lane >= o, x, tb[pl.ds(r, 16, stride=8), :])
            else:
                x = tb[pl.ds(r, 16, stride=8), :]
            x = roll(x, -o)
            if o + 128 > 240:
                x = jnp.where(lane >= 240 - o, roll(ta[pl.ds(r + 1, 16, stride=8), :], 240 - o), x)
            flat[pl.ds(row + k, 16, stride=15), :] = x
        return
    per = 128 // kind
    lane = lanes(kind)
    x = ta[pl.ds(0, kind, stride=per), :]
    for q in range(1, per):
        x = jnp.where(lane >= q * kind, roll(ta[pl.ds(q, kind, stride=per), :], q * kind), x)
    flat[pl.ds(row, kind), :] = x


def to_tiles(kind, tiles, flat, ta, tb, base, stride, row):
    def put(i, value):
        tiles[pl.ds(pl.multiple_of(base + i * stride, 8), 8), :] = value

    if kind == "T":
        put(0, flat[pl.ds(row, 8), :])
        return
    if kind == "R":
        for c in range(BLK):
            put(c, flat[pl.ds(row + c, 8, stride=BLK), :])
        return
    if kind == 240:
        lane = lanes(16)
        for r in range(8):
            k, o = divmod(240 * r, 128)
            f = [flat[pl.ds(row + k + i, 16, stride=15), :] for i in range(3 if k + 2 < 15 else 2)]
            first = f[0] if o == 0 else roll(jnp.where(lane >= o, f[0], f[1]), -o)
            second = f[1] if o == 0 else roll(jnp.where(lane >= o, f[1], f[2]) if len(f) > 2 else f[1], -o)
            ta[pl.ds(r, 16, stride=8), :] = first
            tb[pl.ds(r, 16, stride=8), :] = second
        grid = ta[...].T
        for i in range(16):
            put(i, grid[8 * i:8 * i + 8])
        grid = tb[...].T
        for i in range(14):
            put(16 + i, grid[8 * i:8 * i + 8])
        return
    per = 128 // kind
    f = flat[pl.ds(row, kind), :]
    for q in range(per):
        ta[pl.ds(q, kind, stride=per), :] = roll(f, -q * kind)
    grid = ta[...].T
    for i in range(kind // 8):
        put(i, grid[8 * i:8 * i + 8])


def adam_kernel(entry, span, scal, g_ref, sq_ref, m_ref, v_ref, p_ref, m_out, v_out, p_out, a_ref,
                tiles, flat, ta, tb, low, g_sem, a_sem):
    me = lax.axis_index("dp")
    b = pl.program_id(0)
    load = pltpu.make_async_copy(g_ref, tiles, g_sem)

    @pl.when(b == 0)
    def _():
        load.start()
        load.wait()

    def each(which, work):
        for n, kind in enumerate(KINDS):
            at = (n * 3) * DEPTH

            def body(u, carry, kind=kind, at=at):
                work(kind, tiles, flat, ta, tb, entry[me, at + u],
                     entry[me, at + DEPTH + u], entry[me, at + 2 * DEPTH + u])
                return carry

            first = (n * 2 + which) * (NB + 1) + b
            lax.fori_loop(span[me, first], span[me, first + 1], body, 0)

    each(0, to_flat)

    learn_rate, b1, c1, b2, c2, i1, i2, decay, max_norm = [scal[i] for i in range(9)]
    norm = jnp.sqrt(sq_ref[...])
    clip = jnp.minimum(1.0, max_norm / (norm + CLIP_EPS))[0:1, :]
    STEP = 24

    @pl.loop(0, BR // STEP)
    def _(i):
        rows = pl.ds(i * STEP, STEP)
        local = b * BR + i * STEP
        here = pl.ds(pl.multiple_of(GUARD + local, 8), STEP)
        h = flat[here, :] * clip
        m = b1 * m_ref[rows, :] + c1 * h
        v = b2 * v_ref[rows, :] + c2 * (h * h)
        p = p_ref[rows, :]
        m_out[rows, :] = m
        v_out[rows, :] = v
        where = me * SROWS + local + lax.broadcasted_iota(jnp.int32, (STEP, 128), 0)
        step = (m * i1) / (jnp.sqrt(v * i2) + ADAM_EPS) + jnp.where(where < DECAY // 128, decay * p, 0.0)
        p = p - learn_rate * step
        p_out[rows, :] = p
        flat[here, :] = p

    each(1, to_tiles)

    @pl.when(b == NB - 1)
    def _():
        @pl.loop(0, NR // 96)
        def _(i):
            rows = pl.ds(pl.multiple_of(i * 96, 96), 96)
            low[rows, :] = tiles[rows, :].astype(jnp.bfloat16)

        put = pltpu.make_async_copy(low, a_ref.at[pl.ds(pl.multiple_of(me * NR, 16), NR)], a_sem)
        put.start()
        put.wait()


def adam(scal, g, sq, m, v, p):
    block = pl.BlockSpec((BR, 128), lambda b, *_: (b, 0))
    anywhere = pl.BlockSpec(memory_space=pl.ANY)
    flat_shape = jax.ShapeDtypeStruct((SROWS, 128), jnp.float32)
    return pl.pallas_call(
        adam_kernel,
        name="adam",
        grid_spec=pltpu.PrefetchScalarGridSpec(
            num_scalar_prefetch=3, grid=(NB,),
            in_specs=[anywhere, pl.BlockSpec((8, 128), lambda b, *_: (0, 0)), block, block, block],
            out_specs=[block, block, block, anywhere],
            scratch_shapes=[
                pltpu.VMEM((NR, 128), jnp.float32), pltpu.VMEM((NB * BR + 2 * GUARD + 8, 128), jnp.float32),
                pltpu.VMEM((128, 128), jnp.float32), pltpu.VMEM((128, 128), jnp.float32),
                pltpu.VMEM((NR, 128), jnp.bfloat16), pltpu.SemaphoreType.DMA, pltpu.SemaphoreType.DMA]),
        out_shape=[flat_shape, flat_shape, flat_shape, jax.ShapeDtypeStruct((DEV * NR, 128), jnp.bfloat16)],
        compiler_params=pltpu.CompilerParams(dimension_semantics=("arbitrary",), vmem_limit_bytes=63 << 20),
    )(jnp.asarray(ENTRY.reshape(DEV, -1)), jnp.asarray(SPAN.reshape(DEV, -1)), scal, g, sq, m, v, p)


def ag_kernel(a_in, a_ref, send, recv):
    del a_in
    me = lax.axis_index("dp")
    barrier_all(me)
    half = NR // 2
    xn, yn, pn = flip(me, 2), flip(me, 4), flip(me, 1)
    diag = flip(xn, 4)

    def copy(kind, d, k):
        owner = (me, me, me, xn if d == 0 else yn, xn, yn, diag)[kind]
        target = (xn, yn, pn, yn if d == 0 else xn, pn, pn, pn)[kind]
        part = a_ref.at[pl.ds(owner * NR + d * half + k * CR, CR)]
        return pltpu.make_async_remote_copy(
            src_ref=part, dst_ref=part, send_sem=send.at[kind, d, k], recv_sem=recv.at[kind, d, k],
            device_id=(target,), device_id_type=MESH)

    for turn in range(2):
        @pl.loop(0, NCH)
        def _(k):
            copy(0, turn, k).start()
            copy(1, 1 - turn, k).start()
            copy(2, turn, k).start()

    @pl.loop(0, NCH)
    def _(k):
        copy(0, 0, k).wait_recv()
        copy(3, 0, k).start()
        copy(4, 0, k).start()
        copy(1, 1, k).wait_recv()
        copy(3, 1, k).start()
        copy(5, 1, k).start()

    @pl.loop(0, NCH)
    def _(k):
        copy(0, 1, k).wait_recv()
        copy(4, 1, k).start()
        copy(1, 0, k).wait_recv()
        copy(5, 0, k).start()

    @pl.loop(0, NCH)
    def _(k):
        for d in range(2):
            copy(3, d, k).wait_recv()
            copy(6, d, k).start()

    @pl.loop(0, NCH)
    def _(k):
        for d in range(2):
            for kind in (2, 4, 5, 6):
                copy(kind, d, k).wait_recv()
            for kind in range(7):
                copy(kind, d, k).wait_send()


def all_gather(mine):
    anywhere = pl.BlockSpec(memory_space=pl.ANY)
    return pl.pallas_call(
        ag_kernel,
        name="all_gather",
        out_shape=jax.ShapeDtypeStruct((DEV * NR, 128), jnp.bfloat16),
        in_specs=[anywhere], out_specs=anywhere,
        scratch_shapes=[pltpu.SemaphoreType.DMA((7, 2, NCH)), pltpu.SemaphoreType.DMA((7, 2, NCH))],
        input_output_aliases={0: 0},
        compiler_params=pltpu.CompilerParams(collective_id=1, has_side_effects=True),
    )(mine)


def as_tiles(t, x):
    kind, rows, layers = TENSORS[t]
    if kind == "C":
        x = jnp.swapaxes(x, -1, -2)
    return x.reshape(layers, rows // 8, 8, BLK, 128).transpose(0, 1, 3, 2, 4)


def from_tiles(t, x, shape):
    kind, rows, layers = TENSORS[t]
    x = x.transpose(0, 1, 3, 2, 4)
    if kind == "C":
        return jnp.swapaxes(x.reshape(layers, rows, D), -1, -2)
    return x.reshape(shape)


def pack(views, tail):
    parts = []
    for plist, used in PIECES:
        for t, l, first, last, _ in plist:
            if t == len(TENSORS):
                piece = tail
            elif TENSORS[t][0] == "R":
                piece = views[t][0, first:last]
            else:
                piece = views[t][l, :, first:last]
            parts.append(piece.reshape(-1, 128))
        if used < NT:
            parts.append(jnp.zeros(((NT - used) * 8, 128), jnp.bfloat16))
    return jnp.concatenate(parts, axis=0)


def join(left, right, start, row_step, col_step, tile_step, lane_step, bound):
    pos = start
    for axis, step in enumerate((row_step, col_step, tile_step, lane_step)):
        pos = pos + step * lax.broadcasted_iota(jnp.int32, left.shape, axis)
    return jnp.where(pos < bound, left, right)


def unpack(gathered, shapes):
    outs = []
    for t, (kind, rows, layers) in enumerate(TENSORS):
        per_layer = {}
        for r, (plist, _) in enumerate(PIECES):
            for pt, l, first, last, off in plist:
                if pt == t:
                    per_layer.setdefault(l, []).append((r, first, last, off))
        done = []
        for l in sorted(per_layer):
            axis = 0 if kind == "R" else 1
            parts = []
            for r, first, last, off in per_layer[l]:
                tiles = (last - first) * (BLK if kind == "R" else rows // 8)
                base = (r * NT + off) * 8
                shape = (last - first, BLK, 8, 128) if kind == "R" else (rows // 8, last - first, 8, 128)
                piece = gathered[base:base + tiles * 8].reshape(shape)
                if parts and first < parts[-1][2]:
                    start = STARTS[t] + (first * 8 * D if kind == "R" else l * rows * D + first * 128 * rows)
                    steps = (0, 128, D, 1) if kind == "R" else (8, 0, 1, rows)
                    prev = parts.pop()
                    size = prev[0].shape[axis]
                    left = lax.slice_in_dim(prev[0], size - 1, size, axis=axis)
                    right = lax.slice_in_dim(piece, 0, 1, axis=axis)
                    if size > 1:
                        parts.append((lax.slice_in_dim(prev[0], 0, size - 1, axis=axis), 0, 0))
                    parts.append((join(left, right, start, *steps, r * SHARE), 0, 0))
                    piece = lax.slice_in_dim(piece, 1, last - first, axis=axis)
                parts.append((piece, first, last))
            done.append(jnp.concatenate([p[0] for p in parts], axis=axis))
        whole = jnp.stack(done)
        if kind == "R":
            whole = whole.reshape(1, rows // 8, BLK, 8, 128)
        outs.append(from_tiles(t, whole, shapes[t]))
    plist, _ = PIECES[DEV - 1]
    off = plist[-1][4]
    tail = gathered[((DEV - 1) * NT + off) * 8:((DEV - 1) * NT + off) * 8 + TAIL // 128].reshape(-1)
    cut = math.prod(shapes[8])
    return outs + [tail[:cut].reshape(shapes[8]), tail[cut:].reshape(shapes[9])]


def solution(mesh):
    def local_update(*arrays):
        grads = arrays[:10]
        m, v, p, hyper = arrays[10:]
        shapes = [x.shape[1:] for x in grads]
        views = [as_tiles(t, grads[t][0]) for t in range(8)]
        tail = jnp.concatenate([grads[8].reshape(-1), grads[9].reshape(-1)])
        share, squares, _ = reduce_scatter(pack(views, tail))
        learn_rate, b1, b2, decay, max_norm = [hyper[i] for i in range(5)]
        scal = jnp.stack([learn_rate, b1, 1.0 - b1, b2, 1.0 - b2, 1.0 / (1.0 - b1 ** ADAM_STEP),
                          1.0 / (1.0 - b2 ** ADAM_STEP), decay, max_norm])
        m, v, p, mine = adam(scal, share, squares, *[x.reshape(SROWS, 128) for x in (m, v, p)])
        params = unpack(all_gather(mine), shapes)
        return tuple(params) + tuple(x.reshape(SHARE) for x in (m, v, p))

    in_specs = tuple([P("dp")] * 10 + [P("dp"), P("dp"), P("dp"), P()])
    out_specs = tuple([P()] * 10 + [P("dp"), P("dp"), P("dp")])
    return jax.shard_map(local_update, mesh=mesh, in_specs=in_specs, out_specs=out_specs, check_vma=False)
```

```python
import functools
import math

import jax
import jax.numpy as jnp
import numpy as np
from jax import lax
from jax.experimental import pallas as pl
from jax.experimental.pallas import tpu as pltpu
from jax.sharding import PartitionSpec as P

ADAM_STEP = 7
ADAM_EPS = 1e-8
CLIP_EPS = 1e-6
D = 3840
BLK = D // 128
LAYERS = 6
DEV = 8
TENSORS = (("R", 4096, 1), ("C", 64, LAYERS), ("C", 32, LAYERS), ("C", 32, LAYERS), ("R", 64 * LAYERS, 1),
           ("C", 240, LAYERS), ("C", 240, LAYERS), ("R", 240 * LAYERS, 1))
SIZES = tuple(rows * layers * D for _, rows, layers in TENSORS)
STARTS = tuple(sum(SIZES[:i]) for i in range(len(SIZES)))
DECAY = sum(SIZES)
TAIL = LAYERS * 4 * D + LAYERS * 2 * 256
TOTAL = DECAY + TAIL
SHARE = TOTAL // DEV
SROWS = SHARE // 128
NT = 4536
NR = NT * 8
GUARD = 240
NCH = 9
CR = NR // 2 // NCH
MESH = pl.DeviceIdType.MESH


def plan():
    pieces, units = [], []
    for r in range(DEV):
        lo, hi = r * SHARE, (r + 1) * SHARE
        off, plist, ulist = 0, [], []
        for t, (kind, rows, layers) in enumerate(TENSORS):
            if kind == "R":
                a, b = max(lo, STARTS[t]), min(hi, STARTS[t] + SIZES[t])
                if a >= b:
                    continue
                g0, g1 = (a - STARTS[t]) // (8 * D), -((STARTS[t] - b) // (8 * D))
                plist.append((t, 0, g0, g1, off))
                for g in range(g0, g1):
                    ulist.append(("R", off + (g - g0) * BLK, 1, (STARTS[t] + g * 8 * D - lo) // 128))
                off += (g1 - g0) * BLK
                continue
            for l in range(layers):
                s = STARTS[t] + l * rows * D
                a, b = max(lo, s), min(hi, s + rows * D)
                if a >= b:
                    continue
                j0, j1 = (a - s) // (128 * rows), -((s - b) // (128 * rows))
                plist.append((t, l, j0, j1, off))
                whole = j1 - j0 == BLK
                for j in range(j0, j1):
                    at, stride = (j, BLK) if whole else ((j - j0) * (rows // 8), 1)
                    ulist.append((rows, off + at, stride, (s + j * 128 * rows - lo) // 128))
                off += (j1 - j0) * rows // 8
        if hi > DECAY:
            for i in range(TAIL // 1024):
                ulist.append(("T", off + i, 1, (DECAY - lo) // 128 + 8 * i))
            plist.append((len(TENSORS), 0, 0, TAIL // 1024, off))
            off += TAIL // 1024
        assert off <= NT
        pieces.append((plist, off))
        units.append(ulist)
    return pieces, units


PIECES, UNITS = plan()


def flip(dev, bit):
    return dev + bit - 2 * bit * (lax.rem(lax.div(dev, bit), 2))


def barrier_all(me):
    sem = pltpu.get_barrier_semaphore()
    for step in range(1, DEV):
        pl.semaphore_signal(sem, inc=1, device_id=(lax.rem(me + step, DEV),), device_id_type=MESH)
    pl.semaphore_wait(sem, DEV - 1)


def cut_layers():
    return sorted({(t, l) for plist, _ in PIECES for t, l, a, b, _ in plist
                   if t < len(TENSORS) and TENSORS[t][0] == "C" and b - a < BLK})


CUT = cut_layers()


def segments():
    found = []
    for plist, used in PIECES:
        runs = []
        for t, l, first, last, off in plist:
            if t == len(TENSORS):
                src, row, rows = t, 0, -(-last // 2) * 16
            elif TENSORS[t][0] == "R":
                src, row, rows = t, first * BLK * 8, (last - first) * BLK * 8
            elif (t, l) in CUT:
                c = TENSORS[t][1]
                src, row, rows = len(TENSORS) + 1 + CUT.index((t, l)), first * c, (last - first) * c
            else:
                src, row, rows = t, l * BLK * TENSORS[t][1], BLK * TENSORS[t][1]
            if runs and runs[-1][0] == src and runs[-1][1] + runs[-1][3] == row:
                runs[-1][3] += rows
            else:
                runs.append([src, row, off * 8, rows])
        end = runs[-1][2] + runs[-1][3]
        if end < NR:
            runs.append([0, 0, end, NR - end])
        halves = ([], [])
        for src, row, dst, rows in runs:
            while rows > 0:
                n = min(rows, CR - dst % CR)
                d, k = divmod(dst // CR, NCH)
                last = halves[d][-1] if halves[d] else None
                if last and n == CR and last[0] == src and last[4] == CR and last[1] + last[5] * CR == row:
                    last[5] += 1
                else:
                    halves[d].append([src, row, k, dst - d * (NR // 2), n, 1])
                row, dst, rows = row + n, dst + n, rows - n
        found.append(halves)
    return found


def rs_kernel(*refs):
    count = len(TENSORS) + 1 + len(CUT)
    srcs, (g_ref, sq_ref, r_ref, part, land, loads, outs, accum, sq_all,
           send1, recv1, send2, recv2, load_sem, out_sem, sq_send, sq_recv) = refs[:count], refs[count:]
    me = lax.axis_index("dp")
    barrier_all(me)
    half = NR // 2
    segs = segments()

    def bits(d):
        return 2 + 2 * d, 4 - 2 * d

    def landing(d, q, slot, row, rows):
        return r_ref.at[pl.ds(pl.multiple_of(((d * 2 + q) * 3 + slot) * half + row, 16), rows)]

    def hop(d, q, slot, k):
        here = landing(d, q, slot, k * CR, CR)
        return pltpu.make_async_remote_copy(
            src_ref=here, dst_ref=here, send_sem=send1.at[d, q, slot, k], recv_sem=recv1.at[d, q, slot, k],
            device_id=(flip(me, 1),), device_id_type=MESH)

    def pass_on(d, k):
        rows = pl.ds(pl.multiple_of(d * half + k * CR, 16), CR)
        return pltpu.make_async_remote_copy(
            src_ref=part.at[rows], dst_ref=land.at[rows], send_sem=send2.at[d, k], recv_sem=recv2.at[d, k],
            device_id=(flip(me, bits(d)[1]),), device_id_type=MESH)

    @pl.loop(0, 12)
    def _(h):
        q, turn, d = lax.div(h, 6), lax.rem(lax.div(h, 2), 3), lax.rem(h, 2)
        slot = lax.rem(turn + 1, 3)
        first, second = bits(d)
        away = flip(me, first)
        target = jnp.where(slot == 0, flip(me, 1), jnp.where(slot == 1, away, flip(away, 1)))
        owner = jnp.where(q == 0, flip(target, second), target)
        for r in range(DEV):
            for dd in range(2):
                @pl.when((owner == r) & (d == dd))
                def _():
                    for src, row, k0, dst, rows, chunks in segs[r][dd]:
                        def send(i, carry, src=src, row=row, k0=k0, dst=dst, rows=rows):
                            pltpu.make_async_remote_copy(
                                src_ref=srcs[src].at[pl.ds(pl.multiple_of(row + i * CR, 8), rows)],
                                dst_ref=r_ref.at[pl.ds(pl.multiple_of(
                                    ((d * 2 + q) * 3 + slot) * half + dst + i * CR, 8), rows)],
                                send_sem=send1.at[d, q, slot, k0 + i], recv_sem=recv1.at[d, q, slot, k0 + i],
                                device_id=(target,), device_id_type=MESH).start()
                            return carry
                        if chunks == 1:
                            send(0, 0)
                        else:
                            lax.fori_loop(0, chunks, send, 0)

    def load(d, q, slot, k):
        return pltpu.make_async_copy(landing(d, q, slot % 3, k * CR, CR), loads.at[d, slot], load_sem.at[d, slot])

    def load_own(d, q, k):
        owner = flip(me, bits(d)[1]) if q == 0 else me
        for r in range(DEV):
            @pl.when(owner == r)
            def _(r=r):
                for src, row, k0, dst, rows, chunks in segs[r][d]:
                    inside = (k >= k0) & (k < k0 + chunks)
                    at = row if chunks == 1 else pl.multiple_of(row + jnp.where(inside, k - k0, 0) * CR, 8)

                    @pl.when(inside)
                    def _(src=src, at=at, dst=dst, rows=rows):
                        pltpu.make_async_copy(
                            srcs[src].at[pl.ds(at, rows)],
                            loads.at[d, 3, pl.ds(dst % CR, rows)], load_sem.at[d, 3]).start()

    def fetch(d, q, k):
        load_own(d, q, k)
        for slot in range(3):
            hop(d, q, slot, k).wait_recv()
            load(d, q, slot, k).start()

    def ready(d, q, k):
        for slot in range(4):
            load(d, q, slot, k).wait()

    def total(d, rows):
        acc = loads[d, 3, rows, :].astype(jnp.float32)
        for slot in range(3):
            acc = acc + loads[d, slot, rows, :].astype(jnp.float32)
        return acc

    STEP = 112
    accum[...] = jnp.zeros_like(accum)
    used = functools.reduce(lambda acc, r: jnp.where(me == r, PIECES[r][1], acc), range(DEV), 0)

    def out_copy(d, k):
        return pltpu.make_async_copy(
            outs.at[d], g_ref.at[pl.ds(pl.multiple_of(d * half + k * CR, 16), CR)], out_sem.at[d])

    for d in range(2):
        fetch(d, 0, jnp.int32(0))

    @pl.loop(0, NCH)
    def _(k):
        for d in range(2):
            ready(d, 0, k)

            @pl.loop(0, CR // STEP)
            def _(i):
                rows = pl.ds(pl.multiple_of(i * STEP, 16), STEP)
                part[pl.ds(pl.multiple_of(d * half + k * CR + i * STEP, 8), STEP), :] = total(d, rows)

            @pl.when(k + 1 < NCH)
            def _():
                fetch(d, 0, k + 1)

            pass_on(d, k).start()

    for d in range(2):
        fetch(d, 1, jnp.int32(0))

    @pl.loop(0, NCH)
    def _(k):
        for d in range(2):
            ready(d, 1, k)
            pass_on(d, k).wait_recv()

            @pl.when(k > 0)
            def _():
                out_copy(d, k - 1).wait()

            @pl.loop(0, CR // STEP)
            def _(i):
                base = pl.multiple_of(d * half + k * CR + i * STEP, 8)
                rows = pl.ds(pl.multiple_of(i * STEP, 16), STEP)
                g = (total(d, rows) + land[pl.ds(base, STEP), :]) * (1.0 / DEV)
                outs[d, rows, :] = g
                tile = lax.div(base, 8) + lax.broadcasted_iota(jnp.int32, (STEP // 8, 8, 128), 0)
                g3 = g.reshape(STEP // 8, 8, 128)
                keep = counted(me, tile) & (tile < used)
                accum[...] += jnp.sum(jnp.where(keep, g3 * g3, 0.0), axis=0)

            @pl.when(k + 1 < NCH)
            def _():
                fetch(d, 1, k + 1)

            out_copy(d, k).start()

    sq_all[pl.ds(pl.multiple_of(me * 8, 8), 8), :] = accum[...]
    for d in range(2):
        out_copy(d, NCH - 1).wait()
    for d in range(2):
        @pl.loop(0, NCH)
        def _(k):
            for q in range(2):
                for slot in range(3):
                    hop(d, q, slot, k).wait_send()
            pass_on(d, k).wait_send()

    def tell(step):
        return pltpu.make_async_remote_copy(
            src_ref=accum, dst_ref=sq_all.at[pl.ds(pl.multiple_of(me * 8, 8), 8)],
            send_sem=sq_send.at[step], recv_sem=sq_recv.at[step],
            device_id=(lax.rem(me + step + 1, DEV),), device_id_type=MESH)

    for step in range(DEV - 1):
        tell(step).start()
    for step in range(DEV - 1):
        tell(step).wait()
    whole = sq_all[pl.ds(0, 8), :]
    for i in range(1, DEV):
        whole = whole + sq_all[pl.ds(8 * i, 8), :]
    sq_ref[...] = jnp.broadcast_to(jnp.sum(whole, keepdims=True), (8, 128))


def shared_first():
    found = []
    for r in range(1, DEV):
        kind, tile, stride, row = UNITS[r][0]
        if row >= 0:
            continue
        found.append((r, BLK if kind == "R" else kind // 8))
    return found


def counted(me, tile):
    first = functools.reduce(lambda acc, x: jnp.where(me == x[0], x[1], acc), shared_first(), 0)
    return tile >= first


def reduce_scatter(sources):
    half = NR // 2
    return pl.pallas_call(
        rs_kernel,
        name="reduce_scatter",
        out_shape=(jax.ShapeDtypeStruct((NR, 128), jnp.float32), jax.ShapeDtypeStruct((8, 128), jnp.float32),
                   jax.ShapeDtypeStruct((12 * half, 128), jnp.bfloat16)),
        in_specs=[pl.BlockSpec(memory_space=pltpu.HBM)] * len(sources),
        out_specs=(pl.BlockSpec(memory_space=pltpu.HBM), pl.BlockSpec(memory_space=pltpu.VMEM),
                   pl.BlockSpec(memory_space=pltpu.HBM)),
        scratch_shapes=[
            pltpu.VMEM((NR, 128), jnp.float32), pltpu.VMEM((NR, 128), jnp.float32),
            pltpu.VMEM((2, 4, CR, 128), jnp.bfloat16), pltpu.VMEM((2, CR, 128), jnp.float32),
            pltpu.VMEM((8, 128), jnp.float32), pltpu.VMEM((8 * DEV, 128), jnp.float32),
            pltpu.SemaphoreType.DMA((2, 2, 3, NCH)), pltpu.SemaphoreType.DMA((2, 2, 3, NCH)),
            pltpu.SemaphoreType.DMA((2, NCH)), pltpu.SemaphoreType.DMA((2, NCH)),
            pltpu.SemaphoreType.DMA((2, 4)), pltpu.SemaphoreType.DMA((2,)),
            pltpu.SemaphoreType.DMA((DEV - 1,)), pltpu.SemaphoreType.DMA((DEV - 1,))],
        compiler_params=pltpu.CompilerParams(collective_id=0, has_side_effects=True, vmem_limit_bytes=60 << 20),
    )(*sources)


BR = 1128
NB = -(-SROWS // BR)
KINDS = ("R", 240, 64, 32, "T")


def unit_tables():
    depth = max(len([u for u in ulist if u[0] == kind]) for ulist in UNITS for kind in KINDS)
    entry = np.zeros((DEV, len(KINDS), 3, depth), np.int32)
    span = np.zeros((DEV, len(KINDS), 2, NB + 1), np.int32)
    for r, ulist in enumerate(UNITS):
        for n, kind in enumerate(KINDS):
            mine = [u for u in ulist if u[0] == kind]
            length = 8 if kind == "T" else 240 if kind == "R" else kind
            for i, u in enumerate(mine):
                entry[r, n, :, i] = (u[1] * 8, u[2] * 8, u[3] + GUARD)
            for b in range(NB):
                span[r, n, 0, b + 1] = sum(u[3] < (b + 1) * BR for u in mine)
                span[r, n, 1, b + 1] = sum(u[3] + length <= (b + 1) * BR for u in mine) if b < NB - 1 else len(mine)
    return entry, span, depth


ENTRY, SPAN, DEPTH = unit_tables()


def lanes(rows):
    return lax.broadcasted_iota(jnp.int32, (rows, 128), 1)


def roll(x, shift):
    shift = shift % 128
    return x if shift == 0 else pltpu.roll(x, shift, 1)


def to_flat(kind, tiles, flat, ta, tb, base, stride, row):
    def tile(i):
        return tiles[pl.ds(pl.multiple_of(base + i * stride, 8), 8), :]

    if kind == "T":
        flat[pl.ds(row, 8), :] = tile(0)
        return
    if kind == "R":
        for c in range(BLK):
            flat[pl.ds(row + c, 8, stride=BLK), :] = tile(c)
        return
    count = kind // 8
    grid = jnp.concatenate([tile(i) for i in range(min(count, 16))], axis=0)
    if count < 16:
        grid = jnp.concatenate([grid, jnp.zeros((128 - kind, 128), jnp.float32)], axis=0)
    ta[...] = grid.T
    if kind == 240:
        grid = jnp.concatenate([tile(i) for i in range(16, 30)] + [jnp.zeros((16, 128), jnp.float32)], axis=0)
        tb[...] = grid.T
        lane = lanes(16)
        for k in range(15):
            r, o = divmod(128 * k, 240)
            if o < 128:
                x = ta[pl.ds(r, 16, stride=8), :]
                if o > 0:
                    x = jnp.where(lane >= o, x, tb[pl.ds(r, 16, stride=8), :])
            else:
                x = tb[pl.ds(r, 16, stride=8), :]
            x = roll(x, -o)
            if o + 128 > 240:
                x = jnp.where(lane >= 240 - o, roll(ta[pl.ds(r + 1, 16, stride=8), :], 240 - o), x)
            flat[pl.ds(row + k, 16, stride=15), :] = x
        return
    per = 128 // kind
    lane = lanes(kind)
    x = ta[pl.ds(0, kind, stride=per), :]
    for q in range(1, per):
        x = jnp.where(lane >= q * kind, roll(ta[pl.ds(q, kind, stride=per), :], q * kind), x)
    flat[pl.ds(row, kind), :] = x


def to_tiles(kind, tiles, flat, ta, tb, base, stride, row):
    def put(i, value):
        tiles[pl.ds(pl.multiple_of(base + i * stride, 8), 8), :] = value

    if kind == "T":
        put(0, flat[pl.ds(row, 8), :])
        return
    if kind == "R":
        for c in range(BLK):
            put(c, flat[pl.ds(row + c, 8, stride=BLK), :])
        return
    if kind == 240:
        lane = lanes(16)
        for r in range(8):
            k, o = divmod(240 * r, 128)
            f = [flat[pl.ds(row + k + i, 16, stride=15), :] for i in range(3 if k + 2 < 15 else 2)]
            first = f[0] if o == 0 else roll(jnp.where(lane >= o, f[0], f[1]), -o)
            second = f[1] if o == 0 else roll(jnp.where(lane >= o, f[1], f[2]) if len(f) > 2 else f[1], -o)
            ta[pl.ds(r, 16, stride=8), :] = first
            tb[pl.ds(r, 16, stride=8), :] = second
        grid = ta[...].T
        for i in range(16):
            put(i, grid[8 * i:8 * i + 8])
        grid = tb[...].T
        for i in range(14):
            put(16 + i, grid[8 * i:8 * i + 8])
        return
    per = 128 // kind
    f = flat[pl.ds(row, kind), :]
    for q in range(per):
        ta[pl.ds(q, kind, stride=per), :] = roll(f, -q * kind)
    grid = ta[...].T
    for i in range(kind // 8):
        put(i, grid[8 * i:8 * i + 8])


def adam_kernel(entry, span, scal, g_ref, sq_ref, m_ref, v_ref, p_ref, m_out, v_out, p_out, a_ref,
                tiles, flat, ta, tb, low, g_sem, a_sem):
    me = lax.axis_index("dp")
    b = pl.program_id(0)
    load = pltpu.make_async_copy(g_ref, tiles, g_sem)

    @pl.when(b == 0)
    def _():
        load.start()
        load.wait()

    def each(which, work):
        for n, kind in enumerate(KINDS):
            at = (n * 3) * DEPTH

            def body(u, carry, kind=kind, at=at):
                work(kind, tiles, flat, ta, tb, entry[me, at + u],
                     entry[me, at + DEPTH + u], entry[me, at + 2 * DEPTH + u])
                return carry

            first = (n * 2 + which) * (NB + 1) + b
            lax.fori_loop(span[me, first], span[me, first + 1], body, 0)

    each(0, to_flat)

    learn_rate, b1, c1, b2, c2, i1, i2, decay, max_norm = [scal[i] for i in range(9)]
    norm = jnp.sqrt(sq_ref[...])
    clip = jnp.minimum(1.0, max_norm / (norm + CLIP_EPS))[0:1, :]
    STEP = 24

    @pl.loop(0, BR // STEP)
    def _(i):
        rows = pl.ds(i * STEP, STEP)
        local = b * BR + i * STEP
        here = pl.ds(pl.multiple_of(GUARD + local, 8), STEP)
        h = flat[here, :] * clip
        m = b1 * m_ref[rows, :] + c1 * h
        v = b2 * v_ref[rows, :] + c2 * (h * h)
        p = p_ref[rows, :]
        m_out[rows, :] = m
        v_out[rows, :] = v
        where = me * SROWS + local + lax.broadcasted_iota(jnp.int32, (STEP, 128), 0)
        step = (m * i1) / (jnp.sqrt(v * i2) + ADAM_EPS) + jnp.where(where < DECAY // 128, decay * p, 0.0)
        p = p - learn_rate * step
        p_out[rows, :] = p
        flat[here, :] = p

    each(1, to_tiles)

    @pl.when(b == NB - 1)
    def _():
        @pl.loop(0, NR // 96)
        def _(i):
            rows = pl.ds(pl.multiple_of(i * 96, 96), 96)
            low[rows, :] = tiles[rows, :].astype(jnp.bfloat16)

        put = pltpu.make_async_copy(low, a_ref.at[pl.ds(pl.multiple_of(me * NR, 16), NR)], a_sem)
        put.start()
        put.wait()


def adam(scal, g, sq, m, v, p):
    block = pl.BlockSpec((BR, 128), lambda b, *_: (b, 0))
    anywhere = pl.BlockSpec(memory_space=pltpu.HBM)
    flat_shape = jax.ShapeDtypeStruct((SROWS, 128), jnp.float32)
    return pl.pallas_call(
        adam_kernel,
        name="adam",
        grid_spec=pltpu.PrefetchScalarGridSpec(
            num_scalar_prefetch=3, grid=(NB,),
            in_specs=[anywhere, pl.BlockSpec((8, 128), lambda b, *_: (0, 0)), block, block, block],
            out_specs=[block, block, block, anywhere],
            scratch_shapes=[
                pltpu.VMEM((NR, 128), jnp.float32), pltpu.VMEM((NB * BR + 2 * GUARD + 8, 128), jnp.float32),
                pltpu.VMEM((128, 128), jnp.float32), pltpu.VMEM((128, 128), jnp.float32),
                pltpu.VMEM((NR, 128), jnp.bfloat16), pltpu.SemaphoreType.DMA, pltpu.SemaphoreType.DMA]),
        out_shape=[flat_shape, flat_shape, flat_shape, jax.ShapeDtypeStruct((DEV * NR, 128), jnp.bfloat16)],
        compiler_params=pltpu.CompilerParams(dimension_semantics=("arbitrary",), vmem_limit_bytes=63 << 20),
    )(jnp.asarray(ENTRY.reshape(DEV, -1)), jnp.asarray(SPAN.reshape(DEV, -1)), scal, g, sq, m, v, p)


def ag_kernel(a_in, a_ref, send, recv):
    del a_in
    me = lax.axis_index("dp")
    barrier_all(me)
    half = NR // 2
    xn, yn, pn = flip(me, 2), flip(me, 4), flip(me, 1)
    diag = flip(xn, 4)

    def copy(kind, d, k):
        owner = (me, me, me, xn if d == 0 else yn, xn, yn, diag)[kind]
        target = (xn, yn, pn, yn if d == 0 else xn, pn, pn, pn)[kind]
        part = a_ref.at[pl.ds(owner * NR + d * half + k * CR, CR)]
        return pltpu.make_async_remote_copy(
            src_ref=part, dst_ref=part, send_sem=send.at[kind, d, k], recv_sem=recv.at[kind, d, k],
            device_id=(target,), device_id_type=MESH)

    for turn in range(2):
        @pl.loop(0, NCH)
        def _(k):
            copy(0, turn, k).start()
            copy(1, 1 - turn, k).start()
            copy(2, turn, k).start()

    @pl.loop(0, NCH)
    def _(k):
        copy(0, 0, k).wait_recv()
        copy(3, 0, k).start()
        copy(4, 0, k).start()
        copy(1, 1, k).wait_recv()
        copy(3, 1, k).start()
        copy(5, 1, k).start()

    @pl.loop(0, NCH)
    def _(k):
        copy(0, 1, k).wait_recv()
        copy(4, 1, k).start()
        copy(1, 0, k).wait_recv()
        copy(5, 0, k).start()

    @pl.loop(0, NCH)
    def _(k):
        for d in range(2):
            copy(3, d, k).wait_recv()
            copy(6, d, k).start()

    @pl.loop(0, NCH)
    def _(k):
        for d in range(2):
            for kind in (2, 4, 5, 6):
                copy(kind, d, k).wait_recv()
            for kind in range(7):
                copy(kind, d, k).wait_send()


def all_gather(mine):
    anywhere = pl.BlockSpec(memory_space=pltpu.HBM)
    return pl.pallas_call(
        ag_kernel,
        name="all_gather",
        out_shape=jax.ShapeDtypeStruct((DEV * NR, 128), jnp.bfloat16),
        in_specs=[anywhere], out_specs=anywhere,
        scratch_shapes=[pltpu.SemaphoreType.DMA((7, 2, NCH)), pltpu.SemaphoreType.DMA((7, 2, NCH))],
        input_output_aliases={0: 0},
        compiler_params=pltpu.CompilerParams(collective_id=1, has_side_effects=True),
    )(mine)


def as_tiles(t, x):
    kind, rows, layers = TENSORS[t]
    if kind == "C":
        x = jnp.swapaxes(x, -1, -2)
    return x.reshape(layers, rows // 8, 8, BLK, 128).transpose(0, 1, 3, 2, 4)


def from_tiles(t, x, shape):
    kind, rows, layers = TENSORS[t]
    x = x.transpose(0, 1, 3, 2, 4)
    if kind == "C":
        return jnp.swapaxes(x.reshape(layers, rows, D), -1, -2)
    return x.reshape(shape)


def unpack_plan():
    copies, shared, cuts = [], [], {}
    for t, (kind, rows, layers) in enumerate(TENSORS):
        last_seen = None
        for r, (plist, _) in enumerate(PIECES):
            for pt, l, first, last, off in plist:
                if pt != t:
                    continue
                src = r * NT + off
                if (t, l) in CUT:
                    cuts.setdefault((t, l), []).append((first, last, src, r * SHARE))
                    continue
                if kind == "C":
                    copies.append([src, t, l * BLK * rows // 8, BLK * rows // 8])
                    continue
                begin = first
                if last_seen and first < last_seen[0]:
                    copies[-1][3] -= BLK
                    shared.append((t, first, last_seen[1] - BLK, src, STARTS[t] + first * 8 * D, r * SHARE))
                    begin = first + 1
                copies.append([src + (begin - first) * BLK, t, begin * BLK, (last - begin) * BLK])
                last_seen = (last, src + (last - first) * BLK)
    pieces = []
    for src, t, dst, tiles in copies:
        while tiles > 0:
            n = min(tiles, UN)
            pieces.append((src, t, dst, n))
            src, dst, tiles = src + n, dst + n, tiles - n
    return pieces, shared, cuts


UN = 480
UBUF = 12


def unpack_kernel(src_ref, *refs):
    outs = refs[:len(TENSORS)]
    ring, left, right, *layers, in_sem, out_sem, pair_sem, cut_sem = refs[len(TENSORS):]
    pieces, shared, cuts = unpack_plan()

    def take(i):
        src, _, _, n = pieces[i]
        return pltpu.make_async_copy(src_ref.at[pl.ds(src, n)], ring.at[i % UBUF, pl.ds(0, n)], in_sem.at[i % UBUF])

    def give(i):
        _, t, dst, n = pieces[i]
        return pltpu.make_async_copy(ring.at[i % UBUF, pl.ds(0, n)], outs[t].at[pl.ds(dst, n)], out_sem.at[i % UBUF])

    def pair(n):
        _, _, a, b, _, _ = shared[n]
        return (pltpu.make_async_copy(src_ref.at[pl.ds(a, BLK)], left.at[n], pair_sem.at[n, 0]),
                pltpu.make_async_copy(src_ref.at[pl.ds(b, BLK)], right.at[n], pair_sem.at[n, 1]))

    def cut_loads(n):
        (t, _), sides = list(cuts.items())[n]
        c8 = TENSORS[t][1] // 8
        made = []
        for side, (first, last, src, _) in enumerate(sides):
            for j in range(first, last):
                over = side == 1 and first < sides[0][1] and j == first
                to = right.at[len(shared) + n, pl.ds(0, c8)] if over else layers[n].at[pl.ds(0, c8), j]
                made.append(pltpu.make_async_copy(
                    src_ref.at[pl.ds(src + (j - first) * c8, c8)], to, cut_sem.at[n, BLK if over else j]))
        return made

    def cut_stores(n):
        (t, l), _ = list(cuts.items())[n]
        c8 = TENSORS[t][1] // 8
        return [pltpu.make_async_copy(layers[n].at[c], outs[t].at[pl.ds((l * c8 + c) * BLK, BLK)], cut_sem.at[n, c])
                for c in range(c8)]

    def spot(start, row_step, lane_step, tile_step, tiles):
        shape = (tiles, 8, 128)
        return (start + tile_step * lax.broadcasted_iota(jnp.int32, shape, 0)
                + row_step * lax.broadcasted_iota(jnp.int32, shape, 1)
                + lane_step * lax.broadcasted_iota(jnp.int32, shape, 2))

    for n in range(len(shared)):
        for c in pair(n):
            c.start()
    for n in range(len(cuts)):
        for c in cut_loads(n):
            c.start()
    depth = UBUF // 2
    for i in range(depth):
        take(i).start()
    for i in range(len(pieces)):
        if i + depth < len(pieces):
            if i + depth >= UBUF:
                give(i + depth - UBUF).wait()
            take(i + depth).start()
        take(i).wait()
        give(i).start()
        if i == depth:
            for n, (t, _, _, _, start, bound) in enumerate(shared):
                for c in pair(n):
                    c.wait()
                keep = spot(start, D, 1, 128, BLK) < bound
                left[n] = jnp.where(keep, left[n].astype(jnp.float32), right[n].astype(jnp.float32)).astype(jnp.bfloat16)
            for n, ((t, l), sides) in enumerate(cuts.items()):
                for c in cut_loads(n):
                    c.wait()
                rows = TENSORS[t][1]
                j, bound = sides[1][0], sides[1][3]
                if j < sides[0][1]:
                    keep = spot(STARTS[t] + (l * D + j * 128) * rows, 1, rows, 8, rows // 8) < bound
                    one = right[len(shared) + n, pl.ds(0, rows // 8)].astype(jnp.float32)
                    here = pl.ds(0, rows // 8)
                    layers[n][here, j] = jnp.where(keep, layers[n][here, j].astype(jnp.float32), one).astype(jnp.bfloat16)
        if i == depth + 2:
            for n, (t, g, _, _, _, _) in enumerate(shared):
                pltpu.make_async_copy(left.at[n], outs[t].at[pl.ds(g * BLK, BLK)], pair_sem.at[n, 0]).start()
            for n in range(len(cuts)):
                for c in cut_stores(n):
                    c.start()
    for i in range(max(0, len(pieces) - UBUF), len(pieces)):
        give(i).wait()
    for n, (t, g, _, _, _, _) in enumerate(shared):
        pltpu.make_async_copy(left.at[n], outs[t].at[pl.ds(g * BLK, BLK)], pair_sem.at[n, 0]).wait()
    for n in range(len(cuts)):
        for c in cut_stores(n):
            c.wait()


def unpack(gathered, shapes):
    pieces, shared, cuts = unpack_plan()
    anywhere = pl.BlockSpec(memory_space=pltpu.HBM)
    tiles = pl.pallas_call(
        unpack_kernel,
        name="unpack",
        out_shape=[jax.ShapeDtypeStruct((size // 1024, 8, 128), jnp.bfloat16) for size in SIZES],
        in_specs=[anywhere], out_specs=[anywhere] * len(TENSORS),
        scratch_shapes=[
            pltpu.VMEM((UBUF, UN, 8, 128), jnp.bfloat16), pltpu.VMEM((len(shared) + 1, BLK, 8, 128), jnp.bfloat16),
            pltpu.VMEM((len(shared) + len(cuts) + 1, BLK, 8, 128), jnp.bfloat16),
            *[pltpu.VMEM((TENSORS[t][1] // 8 + 1, BLK, 8, 128), jnp.bfloat16) for t, _ in cuts],
            pltpu.SemaphoreType.DMA((UBUF,)), pltpu.SemaphoreType.DMA((UBUF,)),
            pltpu.SemaphoreType.DMA((len(shared), 2)), pltpu.SemaphoreType.DMA((len(cuts), BLK + 1))],
        compiler_params=pltpu.CompilerParams(vmem_limit_bytes=48 << 20),
    )(gathered.reshape(DEV * NT, 8, 128))
    outs = [from_tiles(t, x.reshape(TENSORS[t][2], TENSORS[t][1] // 8, BLK, 8, 128), shapes[t])
            for t, x in enumerate(tiles)]
    plist, _ = PIECES[DEV - 1]
    base = ((DEV - 1) * NT + plist[-1][4]) * 8
    tail = gathered[base:base + TAIL // 128].reshape(-1)
    cut = math.prod(shapes[8])
    return outs + [tail[:cut].reshape(shapes[8]), tail[cut:].reshape(shapes[9])]


def sources(grads):
    views = [as_tiles(t, grads[t][0]) for t in range(len(TENSORS))]
    tail = jnp.concatenate([grads[8].reshape(-1), grads[9].reshape(-1), jnp.zeros((-TAIL % 2048,), jnp.bfloat16)])
    turned = [views[t][l].transpose(1, 0, 2, 3) for t, l in CUT]
    return [x.reshape(-1, 128) for x in views + [tail] + turned]


def solution(mesh):
    def local_update(*arrays):
        grads = arrays[:10]
        m, v, p, hyper = arrays[10:]
        shapes = [x.shape[1:] for x in grads]
        share, squares, _ = reduce_scatter(sources(grads))
        learn_rate, b1, b2, decay, max_norm = [hyper[i] for i in range(5)]
        scal = jnp.stack([learn_rate, b1, 1.0 - b1, b2, 1.0 - b2, 1.0 / (1.0 - b1 ** ADAM_STEP),
                          1.0 / (1.0 - b2 ** ADAM_STEP), decay, max_norm])
        m, v, p, mine = adam(scal, share, squares, *[x.reshape(SROWS, 128) for x in (m, v, p)])
        params = unpack(all_gather(mine), shapes)
        return tuple(params) + tuple(x.reshape(SHARE) for x in (m, v, p))

    in_specs = tuple([P("dp")] * 10 + [P("dp"), P("dp"), P("dp"), P()])
    out_specs = tuple([P()] * 10 + [P("dp"), P("dp"), P("dp")])
    return jax.shard_map(local_update, mesh=mesh, in_specs=in_specs, out_specs=out_specs, check_vma=False)
```

```python
import functools
import math

import jax
import jax.numpy as jnp
import numpy as np
from jax import lax
from jax.experimental import pallas as pl
from jax.experimental.pallas import tpu as pltpu
from jax.sharding import PartitionSpec as P

ADAM_STEP = 7
LN = 128
SB = 8
ADAM_EPS = 1e-8
CLIP_EPS = 1e-6
D = 3840
BLK = D // LN
LAYERS = 6
DEV = 8
TENSORS = (("R", 4096, 1), ("C", 64, LAYERS), ("C", 32, LAYERS), ("C", 32, LAYERS), ("R", 64 * LAYERS, 1),
           ("C", 240, LAYERS), ("C", 240, LAYERS), ("R", 240 * LAYERS, 1))
SIZES = tuple(rows * layers * D for _, rows, layers in TENSORS)
STARTS = tuple(sum(SIZES[:i]) for i in range(len(SIZES)))
DECAY = sum(SIZES)
TAIL = LAYERS * 4 * D + LAYERS * 2 * 256
TOTAL = DECAY + TAIL
SHARE = TOTAL // DEV
SROWS = SHARE // LN
NT = 4536
NR = NT * SB
GUARD = 240
NCH = 9
CR = NR // 2 // NCH
MESH = pl.DeviceIdType.MESH


def plan():
    pieces, units = [], []
    for r in range(DEV):
        lo, hi = r * SHARE, (r + 1) * SHARE
        off, plist, ulist = 0, [], []
        for t, (kind, rows, layers) in enumerate(TENSORS):
            if kind == "R":
                a, b = max(lo, STARTS[t]), min(hi, STARTS[t] + SIZES[t])
                if a >= b:
                    continue
                g0, g1 = (a - STARTS[t]) // (SB * D), -((STARTS[t] - b) // (SB * D))
                plist.append((t, 0, g0, g1, off))
                for g in range(g0, g1):
                    ulist.append(("R", off + (g - g0) * BLK, 1, (STARTS[t] + g * SB * D - lo) // LN))
                off += (g1 - g0) * BLK
                continue
            for l in range(layers):
                s = STARTS[t] + l * rows * D
                a, b = max(lo, s), min(hi, s + rows * D)
                if a >= b:
                    continue
                j0, j1 = (a - s) // (LN * rows), -((s - b) // (LN * rows))
                plist.append((t, l, j0, j1, off))
                whole = j1 - j0 == BLK
                for j in range(j0, j1):
                    at, stride = (j, BLK) if whole else ((j - j0) * (rows // SB), 1)
                    ulist.append((rows, off + at, stride, (s + j * LN * rows - lo) // LN))
                off += (j1 - j0) * rows // SB
        if hi > DECAY:
            for i in range(TAIL // 1024):
                ulist.append(("T", off + i, 1, (DECAY - lo) // LN + SB * i))
            plist.append((len(TENSORS), 0, 0, TAIL // 1024, off))
            off += TAIL // 1024
        assert off <= NT
        pieces.append((plist, off))
        units.append(ulist)
    return pieces, units


PIECES, UNITS = plan()


def flip(dev, bit):
    return dev + bit - 2 * bit * (lax.rem(lax.div(dev, bit), 2))


def barrier_all(me):
    sem = pltpu.get_barrier_semaphore()
    for step in range(1, DEV):
        pl.semaphore_signal(sem, inc=1, device_id=(lax.rem(me + step, DEV),), device_id_type=MESH)
    pl.semaphore_wait(sem, DEV - 1)


def cut_layers():
    return sorted({(t, l) for plist, _ in PIECES for t, l, a, b, _ in plist
                   if t < len(TENSORS) and TENSORS[t][0] == "C" and b - a < BLK})


CUT = cut_layers()


def segments():
    found = []
    for plist, used in PIECES:
        runs = []
        for t, l, first, last, off in plist:
            if t == len(TENSORS):
                src, row, rows = t, 0, -(-last // 2) * 16
            elif TENSORS[t][0] == "R":
                src, row, rows = t, first * BLK * SB, (last - first) * BLK * SB
            elif (t, l) in CUT:
                c = TENSORS[t][1]
                src, row, rows = len(TENSORS) + 1 + CUT.index((t, l)), first * c, (last - first) * c
            else:
                src, row, rows = t, l * BLK * TENSORS[t][1], BLK * TENSORS[t][1]
            if runs and runs[-1][0] == src and runs[-1][1] + runs[-1][3] == row:
                runs[-1][3] += rows
            else:
                runs.append([src, row, off * SB, rows])
        end = runs[-1][2] + runs[-1][3]
        if end < NR:
            runs.append([0, 0, end, NR - end])
        halves = ([], [])
        for src, row, dst, rows in runs:
            while rows > 0:
                n = min(rows, CR - dst % CR)
                d, k = divmod(dst // CR, NCH)
                last = halves[d][-1] if halves[d] else None
                if last and n == CR and last[0] == src and last[4] == CR and last[1] + last[5] * CR == row:
                    last[5] += 1
                else:
                    halves[d].append([src, row, k, dst - d * (NR // 2), n, 1])
                row, dst, rows = row + n, dst + n, rows - n
        found.append(halves)
    return found


def rs_kernel(*refs):
    count = len(TENSORS) + 1 + len(CUT)
    srcs, (g_ref, sq_ref, r_ref, part, land, loads, outs, accum, sq_all,
           send1, recv1, send2, recv2, load_sem, out_sem, sq_send, sq_recv) = refs[:count], refs[count:]
    me = lax.axis_index("dp")
    barrier_all(me)
    half = NR // 2
    segs = segments()

    def bits(d):
        return 2 + 2 * d, 4 - 2 * d

    def landing(d, q, slot, row, rows):
        return r_ref.at[pl.ds(pl.multiple_of(((d * 2 + q) * 3 + slot) * half + row, 16), rows)]

    def hop(d, q, slot, k):
        here = landing(d, q, slot, k * CR, CR)
        return pltpu.make_async_remote_copy(
            src_ref=here, dst_ref=here, send_sem=send1.at[d, q, slot, k], recv_sem=recv1.at[d, q, slot, k],
            device_id=(flip(me, 1),), device_id_type=MESH)

    def pass_on(d, k):
        rows = pl.ds(pl.multiple_of(d * half + k * CR, 16), CR)
        return pltpu.make_async_remote_copy(
            src_ref=part.at[rows], dst_ref=land.at[rows], send_sem=send2.at[d, k], recv_sem=recv2.at[d, k],
            device_id=(flip(me, bits(d)[1]),), device_id_type=MESH)

    @pl.loop(0, 12)
    def _(h):
        q, turn, d = lax.div(h, 6), lax.rem(lax.div(h, 2), 3), lax.rem(h, 2)
        slot = lax.rem(turn + 1, 3)
        first, second = bits(d)
        away = flip(me, first)
        target = jnp.where(slot == 0, flip(me, 1), jnp.where(slot == 1, away, flip(away, 1)))
        owner = jnp.where(q == 0, flip(target, second), target)
        for r in range(DEV):
            for dd in range(2):
                @pl.when((owner == r) & (d == dd))
                def _():
                    for src, row, k0, dst, rows, chunks in segs[r][dd]:
                        def send(i, carry, src=src, row=row, k0=k0, dst=dst, rows=rows):
                            pltpu.make_async_remote_copy(
                                src_ref=srcs[src].at[pl.ds(pl.multiple_of(row + i * CR, SB), rows)],
                                dst_ref=r_ref.at[pl.ds(pl.multiple_of(
                                    ((d * 2 + q) * 3 + slot) * half + dst + i * CR, SB), rows)],
                                send_sem=send1.at[d, q, slot, k0 + i], recv_sem=recv1.at[d, q, slot, k0 + i],
                                device_id=(target,), device_id_type=MESH).start()
                            return carry
                        if chunks == 1:
                            send(0, 0)
                        else:
                            lax.fori_loop(0, chunks, send, 0)

    def load(d, q, slot, k):
        return pltpu.make_async_copy(landing(d, q, slot % 3, k * CR, CR), loads.at[d, slot], load_sem.at[d, slot])

    def load_own(d, q, k):
        owner = flip(me, bits(d)[1]) if q == 0 else me
        for r in range(DEV):
            @pl.when(owner == r)
            def _(r=r):
                for src, row, k0, dst, rows, chunks in segs[r][d]:
                    inside = (k >= k0) & (k < k0 + chunks)
                    at = row if chunks == 1 else pl.multiple_of(row + jnp.where(inside, k - k0, 0) * CR, SB)

                    @pl.when(inside)
                    def _(src=src, at=at, dst=dst, rows=rows):
                        pltpu.make_async_copy(
                            srcs[src].at[pl.ds(at, rows)],
                            loads.at[d, 3, pl.ds(dst % CR, rows)], load_sem.at[d, 3]).start()

    def fetch(d, q, k):
        load_own(d, q, k)
        for slot in range(3):
            hop(d, q, slot, k).wait_recv()
            load(d, q, slot, k).start()

    def ready(d, q, k):
        for slot in range(4):
            load(d, q, slot, k).wait()

    def total(d, rows):
        acc = loads[d, 3, rows, :].astype(jnp.float32)
        for slot in range(3):
            acc = acc + loads[d, slot, rows, :].astype(jnp.float32)
        return acc

    STEP = 112
    accum[...] = jnp.zeros_like(accum)
    used = functools.reduce(lambda acc, r: jnp.where(me == r, PIECES[r][1], acc), range(DEV), 0)

    def out_copy(d, k):
        return pltpu.make_async_copy(
            outs.at[d], g_ref.at[pl.ds(pl.multiple_of(d * half + k * CR, 16), CR)], out_sem.at[d])

    for d in range(2):
        fetch(d, 0, jnp.int32(0))

    @pl.loop(0, NCH)
    def _(k):
        for d in range(2):
            ready(d, 0, k)

            @pl.loop(0, CR // STEP)
            def _(i):
                rows = pl.ds(pl.multiple_of(i * STEP, 16), STEP)
                part[pl.ds(pl.multiple_of(d * half + k * CR + i * STEP, SB), STEP), :] = total(d, rows)

            @pl.when(k + 1 < NCH)
            def _():
                fetch(d, 0, k + 1)

            pass_on(d, k).start()

    for d in range(2):
        fetch(d, 1, jnp.int32(0))

    @pl.loop(0, NCH)
    def _(k):
        for d in range(2):
            ready(d, 1, k)
            pass_on(d, k).wait_recv()

            @pl.when(k > 0)
            def _():
                out_copy(d, k - 1).wait()

            @pl.loop(0, CR // STEP)
            def _(i):
                base = pl.multiple_of(d * half + k * CR + i * STEP, SB)
                rows = pl.ds(pl.multiple_of(i * STEP, 16), STEP)
                g = (total(d, rows) + land[pl.ds(base, STEP), :]) * (1.0 / DEV)
                outs[d, rows, :] = g
                tile = lax.div(base, SB) + lax.broadcasted_iota(jnp.int32, (STEP // SB, SB, LN), 0)
                g3 = g.reshape(STEP // SB, SB, LN)
                keep = counted(me, tile) & (tile < used)
                accum[...] += jnp.sum(jnp.where(keep, g3 * g3, 0.0), axis=0)

            @pl.when(k + 1 < NCH)
            def _():
                fetch(d, 1, k + 1)

            out_copy(d, k).start()

    sq_all[pl.ds(pl.multiple_of(me * SB, SB), SB), :] = accum[...]
    for d in range(2):
        out_copy(d, NCH - 1).wait()
    for d in range(2):
        @pl.loop(0, NCH)
        def _(k):
            for q in range(2):
                for slot in range(3):
                    hop(d, q, slot, k).wait_send()
            pass_on(d, k).wait_send()

    def tell(step):
        return pltpu.make_async_remote_copy(
            src_ref=accum, dst_ref=sq_all.at[pl.ds(pl.multiple_of(me * SB, SB), SB)],
            send_sem=sq_send.at[step], recv_sem=sq_recv.at[step],
            device_id=(lax.rem(me + step + 1, DEV),), device_id_type=MESH)

    for step in range(DEV - 1):
        tell(step).start()
    for step in range(DEV - 1):
        tell(step).wait()
    whole = sq_all[pl.ds(0, SB), :]
    for i in range(1, DEV):
        whole = whole + sq_all[pl.ds(SB * i, SB), :]
    sq_ref[...] = jnp.broadcast_to(jnp.sum(whole, keepdims=True), (SB, LN))


def shared_first():
    found = []
    for r in range(1, DEV):
        kind, tile, stride, row = UNITS[r][0]
        if row >= 0:
            continue
        found.append((r, BLK if kind == "R" else kind // SB))
    return found


def counted(me, tile):
    first = functools.reduce(lambda acc, x: jnp.where(me == x[0], x[1], acc), shared_first(), 0)
    return tile >= first


def reduce_scatter(sources):
    half = NR // 2
    return pl.pallas_call(
        rs_kernel,
        name="reduce_scatter",
        out_shape=(jax.ShapeDtypeStruct((NR, LN), jnp.float32), jax.ShapeDtypeStruct((SB, LN), jnp.float32),
                   jax.ShapeDtypeStruct((12 * half, LN), jnp.bfloat16)),
        in_specs=[pl.BlockSpec(memory_space=pltpu.HBM)] * len(sources),
        out_specs=(pl.BlockSpec(memory_space=pltpu.HBM), pl.BlockSpec(memory_space=pltpu.VMEM),
                   pl.BlockSpec(memory_space=pltpu.HBM)),
        scratch_shapes=[
            pltpu.VMEM((NR, LN), jnp.float32), pltpu.VMEM((NR, LN), jnp.float32),
            pltpu.VMEM((2, 4, CR, LN), jnp.bfloat16), pltpu.VMEM((2, CR, LN), jnp.float32),
            pltpu.VMEM((SB, LN), jnp.float32), pltpu.VMEM((SB * DEV, LN), jnp.float32),
            pltpu.SemaphoreType.DMA((2, 2, 3, NCH)), pltpu.SemaphoreType.DMA((2, 2, 3, NCH)),
            pltpu.SemaphoreType.DMA((2, NCH)), pltpu.SemaphoreType.DMA((2, NCH)),
            pltpu.SemaphoreType.DMA((2, 4)), pltpu.SemaphoreType.DMA((2,)),
            pltpu.SemaphoreType.DMA((DEV - 1,)), pltpu.SemaphoreType.DMA((DEV - 1,))],
        compiler_params=pltpu.CompilerParams(collective_id=0, has_side_effects=True, vmem_limit_bytes=60 << 20),
    )(*sources)


BR = 2304
NB = -(-SROWS // BR)
STEP = 96
KINDS = {"R": 1, 240: 3, 64: SB, 32: 16, "T": 1}
PT = NT // NCH


def unit_tables():
    depth = max(len([u for u in ulist if u[0] == kind]) for ulist in UNITS for kind in KINDS)
    entry = np.zeros((DEV, len(KINDS), 3, depth), np.int32)
    span = np.zeros((DEV, len(KINDS) + 1, 2, NB + 1), np.int32)
    blocks = range(NB)
    for r, ulist in enumerate(UNITS):
        need, made = [NB - 1] * NCH, [0] * NCH
        for n, kind in enumerate(KINDS):
            mine = [u for u in ulist if u[0] == kind]
            length = SB if kind == "T" else GUARD if kind == "R" else kind
            for i, u in enumerate(mine):
                entry[r, n, :, i] = (u[1], u[2], u[3] + GUARD)
                first = max(0, u[3] // BR)
                last = min(NB - 1, (u[3] + length - 1) // BR)
                count = 1 if kind == "T" else BLK if kind == "R" else kind // SB
                for piece in {(u[1] + c * u[2]) // PT for c in range(count)}:
                    need[piece] = min(need[piece], first)
                    made[piece] = max(made[piece], last)
            span[r, n, 0, 1:] = [sum(max(0, u[3] // BR) <= b for u in mine) for b in blocks]
            span[r, n, 1, 1:] = [sum(min(NB - 1, (u[3] + length - 1) // BR) <= b for u in mine) for b in blocks]
        span[r, -1, 0, 1:] = [sum(min(need[i:]) <= b for i in range(NCH)) for b in blocks]
        span[r, -1, 1, 1:] = [sum(max(made[:i + 1]) <= b for i in range(NCH)) for b in blocks]
    return entry, span, depth


ENTRY, SPAN, DEPTH = unit_tables()


def lanes(rows):
    return lax.broadcasted_iota(jnp.int32, (rows, LN), 1)


def roll(x, shift):
    shift = shift % LN
    return x if shift == 0 else pltpu.roll(x, shift, 1)


def swap_blocks(xs, width):
    per = len(xs)
    lane = lanes(xs[0].shape[0])

    def pick(choose):
        out = choose(0)
        for b in range(1, per):
            out = jnp.where(lane >= b * width, choose(b), out)
        return out

    turned = [roll(pick(lambda b: xs[(b + t) % per]), t * width) for t in range(per)]
    return [pick(lambda b: turned[(b - j) % per]) for j in range(per)]


def to_flat(kind, units, tiles, flat, low, ta, tb):
    del low
    if kind == "T" or kind == "R":
        for base, _, row in units:
            if kind == "T":
                flat[pl.ds(row, SB), :] = tiles[base]
            else:
                for c in range(BLK):
                    flat[pl.ds(row + c, SB, stride=BLK), :] = tiles[base + c]
        return
    if kind < LN:
        per = LN // kind
        sets = [units[i:i + per] for i in range(0, len(units), per)]
        for n, some in enumerate(sets):
            ta[n] = jnp.concatenate([tiles[base + i * stride] for base, stride, _ in some for i in range(kind // SB)]).T
        for n, some in enumerate(sets):
            for unit, x in zip(some, swap_blocks([ta[n, pl.ds(q, kind, stride=per), :] for q in range(per)], kind)):
                flat[pl.ds(unit[-1], kind), :] = x
        return
    for n, (base, stride, row) in enumerate(units):
        ta[n] = jnp.concatenate([tiles[base + i * stride] for i in range(16)]).T
        tb[n] = jnp.concatenate([tiles[base + i * stride] for i in range(16, BLK)] + [jnp.zeros((16, LN))]).T
    lane = lanes(16)
    for k in range(15):
        r, o = divmod(LN * k, kind)
        for n, (_, _, row) in enumerate(units):
            x = (ta if o < LN else tb)[n, pl.ds(r, 16, stride=SB), :]
            if 0 < o < LN:
                x = jnp.where(lane >= o, x, tb[n, pl.ds(r, 16, stride=SB), :])
            x = roll(x, -o)
            if o + LN > kind:
                x = jnp.where(lane >= kind - o, roll(ta[n, pl.ds(r + 1, 16, stride=SB), :], kind - o), x)
            flat[pl.ds(row + k, 16, stride=15), :] = x


def to_tiles(kind, units, tiles, flat, low, ta, tb):
    del tiles

    def put(at, value):
        low[at] = value.astype(jnp.bfloat16)

    if kind == "T" or kind == "R":
        for base, _, row in units:
            if kind == "T":
                put(base, flat[pl.ds(row, SB), :])
            else:
                for c in range(BLK):
                    put(base + c, flat[pl.ds(row + c, SB, stride=BLK), :])
        return
    if kind < LN:
        per = LN // kind
        sets = [units[i:i + per] for i in range(0, len(units), per)]
        for n, some in enumerate(sets):
            for q, x in enumerate(swap_blocks([flat[pl.ds(row, kind), :] for _, _, row in some], kind)):
                ta[n, pl.ds(q, kind, stride=per), :] = x
        for n, some in enumerate(sets):
            grid = ta[n].T.reshape(16, SB, LN)
            for u, (base, stride, _) in enumerate(some):
                for i in range(kind // SB):
                    put(base + i * stride, grid[u * (kind // SB) + i])
        return
    lane = lanes(16)
    for r in range(SB):
        k, o = divmod(kind * r, LN)
        for n, (_, _, row) in enumerate(units):
            f = [flat[pl.ds(row + k + i, 16, stride=15), :] for i in range(3 if k + 2 < 15 else 2)]
            ta[n, pl.ds(r, 16, stride=SB), :] = f[0] if o == 0 else roll(jnp.where(lane >= o, f[0], f[1]), -o)
            tb[n, pl.ds(r, 16, stride=SB), :] = f[1] if o == 0 else roll(jnp.where(lane >= o, f[1], f[-1]), -o)
    for n, (base, stride, _) in enumerate(units):
        grid = jnp.concatenate([ta[n].T, tb[n].T]).reshape(32, SB, LN)
        for i in range(BLK):
            put(base + i * stride, grid[i])


def adam_kernel(entry, span, scal, g_ref, sq_ref, m_ref, v_ref, p_ref, m_out, v_out, p_out, a_ref,
                tiles, flat, ta, tb, low, g_sem, a_sem):
    me = lax.axis_index("dp")
    b = pl.program_id(0)

    def take(i):
        here = pl.ds(i * PT, PT)
        return pltpu.make_async_copy(g_ref.at[here], tiles.at[here], g_sem.at[i])

    def give(i):
        here = pl.ds(i * PT, PT)
        return pltpu.make_async_copy(low.at[here], a_ref.at[pl.ds(me * NT + i * PT, PT)], a_sem.at[i])

    def span_of(n, which, at):
        return span[me, (n * 2 + which) * (NB + 1) + at]

    @pl.when(b == 0)
    def _():
        for i in range(NCH):
            take(i).start()

    pl.loop(span_of(len(KINDS), 0, b), span_of(len(KINDS), 0, b + 1))(lambda i: take(i).wait())

    def each(which, work):
        for n, (kind, group) in enumerate(KINDS.items()):
            first, last = span_of(n, which, b), span_of(n, which, b + 1)
            at = n * 3 * DEPTH

            @pl.loop(0, lax.div(last - first + group - 1, group))
            def _(t):
                some = [jnp.minimum(first + t * group + x, last - 1) + at for x in range(group)]
                work(kind, [(entry[me, u], entry[me, u + DEPTH], entry[me, u + 2 * DEPTH]) for u in some],
                     tiles, flat, low, ta, tb)

    each(0, to_flat)

    learn_rate, b1, c1, b2, c2, i1, i2, decay, max_norm = [scal[i] for i in range(9)]
    clip = jnp.minimum(1.0, max_norm / (jnp.sqrt(sq_ref[...]) + CLIP_EPS))[:1]

    @pl.loop(0, BR // STEP)
    def _(i):
        rows = pl.ds(pl.multiple_of(i * STEP, SB), STEP)
        local = b * BR + i * STEP
        here = pl.ds(pl.multiple_of(GUARD + local, SB), STEP)
        h = flat[here, :] * clip
        m = b1 * m_ref[rows, :] + c1 * h
        v = b2 * v_ref[rows, :] + c2 * (h * h)
        p = p_ref[rows, :]
        m_out[rows, :] = m
        v_out[rows, :] = v
        where = me * SROWS + local + lax.broadcasted_iota(jnp.int32, (STEP, LN), 0)
        step = (m * i1) / (jnp.sqrt(v * i2) + ADAM_EPS) + jnp.where(where < DECAY // LN, decay * p, 0.0)
        p = p - learn_rate * step
        p_out[rows, :] = p
        flat[here, :] = p

    pl.loop(span_of(len(KINDS), 1, jnp.maximum(b - 1, 0)), span_of(len(KINDS), 1, b))(lambda i: give(i).start())
    each(1, to_tiles)

    @pl.when(b == NB - 1)
    def _():
        sent = span_of(len(KINDS), 1, NB - 1)
        pl.loop(0, sent)(lambda i: give(i).wait())
        pl.loop(sent, NCH)(lambda i: give(i).start())
        pl.loop(sent, NCH)(lambda i: give(i).wait())


def adam(scal, g, sq, m, v, p):
    block = pl.BlockSpec((BR, LN), lambda b, *_: (b, 0))
    anywhere = pl.BlockSpec(memory_space=pltpu.HBM)
    flat_shape = jax.ShapeDtypeStruct((SROWS, LN), jnp.float32)
    turn = pltpu.VMEM((4, LN, LN), jnp.float32)
    return pl.pallas_call(
        adam_kernel,
        name="adam",
        grid_spec=pltpu.PrefetchScalarGridSpec(
            num_scalar_prefetch=3, grid=(NB,),
            in_specs=[anywhere, pl.BlockSpec((SB, LN), lambda b, *_: (0, 0)), block, block, block],
            out_specs=[block, block, block, anywhere],
            scratch_shapes=[
                pltpu.VMEM((NT, SB, LN), jnp.float32), pltpu.VMEM((NB * BR + 2 * GUARD + SB, LN), jnp.float32),
                turn, turn, pltpu.VMEM((NT, SB, LN), jnp.bfloat16),
                pltpu.SemaphoreType.DMA((NCH,)), pltpu.SemaphoreType.DMA((NCH,))]),
        out_shape=[flat_shape, flat_shape, flat_shape, jax.ShapeDtypeStruct((DEV * NT, SB, LN), jnp.bfloat16)],
        compiler_params=pltpu.CompilerParams(dimension_semantics=("arbitrary",), vmem_limit_bytes=63 << 20),
    )(jnp.asarray(ENTRY.reshape(DEV, -1)), jnp.asarray(SPAN.reshape(DEV, -1)), scal, g.reshape(NT, SB, LN), sq, m, v, p)


def ag_kernel(a_in, a_ref, send, recv):
    del a_in
    me = lax.axis_index("dp")
    barrier_all(me)
    half = NR // 2
    xn, yn, pn = flip(me, 2), flip(me, 4), flip(me, 1)
    diag = flip(xn, 4)

    def copy(kind, d, k):
        owner = (me, me, me, xn if d == 0 else yn, xn, yn, diag)[kind]
        target = (xn, yn, pn, yn if d == 0 else xn, pn, pn, pn)[kind]
        part = a_ref.at[pl.ds(owner * NR + d * half + k * CR, CR)]
        return pltpu.make_async_remote_copy(
            src_ref=part, dst_ref=part, send_sem=send.at[kind, d, k], recv_sem=recv.at[kind, d, k],
            device_id=(target,), device_id_type=MESH)

    for turn in range(2):
        @pl.loop(0, NCH)
        def _(k):
            copy(0, turn, k).start()
            copy(1, 1 - turn, k).start()
            copy(2, turn, k).start()

    @pl.loop(0, NCH)
    def _(k):
        copy(0, 0, k).wait_recv()
        copy(3, 0, k).start()
        copy(4, 0, k).start()
        copy(1, 1, k).wait_recv()
        copy(3, 1, k).start()
        copy(5, 1, k).start()

    @pl.loop(0, NCH)
    def _(k):
        copy(0, 1, k).wait_recv()
        copy(4, 1, k).start()
        copy(1, 0, k).wait_recv()
        copy(5, 0, k).start()

    @pl.loop(0, NCH)
    def _(k):
        for d in range(2):
            copy(3, d, k).wait_recv()
            copy(6, d, k).start()

    @pl.loop(0, NCH)
    def _(k):
        for d in range(2):
            for kind in (2, 4, 5, 6):
                copy(kind, d, k).wait_recv()
            for kind in range(7):
                copy(kind, d, k).wait_send()


def all_gather(mine):
    anywhere = pl.BlockSpec(memory_space=pltpu.HBM)
    return pl.pallas_call(
        ag_kernel,
        name="all_gather",
        out_shape=jax.ShapeDtypeStruct((DEV * NR, LN), jnp.bfloat16),
        in_specs=[anywhere], out_specs=anywhere,
        scratch_shapes=[pltpu.SemaphoreType.DMA((7, 2, NCH)), pltpu.SemaphoreType.DMA((7, 2, NCH))],
        input_output_aliases={0: 0},
        compiler_params=pltpu.CompilerParams(collective_id=1, has_side_effects=True),
    )(mine)


def as_tiles(t, x):
    kind, rows, layers = TENSORS[t]
    if kind == "C":
        x = jnp.swapaxes(x, -1, -2)
    return x.reshape(layers, rows // SB, SB, BLK, LN).transpose(0, 1, 3, 2, 4)


def from_tiles(t, x, shape):
    kind, rows, layers = TENSORS[t]
    x = x.transpose(0, 1, 3, 2, 4)
    if kind == "C":
        return jnp.swapaxes(x.reshape(layers, rows, D), -1, -2)
    return x.reshape(shape)


def unpack_plan():
    copies, shared, cuts = [], [], {}
    for t, (kind, rows, layers) in enumerate(TENSORS):
        last_seen = None
        for r, (plist, _) in enumerate(PIECES):
            for pt, l, first, last, off in plist:
                if pt != t:
                    continue
                src = r * NT + off
                if (t, l) in CUT:
                    cuts.setdefault((t, l), []).append((first, last, src, r * SHARE))
                    continue
                if kind == "C":
                    copies.append([src, t, l * BLK * rows // SB, BLK * rows // SB])
                    continue
                begin = first
                if last_seen and first < last_seen[0]:
                    copies[-1][3] -= BLK
                    shared.append((t, first, last_seen[1] - BLK, src, STARTS[t] + first * SB * D, r * SHARE))
                    begin = first + 1
                copies.append([src + (begin - first) * BLK, t, begin * BLK, (last - begin) * BLK])
                last_seen = (last, src + (last - first) * BLK)
    pieces = []
    for src, t, dst, tiles in copies:
        while tiles > 0:
            n = min(tiles, UN)
            pieces.append((src, t, dst, n))
            src, dst, tiles = src + n, dst + n, tiles - n
    return pieces, shared, cuts


UN = 480
UBUF = 12


def unpack_kernel(src_ref, *refs):
    outs = refs[:len(TENSORS)]
    ring, left, right, *layers, in_sem, out_sem, pair_sem, cut_sem = refs[len(TENSORS):]
    pieces, shared, cuts = unpack_plan()

    def take(i):
        src, _, _, n = pieces[i]
        return pltpu.make_async_copy(src_ref.at[pl.ds(src, n)], ring.at[i % UBUF, pl.ds(0, n)], in_sem.at[i % UBUF])

    def give(i):
        _, t, dst, n = pieces[i]
        return pltpu.make_async_copy(ring.at[i % UBUF, pl.ds(0, n)], outs[t].at[pl.ds(dst, n)], out_sem.at[i % UBUF])

    def pair(n):
        _, _, a, b, _, _ = shared[n]
        return (pltpu.make_async_copy(src_ref.at[pl.ds(a, BLK)], left.at[n], pair_sem.at[n, 0]),
                pltpu.make_async_copy(src_ref.at[pl.ds(b, BLK)], right.at[n], pair_sem.at[n, 1]))

    def cut_loads(n):
        (t, _), sides = list(cuts.items())[n]
        c8 = TENSORS[t][1] // SB
        made = []
        for side, (first, last, src, _) in enumerate(sides):
            for j in range(first, last):
                over = side == 1 and first < sides[0][1] and j == first
                to = right.at[len(shared) + n, pl.ds(0, c8)] if over else layers[n].at[pl.ds(0, c8), j]
                made.append(pltpu.make_async_copy(
                    src_ref.at[pl.ds(src + (j - first) * c8, c8)], to, cut_sem.at[n, BLK if over else j]))
        return made

    def cut_stores(n):
        (t, l), _ = list(cuts.items())[n]
        c8 = TENSORS[t][1] // SB
        return [pltpu.make_async_copy(layers[n].at[c], outs[t].at[pl.ds((l * c8 + c) * BLK, BLK)], cut_sem.at[n, c])
                for c in range(c8)]

    def spot(start, row_step, lane_step, tile_step, tiles):
        shape = (tiles, SB, LN)
        return (start + tile_step * lax.broadcasted_iota(jnp.int32, shape, 0)
                + row_step * lax.broadcasted_iota(jnp.int32, shape, 1)
                + lane_step * lax.broadcasted_iota(jnp.int32, shape, 2))

    for n in range(len(shared)):
        for c in pair(n):
            c.start()
    for n in range(len(cuts)):
        for c in cut_loads(n):
            c.start()
    depth = UBUF // 2
    for i in range(depth):
        take(i).start()
    for i in range(len(pieces)):
        if i + depth < len(pieces):
            if i + depth >= UBUF:
                give(i + depth - UBUF).wait()
            take(i + depth).start()
        take(i).wait()
        give(i).start()
        if i == depth:
            for n, (t, _, _, _, start, bound) in enumerate(shared):
                for c in pair(n):
                    c.wait()
                keep = spot(start, D, 1, LN, BLK) < bound
                left[n] = jnp.where(keep, left[n].astype(jnp.float32), right[n].astype(jnp.float32)).astype(jnp.bfloat16)
            for n, ((t, l), sides) in enumerate(cuts.items()):
                for c in cut_loads(n):
                    c.wait()
                rows = TENSORS[t][1]
                j, bound = sides[1][0], sides[1][3]
                if j < sides[0][1]:
                    keep = spot(STARTS[t] + (l * D + j * LN) * rows, 1, rows, SB, rows // SB) < bound
                    one = right[len(shared) + n, pl.ds(0, rows // SB)].astype(jnp.float32)
                    here = pl.ds(0, rows // SB)
                    layers[n][here, j] = jnp.where(keep, layers[n][here, j].astype(jnp.float32), one).astype(jnp.bfloat16)
        if i == depth + 2:
            for n, (t, g, _, _, _, _) in enumerate(shared):
                pltpu.make_async_copy(left.at[n], outs[t].at[pl.ds(g * BLK, BLK)], pair_sem.at[n, 0]).start()
            for n in range(len(cuts)):
                for c in cut_stores(n):
                    c.start()
    for i in range(max(0, len(pieces) - UBUF), len(pieces)):
        give(i).wait()
    for n, (t, g, _, _, _, _) in enumerate(shared):
        pltpu.make_async_copy(left.at[n], outs[t].at[pl.ds(g * BLK, BLK)], pair_sem.at[n, 0]).wait()
    for n in range(len(cuts)):
        for c in cut_stores(n):
            c.wait()


def unpack(gathered, shapes):
    pieces, shared, cuts = unpack_plan()
    anywhere = pl.BlockSpec(memory_space=pltpu.HBM)
    tiles = pl.pallas_call(
        unpack_kernel,
        name="unpack",
        out_shape=[jax.ShapeDtypeStruct((size // 1024, SB, LN), jnp.bfloat16) for size in SIZES],
        in_specs=[anywhere], out_specs=[anywhere] * len(TENSORS),
        scratch_shapes=[
            pltpu.VMEM((UBUF, UN, SB, LN), jnp.bfloat16), pltpu.VMEM((len(shared) + 1, BLK, SB, LN), jnp.bfloat16),
            pltpu.VMEM((len(shared) + len(cuts) + 1, BLK, SB, LN), jnp.bfloat16),
            *[pltpu.VMEM((TENSORS[t][1] // SB + 1, BLK, SB, LN), jnp.bfloat16) for t, _ in cuts],
            pltpu.SemaphoreType.DMA((UBUF,)), pltpu.SemaphoreType.DMA((UBUF,)),
            pltpu.SemaphoreType.DMA((len(shared), 2)), pltpu.SemaphoreType.DMA((len(cuts), BLK + 1))],
        compiler_params=pltpu.CompilerParams(vmem_limit_bytes=48 << 20),
    )(gathered.reshape(DEV * NT, SB, LN))
    outs = [from_tiles(t, x.reshape(TENSORS[t][2], TENSORS[t][1] // SB, BLK, SB, LN), shapes[t])
            for t, x in enumerate(tiles)]
    plist, _ = PIECES[DEV - 1]
    base = ((DEV - 1) * NT + plist[-1][4]) * SB
    tail = gathered[base:base + TAIL // LN].reshape(-1)
    cut = math.prod(shapes[SB])
    return outs + [tail[:cut].reshape(shapes[SB]), tail[cut:].reshape(shapes[9])]


def sources(grads):
    views = [as_tiles(t, grads[t][0]) for t in range(len(TENSORS))]
    tail = jnp.concatenate([grads[SB].reshape(-1), grads[9].reshape(-1), jnp.zeros((-TAIL % 2048,), jnp.bfloat16)])
    turned = []
    for t, l in CUT:
        layer = jnp.swapaxes(lax.optimization_barrier(grads[t][:, l]), 1, 2)
        turned.append(layer.reshape(-1, SB, BLK, LN).transpose(2, 0, 1, 3))
    return [x.reshape(-1, LN) for x in views + [tail] + turned]


def solution(mesh):
    def local_update(*arrays):
        grads = arrays[:10]
        m, v, p, hyper = arrays[10:]
        shapes = [x.shape[1:] for x in grads]
        share, squares, _ = reduce_scatter(sources(grads))
        learn_rate, b1, b2, decay, max_norm = [hyper[i] for i in range(5)]
        scal = jnp.stack([learn_rate, b1, 1.0 - b1, b2, 1.0 - b2, 1.0 / (1.0 - b1 ** ADAM_STEP),
                          1.0 / (1.0 - b2 ** ADAM_STEP), decay, max_norm])
        m, v, p, mine = adam(scal, share, squares, *[x.reshape(SROWS, LN) for x in (m, v, p)])
        params = unpack(all_gather(mine.reshape(DEV * NR, LN)), shapes)
        return tuple(params) + tuple(x.reshape(SHARE) for x in (m, v, p))

    in_specs = tuple([P("dp")] * 10 + [P("dp"), P("dp"), P("dp"), P()])
    out_specs = tuple([P()] * 10 + [P("dp"), P("dp"), P("dp")])
    return jax.shard_map(local_update, mesh=mesh, in_specs=in_specs, out_specs=out_specs, check_vma=False)
```

```python
import functools
import math

import jax
import jax.numpy as jnp
import numpy as np
from jax import lax
from jax.experimental import pallas as pl
from jax.experimental.pallas import tpu as pltpu
from jax.sharding import PartitionSpec as P

ADAM_STEP = 7
LN = 128
SB = 8
ADAM_EPS = 1e-8
CLIP_EPS = 1e-6
D = 3840
BLK = D // LN
LAYERS = 6
DEV = 8
TENSORS = (("R", 4096, 1), ("C", 64, LAYERS), ("C", 32, LAYERS), ("C", 32, LAYERS), ("R", 64 * LAYERS, 1),
           ("C", 240, LAYERS), ("C", 240, LAYERS), ("R", 240 * LAYERS, 1))
SIZES = tuple(rows * layers * D for _, rows, layers in TENSORS)
STARTS = tuple(sum(SIZES[:i]) for i in range(len(SIZES)))
DECAY = sum(SIZES)
TAIL = LAYERS * 4 * D + LAYERS * 2 * 256
TOTAL = DECAY + TAIL
SHARE = TOTAL // DEV
SROWS = SHARE // LN
NT = 4536
NR = NT * SB
GUARD = 240
NCH = 9
CR = NR // 2 // NCH
MESH = pl.DeviceIdType.MESH


def plan():
    pieces, units = [], []
    for r in range(DEV):
        lo, hi = r * SHARE, (r + 1) * SHARE
        off, plist, ulist = 0, [], []
        for t, (kind, rows, layers) in enumerate(TENSORS):
            if kind == "R":
                a, b = max(lo, STARTS[t]), min(hi, STARTS[t] + SIZES[t])
                if a >= b:
                    continue
                g0, g1 = (a - STARTS[t]) // (SB * D), -((STARTS[t] - b) // (SB * D))
                plist.append((t, 0, g0, g1, off))
                for g in range(g0, g1):
                    ulist.append(("R", off + (g - g0) * BLK, 1, (STARTS[t] + g * SB * D - lo) // LN))
                off += (g1 - g0) * BLK
                continue
            for l in range(layers):
                s = STARTS[t] + l * rows * D
                a, b = max(lo, s), min(hi, s + rows * D)
                if a >= b:
                    continue
                j0, j1 = (a - s) // (LN * rows), -((s - b) // (LN * rows))
                plist.append((t, l, j0, j1, off))
                whole = j1 - j0 == BLK
                for j in range(j0, j1):
                    at, stride = (j, BLK) if whole else ((j - j0) * (rows // SB), 1)
                    ulist.append((rows, off + at, stride, (s + j * LN * rows - lo) // LN))
                off += (j1 - j0) * rows // SB
        if hi > DECAY:
            for i in range(TAIL // 1024):
                ulist.append(("T", off + i, 1, (DECAY - lo) // LN + SB * i))
            plist.append((len(TENSORS), 0, 0, TAIL // 1024, off))
            off += TAIL // 1024
        assert off <= NT
        pieces.append((plist, off))
        units.append(ulist)
    return pieces, units


PIECES, UNITS = plan()


def flip(dev, bit):
    return dev + bit - 2 * bit * (lax.rem(lax.div(dev, bit), 2))


def barrier_all(me):
    sem = pltpu.get_barrier_semaphore()
    for step in range(1, DEV):
        pl.semaphore_signal(sem, inc=1, device_id=(lax.rem(me + step, DEV),), device_id_type=MESH)
    pl.semaphore_wait(sem, DEV - 1)


def cut_layers():
    return sorted({(t, l) for plist, _ in PIECES for t, l, a, b, _ in plist
                   if t < len(TENSORS) and TENSORS[t][0] == "C" and b - a < BLK})


CUT = cut_layers()


def segments():
    found = []
    for plist, used in PIECES:
        runs = []
        for t, l, first, last, off in plist:
            if t == len(TENSORS):
                src, row, rows = t, 0, -(-last // 2) * 16
            elif TENSORS[t][0] == "R":
                src, row, rows = t, first * BLK * SB, (last - first) * BLK * SB
            elif (t, l) in CUT:
                c = TENSORS[t][1]
                src, row, rows = len(TENSORS) + 1 + CUT.index((t, l)), first * c, (last - first) * c
            else:
                src, row, rows = t, l * BLK * TENSORS[t][1], BLK * TENSORS[t][1]
            if runs and runs[-1][0] == src and runs[-1][1] + runs[-1][3] == row:
                runs[-1][3] += rows
            else:
                runs.append([src, row, off * SB, rows])
        end = runs[-1][2] + runs[-1][3]
        if end < NR:
            runs.append([0, 0, end, NR - end])
        halves = ([], [])
        for src, row, dst, rows in runs:
            while rows > 0:
                n = min(rows, CR - dst % CR)
                d, k = divmod(dst // CR, NCH)
                last = halves[d][-1] if halves[d] else None
                if last and n == CR and last[0] == src and last[4] == CR and last[1] + last[5] * CR == row:
                    last[5] += 1
                else:
                    halves[d].append([src, row, k, dst - d * (NR // 2), n, 1])
                row, dst, rows = row + n, dst + n, rows - n
        found.append(halves)
    return found


def rs_kernel(*refs):
    count = len(TENSORS) + 1 + len(CUT)
    srcs, (g_ref, sq_ref, r_ref, part, land, loads, outs, accum, sq_all,
           send1, recv1, send2, recv2, load_sem, out_sem, sq_send, sq_recv) = refs[:count], refs[count:]
    me = lax.axis_index("dp")
    barrier_all(me)
    half = NR // 2
    segs = segments()

    def bits(d):
        return 2 + 2 * d, 4 - 2 * d

    def landing(d, q, slot, row, rows):
        return r_ref.at[pl.ds(pl.multiple_of(((d * 2 + q) * 3 + slot) * half + row, 16), rows)]

    def hop(d, q, slot, k):
        here = landing(d, q, slot, k * CR, CR)
        return pltpu.make_async_remote_copy(
            src_ref=here, dst_ref=here, send_sem=send1.at[d, q, slot, k], recv_sem=recv1.at[d, q, slot, k],
            device_id=(flip(me, 1),), device_id_type=MESH)

    def pass_on(d, k):
        rows = pl.ds(pl.multiple_of(d * half + k * CR, 16), CR)
        return pltpu.make_async_remote_copy(
            src_ref=part.at[rows], dst_ref=land.at[rows], send_sem=send2.at[d, k], recv_sem=recv2.at[d, k],
            device_id=(flip(me, bits(d)[1]),), device_id_type=MESH)

    @pl.loop(0, 12)
    def _(h):
        q, turn, d = lax.div(h, 6), lax.rem(lax.div(h, 2), 3), lax.rem(h, 2)
        slot = lax.rem(turn + 1, 3)
        first, second = bits(d)
        away = flip(me, first)
        target = jnp.where(slot == 0, flip(me, 1), jnp.where(slot == 1, away, flip(away, 1)))
        owner = jnp.where(q == 0, flip(target, second), target)
        for r in range(DEV):
            for dd in range(2):
                @pl.when((owner == r) & (d == dd))
                def _():
                    for src, row, k0, dst, rows, chunks in segs[r][dd]:
                        def send(i, carry, src=src, row=row, k0=k0, dst=dst, rows=rows):
                            pltpu.make_async_remote_copy(
                                src_ref=srcs[src].at[pl.ds(pl.multiple_of(row + i * CR, SB), rows)],
                                dst_ref=r_ref.at[pl.ds(pl.multiple_of(
                                    ((d * 2 + q) * 3 + slot) * half + dst + i * CR, SB), rows)],
                                send_sem=send1.at[d, q, slot, k0 + i], recv_sem=recv1.at[d, q, slot, k0 + i],
                                device_id=(target,), device_id_type=MESH).start()
                            return carry
                        if chunks == 1:
                            send(0, 0)
                        else:
                            lax.fori_loop(0, chunks, send, 0)

    def load(d, q, slot, k):
        return pltpu.make_async_copy(landing(d, q, slot % 3, k * CR, CR), loads.at[d, slot], load_sem.at[d, slot])

    def load_own(d, q, k):
        owner = flip(me, bits(d)[1]) if q == 0 else me
        for r in range(DEV):
            @pl.when(owner == r)
            def _(r=r):
                for src, row, k0, dst, rows, chunks in segs[r][d]:
                    inside = (k >= k0) & (k < k0 + chunks)
                    at = row if chunks == 1 else pl.multiple_of(row + jnp.where(inside, k - k0, 0) * CR, SB)

                    @pl.when(inside)
                    def _(src=src, at=at, dst=dst, rows=rows):
                        pltpu.make_async_copy(
                            srcs[src].at[pl.ds(at, rows)],
                            loads.at[d, 3, pl.ds(dst % CR, rows)], load_sem.at[d, 3]).start()

    def fetch(d, q, k):
        load_own(d, q, k)
        for slot in range(3):
            hop(d, q, slot, k).wait_recv()
            load(d, q, slot, k).start()

    def ready(d, q, k):
        for slot in range(4):
            load(d, q, slot, k).wait()

    def total(d, rows):
        acc = loads[d, 3, rows, :].astype(jnp.float32)
        for slot in range(3):
            acc = acc + loads[d, slot, rows, :].astype(jnp.float32)
        return acc

    STEP = 112
    accum[...] = jnp.zeros_like(accum)
    used = functools.reduce(lambda acc, r: jnp.where(me == r, PIECES[r][1], acc), range(DEV), 0)

    def out_copy(d, k):
        return pltpu.make_async_copy(
            outs.at[d], g_ref.at[pl.ds(pl.multiple_of(d * half + k * CR, 16), CR)], out_sem.at[d])

    for d in range(2):
        fetch(d, 0, jnp.int32(0))

    @pl.loop(0, NCH)
    def _(k):
        for d in range(2):
            ready(d, 0, k)

            @pl.loop(0, CR // STEP)
            def _(i):
                rows = pl.ds(pl.multiple_of(i * STEP, 16), STEP)
                part[pl.ds(pl.multiple_of(d * half + k * CR + i * STEP, SB), STEP), :] = total(d, rows)

            @pl.when(k + 1 < NCH)
            def _():
                fetch(d, 0, k + 1)

            pass_on(d, k).start()

    for d in range(2):
        fetch(d, 1, jnp.int32(0))

    @pl.loop(0, NCH)
    def _(k):
        for d in range(2):
            ready(d, 1, k)
            pass_on(d, k).wait_recv()

            @pl.when(k > 0)
            def _():
                out_copy(d, k - 1).wait()

            @pl.loop(0, CR // STEP)
            def _(i):
                base = pl.multiple_of(d * half + k * CR + i * STEP, SB)
                rows = pl.ds(pl.multiple_of(i * STEP, 16), STEP)
                g = (total(d, rows) + land[pl.ds(base, STEP), :]) * (1.0 / DEV)
                outs[d, rows, :] = g
                tile = lax.div(base, SB) + lax.broadcasted_iota(jnp.int32, (STEP // SB, SB, LN), 0)
                g3 = g.reshape(STEP // SB, SB, LN)
                keep = counted(me, tile) & (tile < used)
                accum[...] += jnp.sum(jnp.where(keep, g3 * g3, 0.0), axis=0)

            @pl.when(k + 1 < NCH)
            def _():
                fetch(d, 1, k + 1)

            out_copy(d, k).start()

    sq_all[pl.ds(pl.multiple_of(me * SB, SB), SB), :] = accum[...]
    for d in range(2):
        out_copy(d, NCH - 1).wait()
    for d in range(2):
        @pl.loop(0, NCH)
        def _(k):
            for q in range(2):
                for slot in range(3):
                    hop(d, q, slot, k).wait_send()
            pass_on(d, k).wait_send()

    def tell(step):
        return pltpu.make_async_remote_copy(
            src_ref=accum, dst_ref=sq_all.at[pl.ds(pl.multiple_of(me * SB, SB), SB)],
            send_sem=sq_send.at[step], recv_sem=sq_recv.at[step],
            device_id=(lax.rem(me + step + 1, DEV),), device_id_type=MESH)

    for step in range(DEV - 1):
        tell(step).start()
    for step in range(DEV - 1):
        tell(step).wait()
    whole = sq_all[pl.ds(0, SB), :]
    for i in range(1, DEV):
        whole = whole + sq_all[pl.ds(SB * i, SB), :]
    sq_ref[...] = jnp.broadcast_to(jnp.sum(whole, keepdims=True), (SB, LN))


def shared_first():
    found = []
    for r in range(1, DEV):
        kind, tile, stride, row = UNITS[r][0]
        if row >= 0:
            continue
        found.append((r, BLK if kind == "R" else kind // SB))
    return found


def counted(me, tile):
    first = functools.reduce(lambda acc, x: jnp.where(me == x[0], x[1], acc), shared_first(), 0)
    return tile >= first


def reduce_scatter(sources):
    half = NR // 2
    return pl.pallas_call(
        rs_kernel,
        name="reduce_scatter",
        out_shape=(jax.ShapeDtypeStruct((NR, LN), jnp.float32), jax.ShapeDtypeStruct((SB, LN), jnp.float32),
                   jax.ShapeDtypeStruct((12 * half, LN), jnp.bfloat16)),
        in_specs=[pl.BlockSpec(memory_space=pltpu.HBM)] * len(sources),
        out_specs=(pl.BlockSpec(memory_space=pltpu.HBM), pl.BlockSpec(memory_space=pltpu.VMEM),
                   pl.BlockSpec(memory_space=pltpu.HBM)),
        scratch_shapes=[
            pltpu.VMEM((NR, LN), jnp.float32), pltpu.VMEM((NR, LN), jnp.float32),
            pltpu.VMEM((2, 4, CR, LN), jnp.bfloat16), pltpu.VMEM((2, CR, LN), jnp.float32),
            pltpu.VMEM((SB, LN), jnp.float32), pltpu.VMEM((SB * DEV, LN), jnp.float32),
            pltpu.SemaphoreType.DMA((2, 2, 3, NCH)), pltpu.SemaphoreType.DMA((2, 2, 3, NCH)),
            pltpu.SemaphoreType.DMA((2, NCH)), pltpu.SemaphoreType.DMA((2, NCH)),
            pltpu.SemaphoreType.DMA((2, 4)), pltpu.SemaphoreType.DMA((2,)),
            pltpu.SemaphoreType.DMA((DEV - 1,)), pltpu.SemaphoreType.DMA((DEV - 1,))],
        compiler_params=pltpu.CompilerParams(collective_id=0, has_side_effects=True, vmem_limit_bytes=60 << 20),
    )(*sources)


BR = 2304
NB = -(-SROWS // BR)
STEP = 96
KINDS = {"R": 1, 240: 3, 64: SB, 32: 16, "T": 1}
PIECES_OUT = 2 * NCH
PT = NT // PIECES_OUT


def unit_runs():
    runs = {kind: [] for kind in KINDS}
    need = np.full((PIECES_OUT, DEV), NB - 1)
    made = np.zeros((PIECES_OUT, DEV), int)
    for r, ulist in enumerate(UNITS):
        for kind in KINDS:
            mine = [u for u in ulist if u[0] == kind]
            size, count = UNIT_SIZE[kind]
            found = []
            for i, (_, tile, stride, row) in enumerate(mine):
                first = max(0, row // BR)
                last = min(NB - 1, (row + size - 1) // BR)
                for piece in {(tile + c * stride) // PT for c in range(count)}:
                    need[piece, r] = min(need[piece, r], first)
                    made[piece, r] = max(made[piece, r], last)
                per = 1 if stride == BLK else count
                if not found or stride != found[-1][-1] or row + GUARD != found[-1][2] + found[-1][0] * size:
                    found.append([0, tile, row + GUARD, BLK * count, per, stride])
                n, start, _, step, per, _ = found[-1]
                assert tile == start + n // BLK * step + n % BLK * per
                found[-1][0] += 1
            for slot, run in enumerate(found):
                if slot == len(runs[kind]):
                    runs[kind].append(np.zeros((6, DEV), int))
                runs[kind][slot][:, r] = run
    for i in range(PIECES_OUT):
        need[i] = need[i:].min(axis=0)
        made[i] = made[:i + 1].max(axis=0)
    return runs, need, made


UNIT_SIZE = {"R": (GUARD, BLK), 240: (240, BLK), 64: (64, SB), 32: (32, 4), "T": (SB, 1)}
RUNS, NEED, MADE = unit_runs()


def by_owner(me, values):
    out = int(values[0])
    for r in range(1, DEV):
        if int(values[r]) != int(values[r - 1]):
            out = jnp.where(me >= r, int(values[r]), out)
    return out


def lanes(rows):
    return lax.broadcasted_iota(jnp.int32, (rows, LN), 1)


def roll(x, shift):
    shift = shift % LN
    return x if shift == 0 else pltpu.roll(x, shift, 1)


def swap_blocks(xs, width):
    per = len(xs)
    lane = lanes(xs[0].shape[0])

    def pick(choose):
        out = choose(0)
        for b in range(1, per):
            out = jnp.where(lane >= b * width, choose(b), out)
        return out

    turned = [roll(pick(lambda b: xs[(b + t) % per]), t * width) for t in range(per)]
    return [pick(lambda b: turned[(b - j) % per]) for j in range(per)]


def to_flat(kind, units, tiles, flat, low, ta, tb):
    del low
    if kind == "T" or kind == "R":
        for base, _, row in units:
            if kind == "T":
                flat[pl.ds(row, SB), :] = tiles[base]
            else:
                for c in range(BLK):
                    flat[pl.ds(row + c, SB, stride=BLK), :] = tiles[base + c]
        return
    if kind < LN:
        per = LN // kind
        sets = [units[i:i + per] for i in range(0, len(units), per)]
        for n, some in enumerate(sets):
            ta[n] = jnp.concatenate([tiles[base + i * stride] for base, stride, _ in some for i in range(kind // SB)]).T
        for n, some in enumerate(sets):
            for unit, x in zip(some, swap_blocks([ta[n, pl.ds(q, kind, stride=per), :] for q in range(per)], kind)):
                flat[pl.ds(unit[-1], kind), :] = x
        return
    for n, (base, stride, row) in enumerate(units):
        ta[n] = jnp.concatenate([tiles[base + i * stride] for i in range(16)]).T
        tb[n] = jnp.concatenate([tiles[base + i * stride] for i in range(16, BLK)] + [jnp.zeros((16, LN))]).T
    lane = lanes(16)
    for k in range(15):
        r, o = divmod(LN * k, kind)
        for n, (_, _, row) in enumerate(units):
            x = (ta if o < LN else tb)[n, pl.ds(r, 16, stride=SB), :]
            if 0 < o < LN:
                x = jnp.where(lane >= o, x, tb[n, pl.ds(r, 16, stride=SB), :])
            x = roll(x, -o)
            if o + LN > kind:
                x = jnp.where(lane >= kind - o, roll(ta[n, pl.ds(r + 1, 16, stride=SB), :], kind - o), x)
            flat[pl.ds(row + k, 16, stride=15), :] = x


def to_tiles(kind, units, tiles, flat, low, ta, tb):
    del tiles

    def put(at, value):
        low[at] = value.astype(jnp.bfloat16)

    if kind == "T" or kind == "R":
        for base, _, row in units:
            if kind == "T":
                put(base, flat[pl.ds(row, SB), :])
            else:
                for c in range(BLK):
                    put(base + c, flat[pl.ds(row + c, SB, stride=BLK), :])
        return
    if kind < LN:
        per = LN // kind
        sets = [units[i:i + per] for i in range(0, len(units), per)]
        for n, some in enumerate(sets):
            for q, x in enumerate(swap_blocks([flat[pl.ds(row, kind), :] for _, _, row in some], kind)):
                ta[n, pl.ds(q, kind, stride=per), :] = x
        for n, some in enumerate(sets):
            grid = ta[n].T.reshape(16, SB, LN)
            for u, (base, stride, _) in enumerate(some):
                for i in range(kind // SB):
                    put(base + i * stride, grid[u * (kind // SB) + i])
        return
    lane = lanes(16)
    for r in range(SB):
        k, o = divmod(kind * r, LN)
        for n, (_, _, row) in enumerate(units):
            f = [flat[pl.ds(row + k + i, 16, stride=15), :] for i in range(3 if k + 2 < 15 else 2)]
            ta[n, pl.ds(r, 16, stride=SB), :] = f[0] if o == 0 else roll(jnp.where(lane >= o, f[0], f[1]), -o)
            tb[n, pl.ds(r, 16, stride=SB), :] = f[1] if o == 0 else roll(jnp.where(lane >= o, f[1], f[-1]), -o)
    for n, (base, stride, _) in enumerate(units):
        grid = jnp.concatenate([ta[n].T, tb[n].T]).reshape(32, SB, LN)
        for i in range(BLK):
            put(base + i * stride, grid[i])


def step_kernel(scal, g_ref, sq_ref, m_ref, v_ref, p_ref, m_out, v_out, p_out, a_ref,
                tiles, flat, ta, tb, low, g_sem, a_sem, send, recv):
    me = lax.axis_index("dp")
    b = pl.program_id(0)
    xn, yn, pn = flip(me, 2), flip(me, 4), flip(me, 1)
    diag = flip(xn, 4)

    def take(i):
        here = pl.ds(i * PT, PT)
        return pltpu.make_async_copy(g_ref.at[here], tiles.at[here], g_sem.at[i])

    def keep(i):
        return pltpu.make_async_copy(low.at[pl.ds(i * PT, PT)], a_ref.at[pl.ds(me * NT + i * PT, PT)], a_sem.at[i])

    def copy(kind, d, k):
        owner = (me, me, me, xn if d == 0 else yn, xn, yn, diag)[kind]
        target = (xn, yn, pn, yn if d == 0 else xn, pn, pn, pn)[kind]
        at = (2 * k + d) * PT
        there = a_ref.at[pl.ds(owner * NT + at, PT)]
        return pltpu.make_async_remote_copy(
            src_ref=low.at[pl.ds(at, PT)] if kind < 3 else there, dst_ref=there,
            send_sem=send.at[kind, d, k], recv_sem=recv.at[kind, d, k],
            device_id=(target,), device_id_type=MESH)

    def give(i):
        for kind in range(3):
            copy(kind, i % 2, i // 2).start()
        keep(i).start()

    @pl.when(b == 0)
    def _():
        barrier_all(me)
        for i in range(PIECES_OUT):
            take(i).start()

    made = [by_owner(me, MADE[i]) for i in range(PIECES_OUT)]
    for i in range(PIECES_OUT):
        pl.when(b == made[i] + 1)(functools.partial(give, i))
    for i in range(PIECES_OUT):
        pl.when(b == by_owner(me, NEED[i]))(lambda i=i: take(i).wait())

    def upto(block, count, row, size, whole):
        room = (block + 1) * BR + GUARD - row
        n = lax.div(jnp.where(room > 0, room, 0) + (0 if whole else size - 1), size)
        return jnp.where(n < count, n, count)

    def each(whole, work):
        for kind, group in KINDS.items():
            size = UNIT_SIZE[kind][0]
            for run in RUNS[kind]:
                count, start, row, step, per, stride = [by_owner(me, x) for x in run]
                first = jnp.where(b > 0, upto(b - 1, count, row, size, whole), 0)
                last = upto(b, count, row, size, whole)
                if whole:
                    last = jnp.where(b < NB - 1, last, count)

                @pl.loop(0, lax.div(last - first + group - 1, group))
                def _(t):
                    units = []
                    for x in range(group):
                        i = first + t * group + x
                        i = jnp.where(i < last, i, last - 1)
                        units.append((start + lax.div(i, BLK) * step + lax.rem(i, BLK) * per, stride, row + i * size))
                    work(kind, units, tiles, flat, low, ta, tb)

    each(False, to_flat)

    learn_rate, b1, c1, b2, c2, i1, i2, decay, max_norm = [scal[i] for i in range(9)]
    clip = jnp.minimum(1.0, max_norm / (jnp.sqrt(sq_ref[...]) + CLIP_EPS))[:1]

    @pl.loop(0, BR // STEP)
    def _(i):
        rows = pl.ds(pl.multiple_of(i * STEP, SB), STEP)
        local = b * BR + i * STEP
        here = pl.ds(pl.multiple_of(GUARD + local, SB), STEP)
        h = flat[here, :] * clip
        m = b1 * m_ref[rows, :] + c1 * h
        v = b2 * v_ref[rows, :] + c2 * (h * h)
        p = p_ref[rows, :]
        m_out[rows, :] = m
        v_out[rows, :] = v
        where = me * SROWS + local + lax.broadcasted_iota(jnp.int32, (STEP, LN), 0)
        step = (m * i1) / (jnp.sqrt(v * i2) + ADAM_EPS) + jnp.where(where < DECAY // LN, decay * p, 0.0)
        p = p - learn_rate * step
        p_out[rows, :] = p
        flat[here, :] = p

    each(True, to_tiles)

    @pl.when(b == NB - 1)
    def _():
        for i in range(PIECES_OUT):
            pl.when(made[i] == NB - 1)(functools.partial(give, i))

        @pl.loop(0, NCH)
        def _(k):
            copy(0, 0, k).wait_recv()
            copy(3, 0, k).start()
            copy(4, 0, k).start()
            copy(1, 1, k).wait_recv()
            copy(3, 1, k).start()
            copy(5, 1, k).start()
            copy(0, 1, k).wait_recv()
            copy(4, 1, k).start()
            copy(1, 0, k).wait_recv()
            copy(5, 0, k).start()

        @pl.loop(0, NCH)
        def _(k):
            for d in range(2):
                copy(3, d, k).wait_recv()
                copy(6, d, k).start()

        @pl.loop(0, NCH)
        def _(k):
            for d in range(2):
                for kind in (2, 4, 5, 6):
                    copy(kind, d, k).wait_recv()
                for kind in range(7):
                    copy(kind, d, k).wait_send()
                keep(2 * k + d).wait()


def step_and_gather(scal, g, sq, m, v, p):
    block = pl.BlockSpec((BR, LN), lambda b, *_: (b, 0))
    anywhere = pl.BlockSpec(memory_space=pltpu.HBM)
    flat_shape = jax.ShapeDtypeStruct((SROWS, LN), jnp.float32)
    turn = pltpu.VMEM((4, LN, LN), jnp.float32)
    dma = pltpu.SemaphoreType.DMA
    return pl.pallas_call(
        step_kernel,
        name="step_and_gather",
        grid_spec=pltpu.PrefetchScalarGridSpec(
            num_scalar_prefetch=1, grid=(NB,),
            in_specs=[anywhere, pl.BlockSpec((SB, LN), lambda b, *_: (0, 0)), block, block, block],
            out_specs=[block, block, block, anywhere],
            scratch_shapes=[
                pltpu.VMEM((NT, SB, LN), jnp.float32), pltpu.VMEM((NB * BR + 2 * GUARD + SB, LN), jnp.float32),
                turn, turn, pltpu.VMEM((NT, SB, LN), jnp.bfloat16),
                dma((PIECES_OUT,)), dma((PIECES_OUT,)), dma((7, 2, NCH)), dma((7, 2, NCH))]),
        out_shape=[flat_shape, flat_shape, flat_shape, jax.ShapeDtypeStruct((DEV * NT, SB, LN), jnp.bfloat16)],
        compiler_params=pltpu.CompilerParams(
            dimension_semantics=("arbitrary",), vmem_limit_bytes=63 << 20, collective_id=1, has_side_effects=True),
    )(scal, g.reshape(NT, SB, LN), sq, m, v, p)


def as_tiles(t, x):
    kind, rows, layers = TENSORS[t]
    if kind == "C":
        x = jnp.swapaxes(x, -1, -2)
    return x.reshape(layers, rows // SB, SB, BLK, LN).transpose(0, 1, 3, 2, 4)


def from_tiles(t, x, shape):
    kind, rows, layers = TENSORS[t]
    x = x.transpose(0, 1, 3, 2, 4)
    if kind == "C":
        return jnp.swapaxes(x.reshape(layers, rows, D), -1, -2)
    return x.reshape(shape)


def unpack_plan():
    copies, shared, cuts = [], [], {}
    for t, (kind, rows, layers) in enumerate(TENSORS):
        last_seen = None
        for r, (plist, _) in enumerate(PIECES):
            for pt, l, first, last, off in plist:
                if pt != t:
                    continue
                src = r * NT + off
                if (t, l) in CUT:
                    cuts.setdefault((t, l), []).append((first, last, src, r * SHARE))
                    continue
                if kind == "C":
                    copies.append([src, t, l * BLK * rows // SB, BLK * rows // SB])
                    continue
                begin = first
                if last_seen and first < last_seen[0]:
                    copies[-1][3] -= BLK
                    shared.append((t, first, last_seen[1] - BLK, src, STARTS[t] + first * SB * D, r * SHARE))
                    begin = first + 1
                copies.append([src + (begin - first) * BLK, t, begin * BLK, (last - begin) * BLK])
                last_seen = (last, src + (last - first) * BLK)
    pieces = []
    for src, t, dst, tiles in copies:
        while tiles > 0:
            n = min(tiles, UN)
            pieces.append((src, t, dst, n))
            src, dst, tiles = src + n, dst + n, tiles - n
    return pieces, shared, cuts


UN = 480
UBUF = 12


def unpack_kernel(src_ref, *refs):
    outs = refs[:len(TENSORS)]
    ring, left, right, *layers, in_sem, out_sem, pair_sem, cut_sem = refs[len(TENSORS):]
    pieces, shared, cuts = unpack_plan()

    def take(i):
        src, _, _, n = pieces[i]
        return pltpu.make_async_copy(src_ref.at[pl.ds(src, n)], ring.at[i % UBUF, pl.ds(0, n)], in_sem.at[i % UBUF])

    def give(i):
        _, t, dst, n = pieces[i]
        return pltpu.make_async_copy(ring.at[i % UBUF, pl.ds(0, n)], outs[t].at[pl.ds(dst, n)], out_sem.at[i % UBUF])

    def pair(n):
        _, _, a, b, _, _ = shared[n]
        return (pltpu.make_async_copy(src_ref.at[pl.ds(a, BLK)], left.at[n], pair_sem.at[n, 0]),
                pltpu.make_async_copy(src_ref.at[pl.ds(b, BLK)], right.at[n], pair_sem.at[n, 1]))

    def cut_loads(n):
        (t, _), sides = list(cuts.items())[n]
        c8 = TENSORS[t][1] // SB
        made = []
        for side, (first, last, src, _) in enumerate(sides):
            for j in range(first, last):
                over = side == 1 and first < sides[0][1] and j == first
                to = right.at[len(shared) + n, pl.ds(0, c8)] if over else layers[n].at[pl.ds(0, c8), j]
                made.append(pltpu.make_async_copy(
                    src_ref.at[pl.ds(src + (j - first) * c8, c8)], to, cut_sem.at[n, BLK if over else j]))
        return made

    def cut_stores(n):
        (t, l), _ = list(cuts.items())[n]
        c8 = TENSORS[t][1] // SB
        return [pltpu.make_async_copy(layers[n].at[c], outs[t].at[pl.ds((l * c8 + c) * BLK, BLK)], cut_sem.at[n, c])
                for c in range(c8)]

    def spot(start, row_step, lane_step, tile_step, tiles):
        shape = (tiles, SB, LN)
        return (start + tile_step * lax.broadcasted_iota(jnp.int32, shape, 0)
                + row_step * lax.broadcasted_iota(jnp.int32, shape, 1)
                + lane_step * lax.broadcasted_iota(jnp.int32, shape, 2))

    for n in range(len(shared)):
        for c in pair(n):
            c.start()
    for n in range(len(cuts)):
        for c in cut_loads(n):
            c.start()
    depth = UBUF // 2
    for i in range(depth):
        take(i).start()
    for i in range(len(pieces)):
        if i + depth < len(pieces):
            if i + depth >= UBUF:
                give(i + depth - UBUF).wait()
            take(i + depth).start()
        take(i).wait()
        give(i).start()
        if i == depth:
            for n, (t, _, _, _, start, bound) in enumerate(shared):
                for c in pair(n):
                    c.wait()
                keep = spot(start, D, 1, LN, BLK) < bound
                left[n] = jnp.where(keep, left[n].astype(jnp.float32), right[n].astype(jnp.float32)).astype(jnp.bfloat16)
            for n, ((t, l), sides) in enumerate(cuts.items()):
                for c in cut_loads(n):
                    c.wait()
                rows = TENSORS[t][1]
                j, bound = sides[1][0], sides[1][3]
                if j < sides[0][1]:
                    keep = spot(STARTS[t] + (l * D + j * LN) * rows, 1, rows, SB, rows // SB) < bound
                    one = right[len(shared) + n, pl.ds(0, rows // SB)].astype(jnp.float32)
                    here = pl.ds(0, rows // SB)
                    layers[n][here, j] = jnp.where(keep, layers[n][here, j].astype(jnp.float32), one).astype(jnp.bfloat16)
        if i == depth + 2:
            for n, (t, g, _, _, _, _) in enumerate(shared):
                pltpu.make_async_copy(left.at[n], outs[t].at[pl.ds(g * BLK, BLK)], pair_sem.at[n, 0]).start()
            for n in range(len(cuts)):
                for c in cut_stores(n):
                    c.start()
    for i in range(max(0, len(pieces) - UBUF), len(pieces)):
        give(i).wait()
    for n, (t, g, _, _, _, _) in enumerate(shared):
        pltpu.make_async_copy(left.at[n], outs[t].at[pl.ds(g * BLK, BLK)], pair_sem.at[n, 0]).wait()
    for n in range(len(cuts)):
        for c in cut_stores(n):
            c.wait()


def unpack(gathered, shapes):
    pieces, shared, cuts = unpack_plan()
    anywhere = pl.BlockSpec(memory_space=pltpu.HBM)
    tiles = pl.pallas_call(
        unpack_kernel,
        name="unpack",
        out_shape=[jax.ShapeDtypeStruct((size // 1024, SB, LN), jnp.bfloat16) for size in SIZES],
        in_specs=[anywhere], out_specs=[anywhere] * len(TENSORS),
        scratch_shapes=[
            pltpu.VMEM((UBUF, UN, SB, LN), jnp.bfloat16), pltpu.VMEM((len(shared) + 1, BLK, SB, LN), jnp.bfloat16),
            pltpu.VMEM((len(shared) + len(cuts) + 1, BLK, SB, LN), jnp.bfloat16),
            *[pltpu.VMEM((TENSORS[t][1] // SB + 1, BLK, SB, LN), jnp.bfloat16) for t, _ in cuts],
            pltpu.SemaphoreType.DMA((UBUF,)), pltpu.SemaphoreType.DMA((UBUF,)),
            pltpu.SemaphoreType.DMA((len(shared), 2)), pltpu.SemaphoreType.DMA((len(cuts), BLK + 1))],
        compiler_params=pltpu.CompilerParams(vmem_limit_bytes=48 << 20),
    )(gathered.reshape(DEV * NT, SB, LN))
    outs = [from_tiles(t, x.reshape(TENSORS[t][2], TENSORS[t][1] // SB, BLK, SB, LN), shapes[t])
            for t, x in enumerate(tiles)]
    plist, _ = PIECES[DEV - 1]
    base = ((DEV - 1) * NT + plist[-1][4]) * SB
    tail = gathered[base:base + TAIL // LN].reshape(-1)
    cut = math.prod(shapes[SB])
    return outs + [tail[:cut].reshape(shapes[SB]), tail[cut:].reshape(shapes[9])]


def sources(grads):
    views = [as_tiles(t, grads[t][0]) for t in range(len(TENSORS))]
    tail = jnp.concatenate([grads[SB].reshape(-1), grads[9].reshape(-1), jnp.zeros((-TAIL % 2048,), jnp.bfloat16)])
    turned = []
    for t, l in CUT:
        layer = jnp.swapaxes(lax.optimization_barrier(grads[t][:, l]), 1, 2)
        turned.append(layer.reshape(-1, SB, BLK, LN).transpose(2, 0, 1, 3))
    return [x.reshape(-1, LN) for x in views + [tail] + turned]


def solution(mesh):
    def local_update(*arrays):
        grads = arrays[:10]
        m, v, p, hyper = arrays[10:]
        shapes = [x.shape[1:] for x in grads]
        share, squares, _ = reduce_scatter(sources(grads))
        learn_rate, b1, b2, decay, max_norm = [hyper[i] for i in range(5)]
        scal = jnp.stack([learn_rate, b1, 1.0 - b1, b2, 1.0 - b2, 1.0 / (1.0 - b1 ** ADAM_STEP),
                          1.0 / (1.0 - b2 ** ADAM_STEP), decay, max_norm])
        m, v, p, gathered = step_and_gather(scal, share, squares, *[x.reshape(SROWS, LN) for x in (m, v, p)])
        params = unpack(gathered.reshape(DEV * NR, LN), shapes)
        return tuple(params) + tuple(x.reshape(SHARE) for x in (m, v, p))

    in_specs = tuple([P("dp")] * 10 + [P("dp"), P("dp"), P("dp"), P()])
    out_specs = tuple([P()] * 10 + [P("dp"), P("dp"), P("dp")])
    return jax.shard_map(local_update, mesh=mesh, in_specs=in_specs, out_specs=out_specs, check_vma=False)
```

```python
import functools
import math

import jax
import jax.numpy as jnp
import numpy as np
from jax import lax
from jax.experimental import pallas as pl
from jax.experimental.pallas import tpu as pltpu
from jax.sharding import PartitionSpec as P

ADAM_STEP = 7
LN = 128
SB = 8
ADAM_EPS = 1e-8
CLIP_EPS = 1e-6
D = 3840
BLK = D // LN
LAYERS = 6
DEV = 8
TENSORS = (("R", 4096, 1), ("C", 64, LAYERS), ("C", 32, LAYERS), ("C", 32, LAYERS), ("R", 64 * LAYERS, 1),
           ("C", 240, LAYERS), ("C", 240, LAYERS), ("R", 240 * LAYERS, 1))
SIZES = tuple(rows * layers * D for _, rows, layers in TENSORS)
STARTS = tuple(sum(SIZES[:i]) for i in range(len(SIZES)))
DECAY = sum(SIZES)
TAIL = LAYERS * 4 * D + LAYERS * 2 * 256
TOTAL = DECAY + TAIL
SHARE = TOTAL // DEV
SROWS = SHARE // LN
NT = 4536
NR = NT * SB
GUARD = 240
NCH = 9
CR = NR // 2 // NCH
MESH = pl.DeviceIdType.MESH


def plan():
    pieces, units = [], []
    for r in range(DEV):
        lo, hi = r * SHARE, (r + 1) * SHARE
        off, plist, ulist = 0, [], []
        for t, (kind, rows, layers) in enumerate(TENSORS):
            if kind == "R":
                a, b = max(lo, STARTS[t]), min(hi, STARTS[t] + SIZES[t])
                if a >= b:
                    continue
                g0, g1 = (a - STARTS[t]) // (SB * D), -((STARTS[t] - b) // (SB * D))
                plist.append((t, 0, g0, g1, off))
                for g in range(g0, g1):
                    ulist.append(("R", off + (g - g0) * BLK, 1, (STARTS[t] + g * SB * D - lo) // LN))
                off += (g1 - g0) * BLK
                continue
            for l in range(layers):
                s = STARTS[t] + l * rows * D
                a, b = max(lo, s), min(hi, s + rows * D)
                if a >= b:
                    continue
                j0, j1 = (a - s) // (LN * rows), -((s - b) // (LN * rows))
                plist.append((t, l, j0, j1, off))
                whole = j1 - j0 == BLK
                for j in range(j0, j1):
                    at, stride = (j, BLK) if whole else ((j - j0) * (rows // SB), 1)
                    ulist.append((rows, off + at, stride, (s + j * LN * rows - lo) // LN))
                off += (j1 - j0) * rows // SB
        if hi > DECAY:
            for i in range(TAIL // 1024):
                ulist.append(("T", off + i, 1, (DECAY - lo) // LN + SB * i))
            plist.append((len(TENSORS), 0, 0, TAIL // 1024, off))
            off += TAIL // 1024
        assert off <= NT
        pieces.append((plist, off))
        units.append(ulist)
    return pieces, units


PIECES, UNITS = plan()


def flip(dev, bit):
    return dev + bit - 2 * bit * (lax.rem(lax.div(dev, bit), 2))


def barrier_all(me):
    sem = pltpu.get_barrier_semaphore()
    for step in range(1, DEV):
        pl.semaphore_signal(sem, inc=1, device_id=(lax.rem(me + step, DEV),), device_id_type=MESH)
    pl.semaphore_wait(sem, DEV - 1)


def cut_layers():
    return sorted({(t, l) for plist, _ in PIECES for t, l, a, b, _ in plist
                   if t < len(TENSORS) and TENSORS[t][0] == "C" and b - a < BLK})


CUT = cut_layers()


def segments():
    found = []
    for plist, used in PIECES:
        runs = []
        for t, l, first, last, off in plist:
            if t == len(TENSORS):
                src, row, rows = t, 0, -(-last // 2) * 16
            elif TENSORS[t][0] == "R":
                src, row, rows = t, first * BLK * SB, (last - first) * BLK * SB
            elif (t, l) in CUT:
                c = TENSORS[t][1]
                src, row, rows = len(TENSORS) + 1 + CUT.index((t, l)), first * c, (last - first) * c
            else:
                src, row, rows = t, l * BLK * TENSORS[t][1], BLK * TENSORS[t][1]
            if runs and runs[-1][0] == src and runs[-1][1] + runs[-1][3] == row:
                runs[-1][3] += rows
            else:
                runs.append([src, row, off * SB, rows])
        end = runs[-1][2] + runs[-1][3]
        if end < NR:
            runs.append([0, 0, end, NR - end])
        halves = ([], [])
        for src, row, dst, rows in runs:
            while rows > 0:
                n = min(rows, CR - dst % CR)
                d, k = divmod(dst // CR, NCH)
                last = halves[d][-1] if halves[d] else None
                if last and n == CR and last[0] == src and last[4] == CR and last[1] + last[5] * CR == row:
                    last[5] += 1
                else:
                    halves[d].append([src, row, k, dst - d * (NR // 2), n, 1])
                row, dst, rows = row + n, dst + n, rows - n
        found.append(halves)
    return found


def rs_kernel(*refs):
    count = len(TENSORS) + 1 + len(CUT)
    srcs, (g_ref, sq_ref, r_ref, part, land, loads, outs, accum, sq_all,
           send1, recv1, send2, recv2, load_sem, out_sem, sq_send, sq_recv) = refs[:count], refs[count:]
    me = lax.axis_index("dp")
    barrier_all(me)
    half = NR // 2
    segs = segments()

    def bits(d):
        return 2 + 2 * d, 4 - 2 * d

    def landing(d, q, slot, row, rows):
        return r_ref.at[pl.ds(pl.multiple_of(((d * 2 + q) * 3 + slot) * half + row, 16), rows)]

    def hop(d, q, slot, k):
        here = landing(d, q, slot, k * CR, CR)
        return pltpu.make_async_remote_copy(
            src_ref=here, dst_ref=here, send_sem=send1.at[d, q, slot, k], recv_sem=recv1.at[d, q, slot, k],
            device_id=(flip(me, 1),), device_id_type=MESH)

    def pass_on(d, k):
        rows = pl.ds(pl.multiple_of(d * half + k * CR, 16), CR)
        return pltpu.make_async_remote_copy(
            src_ref=part.at[rows], dst_ref=land.at[rows], send_sem=send2.at[d, k], recv_sem=recv2.at[d, k],
            device_id=(flip(me, bits(d)[1]),), device_id_type=MESH)

    @pl.loop(0, 12)
    def _(h):
        q, turn, d = lax.div(h, 6), lax.rem(lax.div(h, 2), 3), lax.rem(h, 2)
        slot = lax.rem(turn + 1, 3)
        first, second = bits(d)
        away = flip(me, first)
        target = jnp.where(slot == 0, flip(me, 1), jnp.where(slot == 1, away, flip(away, 1)))
        owner = jnp.where(q == 0, flip(target, second), target)
        for r in range(DEV):
            for dd in range(2):
                @pl.when((owner == r) & (d == dd))
                def _():
                    for src, row, k0, dst, rows, chunks in segs[r][dd]:
                        def send(i, carry, src=src, row=row, k0=k0, dst=dst, rows=rows):
                            pltpu.make_async_remote_copy(
                                src_ref=srcs[src].at[pl.ds(pl.multiple_of(row + i * CR, SB), rows)],
                                dst_ref=r_ref.at[pl.ds(pl.multiple_of(
                                    ((d * 2 + q) * 3 + slot) * half + dst + i * CR, SB), rows)],
                                send_sem=send1.at[d, q, slot, k0 + i], recv_sem=recv1.at[d, q, slot, k0 + i],
                                device_id=(target,), device_id_type=MESH).start()
                            return carry
                        if chunks == 1:
                            send(0, 0)
                        else:
                            lax.fori_loop(0, chunks, send, 0)

    def load(d, q, slot, k):
        return pltpu.make_async_copy(landing(d, q, slot % 3, k * CR, CR), loads.at[d, slot], load_sem.at[d, slot])

    def load_own(d, q, k):
        owner = flip(me, bits(d)[1]) if q == 0 else me
        for r in range(DEV):
            @pl.when(owner == r)
            def _(r=r):
                for src, row, k0, dst, rows, chunks in segs[r][d]:
                    inside = (k >= k0) & (k < k0 + chunks)
                    at = row if chunks == 1 else pl.multiple_of(row + jnp.where(inside, k - k0, 0) * CR, SB)

                    @pl.when(inside)
                    def _(src=src, at=at, dst=dst, rows=rows):
                        pltpu.make_async_copy(
                            srcs[src].at[pl.ds(at, rows)],
                            loads.at[d, 3, pl.ds(dst % CR, rows)], load_sem.at[d, 3]).start()

    def fetch(d, q, k):
        load_own(d, q, k)
        for slot in range(3):
            hop(d, q, slot, k).wait_recv()
            load(d, q, slot, k).start()

    def ready(d, q, k):
        for slot in range(4):
            load(d, q, slot, k).wait()

    def total(d, rows):
        acc = loads[d, 3, rows, :].astype(jnp.float32)
        for slot in range(3):
            acc = acc + loads[d, slot, rows, :].astype(jnp.float32)
        return acc

    STEP = 112
    accum[...] = jnp.zeros_like(accum)
    used = functools.reduce(lambda acc, r: jnp.where(me == r, PIECES[r][1], acc), range(DEV), 0)

    def out_copy(d, k):
        return pltpu.make_async_copy(
            outs.at[d], g_ref.at[pl.ds(pl.multiple_of(d * half + k * CR, 16), CR)], out_sem.at[d])

    for d in range(2):
        fetch(d, 0, jnp.int32(0))

    @pl.loop(0, NCH)
    def _(k):
        for d in range(2):
            ready(d, 0, k)

            @pl.loop(0, CR // STEP)
            def _(i):
                rows = pl.ds(pl.multiple_of(i * STEP, 16), STEP)
                part[pl.ds(pl.multiple_of(d * half + k * CR + i * STEP, SB), STEP), :] = total(d, rows)

            @pl.when(k + 1 < NCH)
            def _():
                fetch(d, 0, k + 1)

            pass_on(d, k).start()

    for d in range(2):
        fetch(d, 1, jnp.int32(0))

    @pl.loop(0, NCH)
    def _(k):
        for d in range(2):
            ready(d, 1, k)
            pass_on(d, k).wait_recv()

            @pl.when(k > 0)
            def _():
                out_copy(d, k - 1).wait()

            @pl.loop(0, CR // STEP)
            def _(i):
                base = pl.multiple_of(d * half + k * CR + i * STEP, SB)
                rows = pl.ds(pl.multiple_of(i * STEP, 16), STEP)
                g = (total(d, rows) + land[pl.ds(base, STEP), :]) * (1.0 / DEV)
                outs[d, rows, :] = g
                tile = lax.div(base, SB) + lax.broadcasted_iota(jnp.int32, (STEP // SB, SB, LN), 0)
                g3 = g.reshape(STEP // SB, SB, LN)
                keep = counted(me, tile) & (tile < used)
                accum[...] += jnp.sum(jnp.where(keep, g3 * g3, 0.0), axis=0)

            @pl.when(k + 1 < NCH)
            def _():
                fetch(d, 1, k + 1)

            out_copy(d, k).start()

    sq_all[pl.ds(pl.multiple_of(me * SB, SB), SB), :] = accum[...]
    for d in range(2):
        out_copy(d, NCH - 1).wait()
    for d in range(2):
        @pl.loop(0, NCH)
        def _(k):
            for q in range(2):
                for slot in range(3):
                    hop(d, q, slot, k).wait_send()
            pass_on(d, k).wait_send()

    def tell(step):
        return pltpu.make_async_remote_copy(
            src_ref=accum, dst_ref=sq_all.at[pl.ds(pl.multiple_of(me * SB, SB), SB)],
            send_sem=sq_send.at[step], recv_sem=sq_recv.at[step],
            device_id=(lax.rem(me + step + 1, DEV),), device_id_type=MESH)

    for step in range(DEV - 1):
        tell(step).start()
    for step in range(DEV - 1):
        tell(step).wait()
    whole = sq_all[pl.ds(0, SB), :]
    for i in range(1, DEV):
        whole = whole + sq_all[pl.ds(SB * i, SB), :]
    sq_ref[...] = jnp.broadcast_to(jnp.sum(whole, keepdims=True), (SB, LN))


def shared_first():
    found = []
    for r in range(1, DEV):
        kind, tile, stride, row = UNITS[r][0]
        if row >= 0:
            continue
        found.append((r, BLK if kind == "R" else kind // SB))
    return found


def counted(me, tile):
    first = functools.reduce(lambda acc, x: jnp.where(me == x[0], x[1], acc), shared_first(), 0)
    return tile >= first


def reduce_scatter(sources):
    half = NR // 2
    return pl.pallas_call(
        rs_kernel,
        name="reduce_scatter",
        out_shape=(jax.ShapeDtypeStruct((NR, LN), jnp.float32), jax.ShapeDtypeStruct((SB, LN), jnp.float32),
                   jax.ShapeDtypeStruct((12 * half, LN), jnp.bfloat16)),
        in_specs=[pl.BlockSpec(memory_space=pltpu.HBM)] * len(sources),
        out_specs=(pl.BlockSpec(memory_space=pltpu.HBM), pl.BlockSpec(memory_space=pltpu.VMEM),
                   pl.BlockSpec(memory_space=pltpu.HBM)),
        scratch_shapes=[
            pltpu.VMEM((NR, LN), jnp.float32), pltpu.VMEM((NR, LN), jnp.float32),
            pltpu.VMEM((2, 4, CR, LN), jnp.bfloat16), pltpu.VMEM((2, CR, LN), jnp.float32),
            pltpu.VMEM((SB, LN), jnp.float32), pltpu.VMEM((SB * DEV, LN), jnp.float32),
            pltpu.SemaphoreType.DMA((2, 2, 3, NCH)), pltpu.SemaphoreType.DMA((2, 2, 3, NCH)),
            pltpu.SemaphoreType.DMA((2, NCH)), pltpu.SemaphoreType.DMA((2, NCH)),
            pltpu.SemaphoreType.DMA((2, 4)), pltpu.SemaphoreType.DMA((2,)),
            pltpu.SemaphoreType.DMA((DEV - 1,)), pltpu.SemaphoreType.DMA((DEV - 1,))],
        compiler_params=pltpu.CompilerParams(collective_id=0, has_side_effects=True, vmem_limit_bytes=60 << 20),
    )(*sources)


BR = 1152
NB = -(-SROWS // BR)
STEP = 96
KINDS = {"R": 1, 240: 3, 64: SB, 32: 16, "T": 1}
ACH = 18
PIECES_OUT = 2 * ACH
PT = NT // PIECES_OUT


def unit_runs():
    runs = {kind: [] for kind in KINDS}
    need = np.full((PIECES_OUT, DEV), NB - 1)
    made = np.zeros((PIECES_OUT, DEV), int)
    for r, ulist in enumerate(UNITS):
        for kind in KINDS:
            mine = [u for u in ulist if u[0] == kind]
            size, count = UNIT_SIZE[kind]
            found = []
            for i, (_, tile, stride, row) in enumerate(mine):
                first = max(0, row // BR)
                last = min(NB - 1, (row + size - 1) // BR)
                for piece in {(tile + c * stride) // PT for c in range(count)}:
                    need[piece, r] = min(need[piece, r], first)
                    made[piece, r] = max(made[piece, r], last)
                per = 1 if stride == BLK else count
                if not found or stride != found[-1][-1] or row + GUARD != found[-1][2] + found[-1][0] * size:
                    found.append([0, tile, row + GUARD, BLK * count, per, stride])
                n, start, _, step, per, _ = found[-1]
                assert tile == start + n // BLK * step + n % BLK * per
                found[-1][0] += 1
            for slot, run in enumerate(found):
                if slot == len(runs[kind]):
                    runs[kind].append(np.zeros((6, DEV), int))
                runs[kind][slot][:, r] = run
    for i in range(PIECES_OUT):
        need[i] = need[i:].min(axis=0)
        made[i] = made[:i + 1].max(axis=0)
    return runs, need, made


UNIT_SIZE = {"R": (GUARD, BLK), 240: (240, BLK), 64: (64, SB), 32: (32, 4), "T": (SB, 1)}
RUNS, NEED, MADE = unit_runs()


def by_owner(me, values):
    out = int(values[0])
    for r in range(1, DEV):
        if int(values[r]) != int(values[r - 1]):
            out = jnp.where(me >= r, int(values[r]), out)
    return out


def lanes(rows):
    return lax.broadcasted_iota(jnp.int32, (rows, LN), 1)


def roll(x, shift):
    shift = shift % LN
    return x if shift == 0 else pltpu.roll(x, shift, 1)


def swap_blocks(xs, width):
    per = len(xs)
    lane = lanes(xs[0].shape[0])

    def pick(choose):
        out = choose(0)
        for b in range(1, per):
            out = jnp.where(lane >= b * width, choose(b), out)
        return out

    turned = [roll(pick(lambda b: xs[(b + t) % per]), t * width) for t in range(per)]
    return [pick(lambda b: turned[(b - j) % per]) for j in range(per)]


def to_flat(kind, units, tiles, flat, low, ta, tb):
    del low
    if kind == "T" or kind == "R":
        for base, _, row in units:
            if kind == "T":
                flat[pl.ds(row, SB), :] = tiles[base]
            else:
                for c in range(BLK):
                    flat[pl.ds(row + c, SB, stride=BLK), :] = tiles[base + c]
        return
    if kind < LN:
        per = LN // kind
        sets = [units[i:i + per] for i in range(0, len(units), per)]
        for n, some in enumerate(sets):
            ta[n] = jnp.concatenate([tiles[base + i * stride] for base, stride, _ in some for i in range(kind // SB)]).T
        for n, some in enumerate(sets):
            for unit, x in zip(some, swap_blocks([ta[n, pl.ds(q, kind, stride=per), :] for q in range(per)], kind)):
                flat[pl.ds(unit[-1], kind), :] = x
        return
    for n, (base, stride, row) in enumerate(units):
        ta[n] = jnp.concatenate([tiles[base + i * stride] for i in range(16)]).T
        tb[n] = jnp.concatenate([tiles[base + i * stride] for i in range(16, BLK)] + [jnp.zeros((16, LN))]).T
    lane = lanes(16)
    for k in range(15):
        r, o = divmod(LN * k, kind)
        for n, (_, _, row) in enumerate(units):
            x = (ta if o < LN else tb)[n, pl.ds(r, 16, stride=SB), :]
            if 0 < o < LN:
                x = jnp.where(lane >= o, x, tb[n, pl.ds(r, 16, stride=SB), :])
            x = roll(x, -o)
            if o + LN > kind:
                x = jnp.where(lane >= kind - o, roll(ta[n, pl.ds(r + 1, 16, stride=SB), :], kind - o), x)
            flat[pl.ds(row + k, 16, stride=15), :] = x


def to_tiles(kind, units, tiles, flat, low, ta, tb):
    del tiles

    def put(at, value):
        low[at] = value.astype(jnp.bfloat16)

    if kind == "T" or kind == "R":
        for base, _, row in units:
            if kind == "T":
                put(base, flat[pl.ds(row, SB), :])
            else:
                for c in range(BLK):
                    put(base + c, flat[pl.ds(row + c, SB, stride=BLK), :])
        return
    if kind < LN:
        per = LN // kind
        sets = [units[i:i + per] for i in range(0, len(units), per)]
        for n, some in enumerate(sets):
            for q, x in enumerate(swap_blocks([flat[pl.ds(row, kind), :] for _, _, row in some], kind)):
                ta[n, pl.ds(q, kind, stride=per), :] = x
        for n, some in enumerate(sets):
            grid = ta[n].T.reshape(16, SB, LN)
            for u, (base, stride, _) in enumerate(some):
                for i in range(kind // SB):
                    put(base + i * stride, grid[u * (kind // SB) + i])
        return
    lane = lanes(16)
    for r in range(SB):
        k, o = divmod(kind * r, LN)
        for n, (_, _, row) in enumerate(units):
            f = [flat[pl.ds(row + k + i, 16, stride=15), :] for i in range(3 if k + 2 < 15 else 2)]
            ta[n, pl.ds(r, 16, stride=SB), :] = f[0] if o == 0 else roll(jnp.where(lane >= o, f[0], f[1]), -o)
            tb[n, pl.ds(r, 16, stride=SB), :] = f[1] if o == 0 else roll(jnp.where(lane >= o, f[1], f[-1]), -o)
    for n, (base, stride, _) in enumerate(units):
        grid = jnp.concatenate([ta[n].T, tb[n].T]).reshape(32, SB, LN)
        for i in range(BLK):
            put(base + i * stride, grid[i])


def step_kernel(scal, g_ref, sq_ref, m_ref, v_ref, p_ref, m_out, v_out, p_out, a_ref,
                tiles, flat, ta, tb, low, g_sem, a_sem, send, recv):
    me = lax.axis_index("dp")
    b = pl.program_id(0)
    xn, yn, pn = flip(me, 2), flip(me, 4), flip(me, 1)
    diag = flip(xn, 4)

    def take(i):
        here = pl.ds(i * PT, PT)
        return pltpu.make_async_copy(g_ref.at[here], tiles.at[here], g_sem.at[i])

    def keep(i):
        return pltpu.make_async_copy(low.at[pl.ds(i * PT, PT)], a_ref.at[pl.ds(me * NT + i * PT, PT)], a_sem.at[i])

    def copy(kind, d, k):
        owner = (me, me, me, xn if d == 0 else yn, xn, yn, diag)[kind]
        target = (xn, yn, pn, yn if d == 0 else xn, pn, pn, pn)[kind]
        at = (2 * k + d) * PT
        there = a_ref.at[pl.ds(owner * NT + at, PT)]
        return pltpu.make_async_remote_copy(
            src_ref=low.at[pl.ds(at, PT)] if kind < 3 else there, dst_ref=there,
            send_sem=send.at[kind, d, k], recv_sem=recv.at[kind, d, k],
            device_id=(target,), device_id_type=MESH)

    def give(i):
        for kind in range(3):
            copy(kind, i % 2, i // 2).start()
        keep(i).start()

    @pl.when(b == 0)
    def _():
        barrier_all(me)

    for i in range(PIECES_OUT):
        pl.when(b == by_owner(me, np.maximum(NEED[i] - 3, 0)))(lambda i=i: take(i).start())
    made = [by_owner(me, MADE[i]) for i in range(PIECES_OUT)]
    for i in range(PIECES_OUT):
        pl.when(b == made[i] + 1)(functools.partial(give, i))
    for i in range(PIECES_OUT):
        pl.when(b == by_owner(me, NEED[i]))(lambda i=i: take(i).wait())

    def upto(block, count, row, size, whole):
        room = (block + 1) * BR + GUARD - row
        n = lax.div(jnp.where(room > 0, room, 0) + (0 if whole else size - 1), size)
        return jnp.where(n < count, n, count)

    def each(whole, work):
        for kind, group in KINDS.items():
            size = UNIT_SIZE[kind][0]
            for run in RUNS[kind]:
                count, start, row, step, per, stride = [by_owner(me, x) for x in run]
                first = jnp.where(b > 0, upto(b - 1, count, row, size, whole), 0)
                last = upto(b, count, row, size, whole)
                if whole:
                    last = jnp.where(b < NB - 1, last, count)

                @pl.loop(0, lax.div(last - first + group - 1, group))
                def _(t):
                    units = []
                    for x in range(group):
                        i = first + t * group + x
                        i = jnp.where(i < last, i, last - 1)
                        units.append((start + lax.div(i, BLK) * step + lax.rem(i, BLK) * per, stride, row + i * size))
                    work(kind, units, tiles, flat, low, ta, tb)

    each(False, to_flat)

    learn_rate, b1, b2, decay, max_norm = [scal[i] for i in range(5)]
    c1, c2 = 1.0 - b1, 1.0 - b2

    def correction(beta):
        return 1.0 / (1.0 - jnp.full((1, LN), beta) ** ADAM_STEP)

    i1, i2 = correction(b1), correction(b2)
    clip = jnp.minimum(1.0, max_norm / (jnp.sqrt(sq_ref[...]) + CLIP_EPS))[:1]

    @pl.loop(0, BR // STEP)
    def _(i):
        rows = pl.ds(pl.multiple_of(i * STEP, SB), STEP)
        local = b * BR + i * STEP
        here = pl.ds(pl.multiple_of(GUARD + local, SB), STEP)
        h = flat[here, :] * clip
        m = b1 * m_ref[rows, :] + c1 * h
        v = b2 * v_ref[rows, :] + c2 * (h * h)
        p = p_ref[rows, :]
        m_out[rows, :] = m
        v_out[rows, :] = v
        where = me * SROWS + local + lax.broadcasted_iota(jnp.int32, (STEP, LN), 0)
        step = (m * i1) / (jnp.sqrt(v * i2) + ADAM_EPS) + jnp.where(where < DECAY // LN, decay * p, 0.0)
        p = p - learn_rate * step
        p_out[rows, :] = p
        flat[here, :] = p

    each(True, to_tiles)

    @pl.when(b == NB - 1)
    def _():
        for i in range(PIECES_OUT):
            pl.when(made[i] == NB - 1)(functools.partial(give, i))

        @pl.loop(0, ACH)
        def _(k):
            copy(0, 0, k).wait_recv()
            copy(3, 0, k).start()
            copy(4, 0, k).start()
            copy(1, 1, k).wait_recv()
            copy(3, 1, k).start()
            copy(5, 1, k).start()
            copy(0, 1, k).wait_recv()
            copy(4, 1, k).start()
            copy(1, 0, k).wait_recv()
            copy(5, 0, k).start()

        @pl.loop(0, ACH)
        def _(k):
            for d in range(2):
                copy(3, d, k).wait_recv()
                copy(6, d, k).start()

        @pl.loop(0, ACH)
        def _(k):
            for d in range(2):
                for kind in (2, 4, 5, 6):
                    copy(kind, d, k).wait_recv()
                for kind in range(7):
                    copy(kind, d, k).wait_send()
                keep(2 * k + d).wait()


def step_and_gather(scal, g, sq, m, v, p):
    block = pl.BlockSpec((BR, LN), lambda b, *_: (b, 0))
    anywhere = pl.BlockSpec(memory_space=pltpu.HBM)
    flat_shape = jax.ShapeDtypeStruct((SROWS, LN), jnp.float32)
    turn = pltpu.VMEM((4, LN, LN), jnp.float32)
    dma = pltpu.SemaphoreType.DMA
    return pl.pallas_call(
        step_kernel,
        name="step_and_gather",
        grid_spec=pltpu.PrefetchScalarGridSpec(
            num_scalar_prefetch=1, grid=(NB,),
            in_specs=[anywhere, pl.BlockSpec((SB, LN), lambda b, *_: (0, 0)), block, block, block],
            out_specs=[block, block, block, anywhere],
            scratch_shapes=[
                pltpu.VMEM((NT, SB, LN), jnp.float32), pltpu.VMEM((NB * BR + 2 * GUARD + SB, LN), jnp.float32),
                turn, turn, pltpu.VMEM((NT, SB, LN), jnp.bfloat16),
                dma((PIECES_OUT,)), dma((PIECES_OUT,)), dma((7, 2, ACH)), dma((7, 2, ACH))]),
        out_shape=[flat_shape, flat_shape, flat_shape, jax.ShapeDtypeStruct((DEV * NT, SB, LN), jnp.bfloat16)],
        compiler_params=pltpu.CompilerParams(
            dimension_semantics=("arbitrary",), vmem_limit_bytes=63 << 20, collective_id=1, has_side_effects=True),
    )(scal, g.reshape(NT, SB, LN), sq, m, v, p)


def as_tiles(t, x):
    kind, rows, layers = TENSORS[t]
    if kind == "C":
        x = jnp.swapaxes(x, -1, -2)
    return x.reshape(layers, rows // SB, SB, BLK, LN).transpose(0, 1, 3, 2, 4)


def from_tiles(t, x, shape):
    kind, rows, layers = TENSORS[t]
    x = x.transpose(0, 1, 3, 2, 4)
    if kind == "C":
        return jnp.swapaxes(x.reshape(layers, rows, D), -1, -2)
    return x.reshape(shape)


def unpack_plan():
    copies, shared, cuts = [], [], {}
    for t, (kind, rows, layers) in enumerate(TENSORS):
        last_seen = None
        for r, (plist, _) in enumerate(PIECES):
            for pt, l, first, last, off in plist:
                if pt != t:
                    continue
                src = r * NT + off
                if (t, l) in CUT:
                    cuts.setdefault((t, l), []).append((first, last, src, r * SHARE))
                    continue
                if kind == "C":
                    copies.append([src, t, l * BLK * rows // SB, BLK * rows // SB])
                    continue
                begin = first
                if last_seen and first < last_seen[0]:
                    copies[-1][3] -= BLK
                    shared.append((t, first, last_seen[1] - BLK, src, STARTS[t] + first * SB * D, r * SHARE))
                    begin = first + 1
                copies.append([src + (begin - first) * BLK, t, begin * BLK, (last - begin) * BLK])
                last_seen = (last, src + (last - first) * BLK)
    pieces = []
    for src, t, dst, tiles in copies:
        while tiles > 0:
            n = min(tiles, UN)
            pieces.append((src, t, dst, n))
            src, dst, tiles = src + n, dst + n, tiles - n
    return pieces, shared, cuts


UN = 480
UBUF = 12


def unpack_kernel(src_ref, *refs):
    outs = refs[:len(TENSORS)]
    ring, left, right, *layers, in_sem, out_sem, pair_sem, cut_sem = refs[len(TENSORS):]
    pieces, shared, cuts = unpack_plan()

    def take(i):
        src, _, _, n = pieces[i]
        return pltpu.make_async_copy(src_ref.at[pl.ds(src, n)], ring.at[i % UBUF, pl.ds(0, n)], in_sem.at[i % UBUF])

    def give(i):
        _, t, dst, n = pieces[i]
        return pltpu.make_async_copy(ring.at[i % UBUF, pl.ds(0, n)], outs[t].at[pl.ds(dst, n)], out_sem.at[i % UBUF])

    def pair(n):
        _, _, a, b, _, _ = shared[n]
        return (pltpu.make_async_copy(src_ref.at[pl.ds(a, BLK)], left.at[n], pair_sem.at[n, 0]),
                pltpu.make_async_copy(src_ref.at[pl.ds(b, BLK)], right.at[n], pair_sem.at[n, 1]))

    def cut_loads(n):
        (t, _), sides = list(cuts.items())[n]
        c8 = TENSORS[t][1] // SB
        made = []
        for side, (first, last, src, _) in enumerate(sides):
            for j in range(first, last):
                over = side == 1 and first < sides[0][1] and j == first
                to = right.at[len(shared) + n, pl.ds(0, c8)] if over else layers[n].at[pl.ds(0, c8), j]
                made.append(pltpu.make_async_copy(
                    src_ref.at[pl.ds(src + (j - first) * c8, c8)], to, cut_sem.at[n, BLK if over else j]))
        return made

    def cut_stores(n):
        (t, l), _ = list(cuts.items())[n]
        c8 = TENSORS[t][1] // SB
        return [pltpu.make_async_copy(layers[n].at[c], outs[t].at[pl.ds((l * c8 + c) * BLK, BLK)], cut_sem.at[n, c])
                for c in range(c8)]

    def spot(start, row_step, lane_step, tile_step, tiles):
        shape = (tiles, SB, LN)
        return (start + tile_step * lax.broadcasted_iota(jnp.int32, shape, 0)
                + row_step * lax.broadcasted_iota(jnp.int32, shape, 1)
                + lane_step * lax.broadcasted_iota(jnp.int32, shape, 2))

    for n in range(len(shared)):
        for c in pair(n):
            c.start()
    for n in range(len(cuts)):
        for c in cut_loads(n):
            c.start()
    depth = UBUF // 2
    for i in range(depth):
        take(i).start()
    for i in range(len(pieces)):
        if i + depth < len(pieces):
            if i + depth >= UBUF:
                give(i + depth - UBUF).wait()
            take(i + depth).start()
        take(i).wait()
        give(i).start()
        if i == depth:
            for n, (t, _, _, _, start, bound) in enumerate(shared):
                for c in pair(n):
                    c.wait()
                keep = spot(start, D, 1, LN, BLK) < bound
                left[n] = jnp.where(keep, left[n].astype(jnp.float32), right[n].astype(jnp.float32)).astype(jnp.bfloat16)
            for n, ((t, l), sides) in enumerate(cuts.items()):
                for c in cut_loads(n):
                    c.wait()
                rows = TENSORS[t][1]
                j, bound = sides[1][0], sides[1][3]
                if j < sides[0][1]:
                    keep = spot(STARTS[t] + (l * D + j * LN) * rows, 1, rows, SB, rows // SB) < bound
                    one = right[len(shared) + n, pl.ds(0, rows // SB)].astype(jnp.float32)
                    here = pl.ds(0, rows // SB)
                    layers[n][here, j] = jnp.where(keep, layers[n][here, j].astype(jnp.float32), one).astype(jnp.bfloat16)
        if i == depth + 2:
            for n, (t, g, _, _, _, _) in enumerate(shared):
                pltpu.make_async_copy(left.at[n], outs[t].at[pl.ds(g * BLK, BLK)], pair_sem.at[n, 0]).start()
            for n in range(len(cuts)):
                for c in cut_stores(n):
                    c.start()
    for i in range(max(0, len(pieces) - UBUF), len(pieces)):
        give(i).wait()
    for n, (t, g, _, _, _, _) in enumerate(shared):
        pltpu.make_async_copy(left.at[n], outs[t].at[pl.ds(g * BLK, BLK)], pair_sem.at[n, 0]).wait()
    for n in range(len(cuts)):
        for c in cut_stores(n):
            c.wait()


def unpack(gathered, shapes):
    pieces, shared, cuts = unpack_plan()
    anywhere = pl.BlockSpec(memory_space=pltpu.HBM)
    tiles = pl.pallas_call(
        unpack_kernel,
        name="unpack",
        out_shape=[jax.ShapeDtypeStruct((size // 1024, SB, LN), jnp.bfloat16) for size in SIZES],
        in_specs=[anywhere], out_specs=[anywhere] * len(TENSORS),
        scratch_shapes=[
            pltpu.VMEM((UBUF, UN, SB, LN), jnp.bfloat16), pltpu.VMEM((len(shared) + 1, BLK, SB, LN), jnp.bfloat16),
            pltpu.VMEM((len(shared) + len(cuts) + 1, BLK, SB, LN), jnp.bfloat16),
            *[pltpu.VMEM((TENSORS[t][1] // SB + 1, BLK, SB, LN), jnp.bfloat16) for t, _ in cuts],
            pltpu.SemaphoreType.DMA((UBUF,)), pltpu.SemaphoreType.DMA((UBUF,)),
            pltpu.SemaphoreType.DMA((len(shared), 2)), pltpu.SemaphoreType.DMA((len(cuts), BLK + 1))],
        compiler_params=pltpu.CompilerParams(vmem_limit_bytes=48 << 20),
    )(gathered.reshape(DEV * NT, SB, LN))
    outs = [from_tiles(t, x.reshape(TENSORS[t][2], TENSORS[t][1] // SB, BLK, SB, LN), shapes[t])
            for t, x in enumerate(tiles)]
    plist, _ = PIECES[DEV - 1]
    base = ((DEV - 1) * NT + plist[-1][4]) * SB
    tail = gathered[base:base + TAIL // LN].reshape(-1)
    cut = math.prod(shapes[SB])
    return outs + [tail[:cut].reshape(shapes[SB]), tail[cut:].reshape(shapes[9])]


def turn_kernel(*refs):
    count = len(CUT)
    srcs, outs, bufs, sems, done = refs[:count], refs[count:2 * count], refs[2 * count:3 * count], *refs[3 * count:]

    def take(n, c):
        t, l = CUT[n]
        c8 = TENSORS[t][1] // SB
        return pltpu.make_async_copy(srcs[n].at[pl.ds((l * c8 + c) * BLK, BLK)], bufs[n].at[:, c], sems.at[n, c])

    def give(n):
        return pltpu.make_async_copy(bufs[n], outs[n], done.at[n])

    every = [(n, c) for n, (t, _) in enumerate(CUT) for c in range(TENSORS[t][1] // SB)]
    for n, c in every:
        take(n, c).start()
    for n, c in every:
        take(n, c).wait()
        if (n, c + 1) not in every:
            give(n).start()
    for n in range(count):
        give(n).wait()


def turn(views):
    shapes = [(BLK, TENSORS[t][1] // SB, SB, LN) for t, _ in CUT]
    anywhere = pl.BlockSpec(memory_space=pltpu.HBM)
    return pl.pallas_call(
        turn_kernel,
        name="turn",
        out_shape=[jax.ShapeDtypeStruct(x, jnp.bfloat16) for x in shapes],
        in_specs=[anywhere] * len(CUT), out_specs=[anywhere] * len(CUT),
        scratch_shapes=[pltpu.VMEM(x, jnp.bfloat16) for x in shapes]
        + [pltpu.SemaphoreType.DMA((len(CUT), BLK)), pltpu.SemaphoreType.DMA((len(CUT),))],
    )(*[views[t].reshape(-1, SB, LN) for t, _ in CUT])


def sources(grads):
    views = [as_tiles(t, grads[t][0]) for t in range(len(TENSORS))]
    tail = jnp.concatenate([grads[SB].reshape(-1), grads[9].reshape(-1), jnp.zeros((-TAIL % 2048,), jnp.bfloat16)])
    return [x.reshape(-1, LN) for x in [*views, tail, *turn(views)]]


def solution(mesh):
    def local_update(*arrays):
        grads = arrays[:10]
        m, v, p, hyper = arrays[10:]
        shapes = [x.shape[1:] for x in grads]
        share, squares, _ = reduce_scatter(sources(grads))
        m, v, p, gathered = step_and_gather(hyper, share, squares, *[x.reshape(SROWS, LN) for x in (m, v, p)])
        params = unpack(gathered.reshape(DEV * NR, LN), shapes)
        return tuple(params) + tuple(x.reshape(SHARE) for x in (m, v, p))

    in_specs = tuple([P("dp")] * 10 + [P("dp"), P("dp"), P("dp"), P()])
    out_specs = tuple([P()] * 10 + [P("dp"), P("dp"), P("dp")])
    return jax.shard_map(local_update, mesh=mesh, in_specs=in_specs, out_specs=out_specs, check_vma=False)
```

```python
import functools
import math

import jax
import jax.numpy as jnp
import numpy as np
from jax import lax
from jax.experimental import pallas as pl
from jax.experimental.pallas import tpu as pltpu
from jax.sharding import PartitionSpec as P

ADAM_STEP = 7
LN = 128
SB = 8
ADAM_EPS = 1e-8
CLIP_EPS = 1e-6
D = 3840
BLK = D // LN
LAYERS = 6
DEV = 8
TENSORS = (("R", 4096, 1), ("C", 64, LAYERS), ("C", 32, LAYERS), ("C", 32, LAYERS), ("R", 64 * LAYERS, 1),
           ("C", 240, LAYERS), ("C", 240, LAYERS), ("R", 240 * LAYERS, 1))
SIZES = tuple(rows * layers * D for _, rows, layers in TENSORS)
STARTS = tuple(sum(SIZES[:i]) for i in range(len(SIZES)))
DECAY = sum(SIZES)
TAIL = LAYERS * 4 * D + LAYERS * 2 * 256
TOTAL = DECAY + TAIL
SHARE = TOTAL // DEV
SROWS = SHARE // LN
NT = 4536
NR = NT * SB
GUARD = 240
NCH = 9
CR = NR // 2 // NCH
MESH = pl.DeviceIdType.MESH


def plan():
    pieces, units = [], []
    for r in range(DEV):
        lo, hi = r * SHARE, (r + 1) * SHARE
        off, plist, ulist = 0, [], []
        for t, (kind, rows, layers) in enumerate(TENSORS):
            if kind == "R":
                a, b = max(lo, STARTS[t]), min(hi, STARTS[t] + SIZES[t])
                if a >= b:
                    continue
                g0, g1 = (a - STARTS[t]) // (SB * D), -((STARTS[t] - b) // (SB * D))
                plist.append((t, 0, g0, g1, off))
                for g in range(g0, g1):
                    ulist.append(("R", off + (g - g0) * BLK, 1, (STARTS[t] + g * SB * D - lo) // LN))
                off += (g1 - g0) * BLK
                continue
            for l in range(layers):
                s = STARTS[t] + l * rows * D
                a, b = max(lo, s), min(hi, s + rows * D)
                if a >= b:
                    continue
                j0, j1 = (a - s) // (LN * rows), -((s - b) // (LN * rows))
                plist.append((t, l, j0, j1, off))
                whole = j1 - j0 == BLK
                for j in range(j0, j1):
                    at, stride = (j, BLK) if whole else ((j - j0) * (rows // SB), 1)
                    ulist.append((rows, off + at, stride, (s + j * LN * rows - lo) // LN))
                off += (j1 - j0) * rows // SB
        if hi > DECAY:
            for i in range(TAIL // 1024):
                ulist.append(("T", off + i, 1, (DECAY - lo) // LN + SB * i))
            plist.append((len(TENSORS), 0, 0, TAIL // 1024, off))
            off += TAIL // 1024
        assert off <= NT
        pieces.append((plist, off))
        units.append(ulist)
    return pieces, units


PIECES, UNITS = plan()


def flip(dev, bit):
    return dev + bit - 2 * bit * (lax.rem(lax.div(dev, bit), 2))


def barrier_all(me):
    sem = pltpu.get_barrier_semaphore()
    for step in range(1, DEV):
        pl.semaphore_signal(sem, inc=1, device_id=(lax.rem(me + step, DEV),), device_id_type=MESH)
    pl.semaphore_wait(sem, DEV - 1)


def cut_layers():
    return sorted({(t, l) for plist, _ in PIECES for t, l, a, b, _ in plist
                   if t < len(TENSORS) and TENSORS[t][0] == "C" and b - a < BLK})


CUT = cut_layers()


def segments():
    found = []
    for plist, used in PIECES:
        runs = []
        for t, l, first, last, off in plist:
            if t == len(TENSORS):
                src, row, rows = t, 0, -(-last // 2) * 16
            elif TENSORS[t][0] == "R":
                src, row, rows = t, first * BLK * SB, (last - first) * BLK * SB
            elif (t, l) in CUT:
                c = TENSORS[t][1]
                src, row, rows = len(TENSORS) + 1 + CUT.index((t, l)), first * c, (last - first) * c
            else:
                src, row, rows = t, l * BLK * TENSORS[t][1], BLK * TENSORS[t][1]
            if runs and runs[-1][0] == src and runs[-1][1] + runs[-1][3] == row:
                runs[-1][3] += rows
            else:
                runs.append([src, row, off * SB, rows])
        end = runs[-1][2] + runs[-1][3]
        if end < NR:
            runs.append([0, 0, end, NR - end])
        halves = ([], [])
        for src, row, dst, rows in runs:
            while rows > 0:
                n = min(rows, CR - dst % CR)
                d, k = divmod(dst // CR, NCH)
                last = halves[d][-1] if halves[d] else None
                if last and n == CR and last[0] == src and last[4] == CR and last[1] + last[5] * CR == row:
                    last[5] += 1
                else:
                    halves[d].append([src, row, k, dst - d * (NR // 2), n, 1])
                row, dst, rows = row + n, dst + n, rows - n
        found.append(halves)
    return found


def rs_kernel(*refs):
    count = len(TENSORS) + 1 + len(CUT)
    srcs, (g_ref, sq_ref, r_ref, part, land, loads, outs, accum, sq_all,
           send1, recv1, send2, recv2, load_sem, out_sem, sq_send, sq_recv) = refs[:count], refs[count:]
    me = lax.axis_index("dp")
    barrier_all(me)
    half = NR // 2
    segs = segments()

    def bits(d):
        return 2 + 2 * d, 4 - 2 * d

    def landing(d, q, slot, row, rows):
        return r_ref.at[pl.ds(pl.multiple_of(((d * 2 + q) * 3 + slot) * half + row, 16), rows)]

    def hop(d, q, slot, k):
        here = landing(d, q, slot, k * CR, CR)
        return pltpu.make_async_remote_copy(
            src_ref=here, dst_ref=here, send_sem=send1.at[d, q, slot, k], recv_sem=recv1.at[d, q, slot, k],
            device_id=(flip(me, 1),), device_id_type=MESH)

    def pass_on(d, k):
        rows = pl.ds(pl.multiple_of(d * half + k * CR, 16), CR)
        return pltpu.make_async_remote_copy(
            src_ref=part.at[rows], dst_ref=land.at[rows], send_sem=send2.at[d, k], recv_sem=recv2.at[d, k],
            device_id=(flip(me, bits(d)[1]),), device_id_type=MESH)

    @pl.loop(0, 12)
    def _(h):
        q, turn, d = lax.div(h, 6), lax.rem(lax.div(h, 2), 3), lax.rem(h, 2)
        slot = lax.rem(turn + 1, 3)
        first, second = bits(d)
        away = flip(me, first)
        target = jnp.where(slot == 0, flip(me, 1), jnp.where(slot == 1, away, flip(away, 1)))
        owner = jnp.where(q == 0, flip(target, second), target)
        for r in range(DEV):
            for dd in range(2):
                @pl.when((owner == r) & (d == dd))
                def _():
                    for src, row, k0, dst, rows, chunks in segs[r][dd]:
                        def send(i, carry, src=src, row=row, k0=k0, dst=dst, rows=rows):
                            pltpu.make_async_remote_copy(
                                src_ref=srcs[src].at[pl.ds(pl.multiple_of(row + i * CR, SB), rows)],
                                dst_ref=r_ref.at[pl.ds(pl.multiple_of(
                                    ((d * 2 + q) * 3 + slot) * half + dst + i * CR, SB), rows)],
                                send_sem=send1.at[d, q, slot, k0 + i], recv_sem=recv1.at[d, q, slot, k0 + i],
                                device_id=(target,), device_id_type=MESH).start()
                            return carry
                        if chunks == 1:
                            send(0, 0)
                        else:
                            lax.fori_loop(0, chunks, send, 0)

    def load(d, q, slot, k):
        return pltpu.make_async_copy(landing(d, q, slot % 3, k * CR, CR), loads.at[d, slot], load_sem.at[d, slot])

    def load_own(d, q, k):
        owner = flip(me, bits(d)[1]) if q == 0 else me
        for r in range(DEV):
            @pl.when(owner == r)
            def _(r=r):
                for src, row, k0, dst, rows, chunks in segs[r][d]:
                    inside = (k >= k0) & (k < k0 + chunks)
                    at = row if chunks == 1 else pl.multiple_of(row + jnp.where(inside, k - k0, 0) * CR, SB)

                    @pl.when(inside)
                    def _(src=src, at=at, dst=dst, rows=rows):
                        pltpu.make_async_copy(
                            srcs[src].at[pl.ds(at, rows)],
                            loads.at[d, 3, pl.ds(dst % CR, rows)], load_sem.at[d, 3]).start()

    def fetch(d, q, k):
        load_own(d, q, k)
        for slot in range(3):
            hop(d, q, slot, k).wait_recv()
            load(d, q, slot, k).start()

    def ready(d, q, k):
        for slot in range(4):
            load(d, q, slot, k).wait()

    def total(d, rows):
        acc = loads[d, 3, rows, :].astype(jnp.float32)
        for slot in range(3):
            acc = acc + loads[d, slot, rows, :].astype(jnp.float32)
        return acc

    STEP = 112
    accum[...] = jnp.zeros_like(accum)
    used = functools.reduce(lambda acc, r: jnp.where(me == r, PIECES[r][1], acc), range(DEV), 0)

    def out_copy(d, k):
        return pltpu.make_async_copy(
            outs.at[d], g_ref.at[pl.ds(pl.multiple_of(d * half + k * CR, 16), CR)], out_sem.at[d])

    for d in range(2):
        fetch(d, 0, jnp.int32(0))

    @pl.loop(0, NCH)
    def _(k):
        for d in range(2):
            ready(d, 0, k)

            @pl.loop(0, CR // STEP)
            def _(i):
                rows = pl.ds(pl.multiple_of(i * STEP, 16), STEP)
                part[pl.ds(pl.multiple_of(d * half + k * CR + i * STEP, SB), STEP), :] = total(d, rows)

            @pl.when(k + 1 < NCH)
            def _():
                fetch(d, 0, k + 1)

            pass_on(d, k).start()

    for d in range(2):
        fetch(d, 1, jnp.int32(0))

    @pl.loop(0, NCH)
    def _(k):
        for d in range(2):
            for q in range(2):
                for slot in range(3):
                    hop(d, q, slot, k).wait_send()
            ready(d, 1, k)
            pass_on(d, k).wait_recv()

            @pl.when(k > 0)
            def _():
                out_copy(d, k - 1).wait()

            @pl.loop(0, CR // STEP)
            def _(i):
                base = pl.multiple_of(d * half + k * CR + i * STEP, SB)
                rows = pl.ds(pl.multiple_of(i * STEP, 16), STEP)
                g = (total(d, rows) + land[pl.ds(base, STEP), :]) * (1.0 / DEV)
                outs[d, rows, :] = g
                tile = lax.div(base, SB) + lax.broadcasted_iota(jnp.int32, (STEP // SB, SB, LN), 0)
                g3 = g.reshape(STEP // SB, SB, LN)
                keep = counted(me, tile) & (tile < used)
                accum[...] += jnp.sum(jnp.where(keep, g3 * g3, 0.0), axis=0)

            @pl.when(k + 1 < NCH)
            def _():
                fetch(d, 1, k + 1)

            out_copy(d, k).start()

    sq_all[pl.ds(pl.multiple_of(me * SB, SB), SB), :] = accum[...]
    for d in range(2):
        out_copy(d, NCH - 1).wait()
    def tell(step):
        return pltpu.make_async_remote_copy(
            src_ref=accum, dst_ref=sq_all.at[pl.ds(pl.multiple_of(me * SB, SB), SB)],
            send_sem=sq_send.at[step], recv_sem=sq_recv.at[step],
            device_id=(lax.rem(me + step + 1, DEV),), device_id_type=MESH)

    for step in range(DEV - 1):
        tell(step).start()
    for d in range(2):
        pl.loop(0, NCH)(lambda k, d=d: pass_on(d, k).wait_send())
    for step in range(DEV - 1):
        tell(step).wait()
    whole = sq_all[pl.ds(0, SB), :]
    for i in range(1, DEV):
        whole = whole + sq_all[pl.ds(SB * i, SB), :]
    sq_ref[...] = jnp.broadcast_to(jnp.sum(whole, keepdims=True), (SB, LN))


def shared_first():
    found = []
    for r in range(1, DEV):
        kind, tile, stride, row = UNITS[r][0]
        if row >= 0:
            continue
        found.append((r, BLK if kind == "R" else kind // SB))
    return found


def counted(me, tile):
    first = functools.reduce(lambda acc, x: jnp.where(me == x[0], x[1], acc), shared_first(), 0)
    return tile >= first


def reduce_scatter(sources):
    half = NR // 2
    return pl.pallas_call(
        rs_kernel,
        name="reduce_scatter",
        out_shape=(jax.ShapeDtypeStruct((NR, LN), jnp.float32), jax.ShapeDtypeStruct((SB, LN), jnp.float32),
                   jax.ShapeDtypeStruct((12 * half, LN), jnp.bfloat16)),
        in_specs=[pl.BlockSpec(memory_space=pltpu.HBM)] * len(sources),
        out_specs=(pl.BlockSpec(memory_space=pltpu.HBM), pl.BlockSpec(memory_space=pltpu.VMEM),
                   pl.BlockSpec(memory_space=pltpu.HBM)),
        scratch_shapes=[
            pltpu.VMEM((NR, LN), jnp.float32), pltpu.VMEM((NR, LN), jnp.float32),
            pltpu.VMEM((2, 4, CR, LN), jnp.bfloat16), pltpu.VMEM((2, CR, LN), jnp.float32),
            pltpu.VMEM((SB, LN), jnp.float32), pltpu.VMEM((SB * DEV, LN), jnp.float32),
            pltpu.SemaphoreType.DMA((2, 2, 3, NCH)), pltpu.SemaphoreType.DMA((2, 2, 3, NCH)),
            pltpu.SemaphoreType.DMA((2, NCH)), pltpu.SemaphoreType.DMA((2, NCH)),
            pltpu.SemaphoreType.DMA((2, 4)), pltpu.SemaphoreType.DMA((2,)),
            pltpu.SemaphoreType.DMA((DEV - 1,)), pltpu.SemaphoreType.DMA((DEV - 1,))],
        compiler_params=pltpu.CompilerParams(collective_id=0, has_side_effects=True, vmem_limit_bytes=60 << 20),
    )(*sources)


BR = 1152
NB = -(-SROWS // BR)
STEP = 96
KINDS = {"R": 1, 240: 3, 64: SB, 32: 16, "T": 1}
ACH = 18
PIECES_OUT = 2 * ACH
PT = NT // PIECES_OUT


def unit_runs():
    runs = {kind: [] for kind in KINDS}
    need = np.full((PIECES_OUT, DEV), NB - 1)
    made = np.zeros((PIECES_OUT, DEV), int)
    for r, ulist in enumerate(UNITS):
        for kind in KINDS:
            mine = [u for u in ulist if u[0] == kind]
            size, count = UNIT_SIZE[kind]
            found = []
            for i, (_, tile, stride, row) in enumerate(mine):
                first = max(0, row // BR)
                last = min(NB - 1, (row + size - 1) // BR)
                for piece in {(tile + c * stride) // PT for c in range(count)}:
                    need[piece, r] = min(need[piece, r], first)
                    made[piece, r] = max(made[piece, r], last)
                per = 1 if stride == BLK else count
                if not found or stride != found[-1][-1] or row + GUARD != found[-1][2] + found[-1][0] * size:
                    found.append([0, tile, row + GUARD, BLK * count, per, stride])
                n, start, _, step, per, _ = found[-1]
                assert tile == start + n // BLK * step + n % BLK * per
                found[-1][0] += 1
            for slot, run in enumerate(found):
                if slot == len(runs[kind]):
                    runs[kind].append(np.zeros((6, DEV), int))
                runs[kind][slot][:, r] = run
    for i in range(PIECES_OUT):
        need[i] = need[i:].min(axis=0)
        made[i] = made[:i + 1].max(axis=0)
    return runs, need, made


UNIT_SIZE = {"R": (GUARD, BLK), 240: (240, BLK), 64: (64, SB), 32: (32, 4), "T": (SB, 1)}
RUNS, NEED, MADE = unit_runs()


def by_owner(me, values):
    out = int(values[0])
    for r in range(1, DEV):
        if int(values[r]) != int(values[r - 1]):
            out = jnp.where(me >= r, int(values[r]), out)
    return out


def lanes(rows):
    return lax.broadcasted_iota(jnp.int32, (rows, LN), 1)


def roll(x, shift):
    shift = shift % LN
    return x if shift == 0 else pltpu.roll(x, shift, 1)


def swap_blocks(xs, width):
    per = len(xs)
    lane = lanes(xs[0].shape[0])

    def pick(choose):
        out = choose(0)
        for b in range(1, per):
            out = jnp.where(lane >= b * width, choose(b), out)
        return out

    turned = [roll(pick(lambda b: xs[(b + t) % per]), t * width) for t in range(per)]
    return [pick(lambda b: turned[(b - j) % per]) for j in range(per)]


def to_flat(kind, units, tiles, flat, low, ta, tb):
    del low
    if kind == "T" or kind == "R":
        for base, _, row in units:
            if kind == "T":
                flat[pl.ds(row, SB), :] = tiles[base]
            else:
                for c in range(BLK):
                    flat[pl.ds(row + c, SB, stride=BLK), :] = tiles[base + c]
        return
    if kind < LN:
        per = LN // kind
        sets = [units[i:i + per] for i in range(0, len(units), per)]
        for n, some in enumerate(sets):
            ta[n] = jnp.concatenate([tiles[base + i * stride] for base, stride, _ in some for i in range(kind // SB)]).T
        for n, some in enumerate(sets):
            for unit, x in zip(some, swap_blocks([ta[n, pl.ds(q, kind, stride=per), :] for q in range(per)], kind)):
                flat[pl.ds(unit[-1], kind), :] = x
        return
    for n, (base, stride, row) in enumerate(units):
        ta[n] = jnp.concatenate([tiles[base + i * stride] for i in range(16)]).T
        tb[n] = jnp.concatenate([tiles[base + i * stride] for i in range(16, BLK)] + [jnp.zeros((16, LN))]).T
    lane = lanes(16)
    for k in range(15):
        r, o = divmod(LN * k, kind)
        for n, (_, _, row) in enumerate(units):
            x = (ta if o < LN else tb)[n, pl.ds(r, 16, stride=SB), :]
            if 0 < o < LN:
                x = jnp.where(lane >= o, x, tb[n, pl.ds(r, 16, stride=SB), :])
            x = roll(x, -o)
            if o + LN > kind:
                x = jnp.where(lane >= kind - o, roll(ta[n, pl.ds(r + 1, 16, stride=SB), :], kind - o), x)
            flat[pl.ds(row + k, 16, stride=15), :] = x


def to_tiles(kind, units, tiles, flat, low, ta, tb):
    del tiles

    def put(at, value):
        low[at] = value.astype(jnp.bfloat16)

    if kind == "T" or kind == "R":
        for base, _, row in units:
            if kind == "T":
                put(base, flat[pl.ds(row, SB), :])
            else:
                for c in range(BLK):
                    put(base + c, flat[pl.ds(row + c, SB, stride=BLK), :])
        return
    if kind < LN:
        per = LN // kind
        sets = [units[i:i + per] for i in range(0, len(units), per)]
        for n, some in enumerate(sets):
            for q, x in enumerate(swap_blocks([flat[pl.ds(row, kind), :] for _, _, row in some], kind)):
                ta[n, pl.ds(q, kind, stride=per), :] = x
        for n, some in enumerate(sets):
            grid = ta[n].T.reshape(16, SB, LN)
            for u, (base, stride, _) in enumerate(some):
                for i in range(kind // SB):
                    put(base + i * stride, grid[u * (kind // SB) + i])
        return
    lane = lanes(16)
    for r in range(SB):
        k, o = divmod(kind * r, LN)
        for n, (_, _, row) in enumerate(units):
            f = [flat[pl.ds(row + k + i, 16, stride=15), :] for i in range(3 if k + 2 < 15 else 2)]
            ta[n, pl.ds(r, 16, stride=SB), :] = f[0] if o == 0 else roll(jnp.where(lane >= o, f[0], f[1]), -o)
            tb[n, pl.ds(r, 16, stride=SB), :] = f[1] if o == 0 else roll(jnp.where(lane >= o, f[1], f[-1]), -o)
    for n, (base, stride, _) in enumerate(units):
        grid = jnp.concatenate([ta[n].T, tb[n].T]).reshape(32, SB, LN)
        for i in range(BLK):
            put(base + i * stride, grid[i])


def step_kernel(scal, g_ref, sq_ref, m_ref, v_ref, p_ref, m_out, v_out, p_out, a_ref,
                tiles, flat, ta, tb, low, g_sem, a_sem, send, recv):
    me = lax.axis_index("dp")
    b = pl.program_id(0)
    xn, yn, pn = flip(me, 2), flip(me, 4), flip(me, 1)
    diag = flip(xn, 4)

    def take(i):
        here = pl.ds(i * PT, PT)
        return pltpu.make_async_copy(g_ref.at[here], tiles.at[here], g_sem.at[i])

    def keep(i):
        return pltpu.make_async_copy(low.at[pl.ds(i * PT, PT)], a_ref.at[pl.ds(me * NT + i * PT, PT)], a_sem.at[i])

    def copy(kind, d, k):
        owner = (me, me, me, xn if d == 0 else yn, xn, yn, diag)[kind]
        target = (xn, yn, pn, yn if d == 0 else xn, pn, pn, pn)[kind]
        at = (2 * k + d) * PT
        there = a_ref.at[pl.ds(owner * NT + at, PT)]
        return pltpu.make_async_remote_copy(
            src_ref=low.at[pl.ds(at, PT)] if kind < 3 else there, dst_ref=there,
            send_sem=send.at[kind, d, k], recv_sem=recv.at[kind, d, k],
            device_id=(target,), device_id_type=MESH)

    def give(i):
        for kind in range(3):
            copy(kind, i % 2, i // 2).start()
        keep(i).start()

    for i in range(PIECES_OUT):
        pl.when(b == by_owner(me, np.maximum(NEED[i] - 3, 0)))(lambda i=i: take(i).start())
    pl.when(b == 0)(lambda: barrier_all(me))
    made = [by_owner(me, MADE[i]) for i in range(PIECES_OUT)]
    for i in range(PIECES_OUT):
        pl.when(b == made[i] + 1)(functools.partial(give, i))
    for i in range(PIECES_OUT):
        pl.when(b == by_owner(me, NEED[i]))(lambda i=i: take(i).wait())

    def upto(block, count, row, size, whole):
        room = (block + 1) * BR + GUARD - row
        n = lax.div(jnp.where(room > 0, room, 0) + (0 if whole else size - 1), size)
        return jnp.where(n < count, n, count)

    def each(whole, work):
        for kind, group in KINDS.items():
            size = UNIT_SIZE[kind][0]
            for run in RUNS[kind]:
                count, start, row, step, per, stride = [by_owner(me, x) for x in run]
                first = jnp.where(b > 0, upto(b - 1, count, row, size, whole), 0)
                last = upto(b, count, row, size, whole)
                if whole:
                    last = jnp.where(b < NB - 1, last, count)

                @pl.loop(0, lax.div(last - first + group - 1, group))
                def _(t):
                    units = []
                    for x in range(group):
                        i = first + t * group + x
                        i = jnp.where(i < last, i, last - 1)
                        units.append((start + lax.div(i, BLK) * step + lax.rem(i, BLK) * per, stride, row + i * size))
                    work(kind, units, tiles, flat, low, ta, tb)

    each(False, to_flat)

    learn_rate, b1, b2, decay, max_norm = [scal[i] for i in range(5)]
    c1, c2 = 1.0 - b1, 1.0 - b2

    def correction(beta):
        return 1.0 / (1.0 - jnp.full((1, LN), beta) ** ADAM_STEP)

    i1, i2 = correction(b1), correction(b2)
    clip = jnp.minimum(1.0, max_norm / (jnp.sqrt(sq_ref[...]) + CLIP_EPS))[:1]

    @pl.loop(0, BR // STEP)
    def _(i):
        rows = pl.ds(pl.multiple_of(i * STEP, SB), STEP)
        local = b * BR + i * STEP
        here = pl.ds(pl.multiple_of(GUARD + local, SB), STEP)
        h = flat[here, :] * clip
        m = b1 * m_ref[rows, :] + c1 * h
        v = b2 * v_ref[rows, :] + c2 * (h * h)
        p = p_ref[rows, :]
        m_out[rows, :] = m
        v_out[rows, :] = v
        where = me * SROWS + local + lax.broadcasted_iota(jnp.int32, (STEP, LN), 0)
        step = (m * i1) / (jnp.sqrt(v * i2) + ADAM_EPS) + jnp.where(where < DECAY // LN, decay * p, 0.0)
        p = p - learn_rate * step
        p_out[rows, :] = p
        flat[here, :] = p

    each(True, to_tiles)

    @pl.when(b == NB - 1)
    def _():
        for i in range(PIECES_OUT):
            pl.when(made[i] == NB - 1)(functools.partial(give, i))

        @pl.loop(0, ACH)
        def _(k):
            copy(0, 0, k).wait_recv()
            copy(3, 0, k).start()
            copy(4, 0, k).start()
            copy(1, 1, k).wait_recv()
            copy(3, 1, k).start()
            copy(5, 1, k).start()
            copy(0, 1, k).wait_recv()
            copy(4, 1, k).start()
            copy(1, 0, k).wait_recv()
            copy(5, 0, k).start()

        def finish(k):
            for d in range(2):
                copy(6, d, k).wait_recv()
                copy(3, d, k).wait_send()
                copy(6, d, k).wait_send()

        @pl.loop(0, ACH)
        def _(k):
            for d in range(2):
                copy(3, d, k).wait_recv()
                copy(6, d, k).start()
            for d in range(2):
                for kind in (2, 4, 5):
                    copy(kind, d, k).wait_recv()
                for kind in (0, 1, 2, 4, 5):
                    copy(kind, d, k).wait_send()
                keep(2 * k + d).wait()
            pl.when(k > 1)(lambda: finish(jnp.where(k > 1, k - 2, 0)))

        pl.loop(ACH - 2, ACH)(finish)


def step_and_gather(scal, g, sq, m, v, p):
    block = pl.BlockSpec((BR, LN), lambda b, *_: (b, 0))
    anywhere = pl.BlockSpec(memory_space=pltpu.HBM)
    flat_shape = jax.ShapeDtypeStruct((SROWS, LN), jnp.float32)
    turn = pltpu.VMEM((4, LN, LN), jnp.float32)
    dma = pltpu.SemaphoreType.DMA
    return pl.pallas_call(
        step_kernel,
        name="step_and_gather",
        grid_spec=pltpu.PrefetchScalarGridSpec(
            num_scalar_prefetch=1, grid=(NB,),
            in_specs=[anywhere, pl.BlockSpec((SB, LN), lambda b, *_: (0, 0)), block, block, block],
            out_specs=[block, block, block, anywhere],
            scratch_shapes=[
                pltpu.VMEM((NT, SB, LN), jnp.float32), pltpu.VMEM((NB * BR + 2 * GUARD + SB, LN), jnp.float32),
                turn, turn, pltpu.VMEM((NT, SB, LN), jnp.bfloat16),
                dma((PIECES_OUT,)), dma((PIECES_OUT,)), dma((7, 2, ACH)), dma((7, 2, ACH))]),
        out_shape=[flat_shape, flat_shape, flat_shape, jax.ShapeDtypeStruct((DEV * NT, SB, LN), jnp.bfloat16)],
        compiler_params=pltpu.CompilerParams(
            dimension_semantics=("arbitrary",), vmem_limit_bytes=63 << 20, collective_id=1, has_side_effects=True),
    )(scal, g.reshape(NT, SB, LN), sq, m, v, p)


def as_tiles(t, x):
    kind, rows, layers = TENSORS[t]
    if kind == "C":
        x = jnp.swapaxes(x, -1, -2)
    return x.reshape(layers, rows // SB, SB, BLK, LN).transpose(0, 1, 3, 2, 4)


def from_tiles(t, x, shape):
    kind, rows, layers = TENSORS[t]
    x = x.transpose(0, 1, 3, 2, 4)
    if kind == "C":
        return jnp.swapaxes(x.reshape(layers, rows, D), -1, -2)
    return x.reshape(shape)


def unpack_plan():
    copies, shared, cuts = [], [], {}
    for t, (kind, rows, layers) in enumerate(TENSORS):
        last_seen = None
        for r, (plist, _) in enumerate(PIECES):
            for pt, l, first, last, off in plist:
                if pt != t:
                    continue
                src = r * NT + off
                if (t, l) in CUT:
                    cuts.setdefault((t, l), []).append((first, last, src, r * SHARE))
                    continue
                if kind == "C":
                    copies.append([src, t, l * BLK * rows // SB, BLK * rows // SB])
                    continue
                begin = first
                if last_seen and first < last_seen[0]:
                    copies[-1][3] -= BLK
                    shared.append((t, first, last_seen[1] - BLK, src, STARTS[t] + first * SB * D, r * SHARE))
                    begin = first + 1
                copies.append([src + (begin - first) * BLK, t, begin * BLK, (last - begin) * BLK])
                last_seen = (last, src + (last - first) * BLK)
    pieces = []
    for src, t, dst, tiles in copies:
        while tiles > 0:
            n = min(tiles, UN)
            pieces.append((src, t, dst, n))
            src, dst, tiles = src + n, dst + n, tiles - n
    return pieces, shared, cuts


UN = 480
UBUF = 12


def unpack_kernel(src_ref, *refs):
    outs = refs[:len(TENSORS)]
    ring, left, right, *layers, in_sem, out_sem, pair_sem, cut_sem = refs[len(TENSORS):]
    pieces, shared, cuts = unpack_plan()

    def take(i):
        src, _, _, n = pieces[i]
        return pltpu.make_async_copy(src_ref.at[pl.ds(src, n)], ring.at[i % UBUF, pl.ds(0, n)], in_sem.at[i % UBUF])

    def give(i):
        _, t, dst, n = pieces[i]
        return pltpu.make_async_copy(ring.at[i % UBUF, pl.ds(0, n)], outs[t].at[pl.ds(dst, n)], out_sem.at[i % UBUF])

    def pair(n):
        _, _, a, b, _, _ = shared[n]
        return (pltpu.make_async_copy(src_ref.at[pl.ds(a, BLK)], left.at[n], pair_sem.at[n, 0]),
                pltpu.make_async_copy(src_ref.at[pl.ds(b, BLK)], right.at[n], pair_sem.at[n, 1]))

    def cut_loads(n):
        (t, _), sides = list(cuts.items())[n]
        c8 = TENSORS[t][1] // SB
        made = []
        for side, (first, last, src, _) in enumerate(sides):
            for j in range(first, last):
                over = side == 1 and first < sides[0][1] and j == first
                to = right.at[len(shared) + n, pl.ds(0, c8)] if over else layers[n].at[pl.ds(0, c8), j]
                made.append(pltpu.make_async_copy(
                    src_ref.at[pl.ds(src + (j - first) * c8, c8)], to, cut_sem.at[n, BLK if over else j]))
        return made

    def cut_stores(n):
        (t, l), _ = list(cuts.items())[n]
        c8 = TENSORS[t][1] // SB
        return [pltpu.make_async_copy(layers[n].at[c], outs[t].at[pl.ds((l * c8 + c) * BLK, BLK)], cut_sem.at[n, c])
                for c in range(c8)]

    def spot(start, row_step, lane_step, tile_step, tiles):
        shape = (tiles, SB, LN)
        return (start + tile_step * lax.broadcasted_iota(jnp.int32, shape, 0)
                + row_step * lax.broadcasted_iota(jnp.int32, shape, 1)
                + lane_step * lax.broadcasted_iota(jnp.int32, shape, 2))

    for n in range(len(shared)):
        for c in pair(n):
            c.start()
    for n in range(len(cuts)):
        for c in cut_loads(n):
            c.start()
    depth = UBUF // 2
    for i in range(depth):
        take(i).start()
    for i in range(len(pieces)):
        if i + depth < len(pieces):
            if i + depth >= UBUF:
                give(i + depth - UBUF).wait()
            take(i + depth).start()
        take(i).wait()
        give(i).start()
        if i == depth:
            for n, (t, _, _, _, start, bound) in enumerate(shared):
                for c in pair(n):
                    c.wait()
                keep = spot(start, D, 1, LN, BLK) < bound
                left[n] = jnp.where(keep, left[n].astype(jnp.float32), right[n].astype(jnp.float32)).astype(jnp.bfloat16)
            for n, ((t, l), sides) in enumerate(cuts.items()):
                for c in cut_loads(n):
                    c.wait()
                rows = TENSORS[t][1]
                j, bound = sides[1][0], sides[1][3]
                if j < sides[0][1]:
                    keep = spot(STARTS[t] + (l * D + j * LN) * rows, 1, rows, SB, rows // SB) < bound
                    one = right[len(shared) + n, pl.ds(0, rows // SB)].astype(jnp.float32)
                    here = pl.ds(0, rows // SB)
                    layers[n][here, j] = jnp.where(keep, layers[n][here, j].astype(jnp.float32), one).astype(jnp.bfloat16)
        if i == depth + 2:
            for n, (t, g, _, _, _, _) in enumerate(shared):
                pltpu.make_async_copy(left.at[n], outs[t].at[pl.ds(g * BLK, BLK)], pair_sem.at[n, 0]).start()
            for n in range(len(cuts)):
                for c in cut_stores(n):
                    c.start()
    for i in range(max(0, len(pieces) - UBUF), len(pieces)):
        give(i).wait()
    for n, (t, g, _, _, _, _) in enumerate(shared):
        pltpu.make_async_copy(left.at[n], outs[t].at[pl.ds(g * BLK, BLK)], pair_sem.at[n, 0]).wait()
    for n in range(len(cuts)):
        for c in cut_stores(n):
            c.wait()


def unpack(gathered, shapes):
    pieces, shared, cuts = unpack_plan()
    anywhere = pl.BlockSpec(memory_space=pltpu.HBM)
    tiles = pl.pallas_call(
        unpack_kernel,
        name="unpack",
        out_shape=[jax.ShapeDtypeStruct((size // 1024, SB, LN), jnp.bfloat16) for size in SIZES],
        in_specs=[anywhere], out_specs=[anywhere] * len(TENSORS),
        scratch_shapes=[
            pltpu.VMEM((UBUF, UN, SB, LN), jnp.bfloat16), pltpu.VMEM((len(shared) + 1, BLK, SB, LN), jnp.bfloat16),
            pltpu.VMEM((len(shared) + len(cuts) + 1, BLK, SB, LN), jnp.bfloat16),
            *[pltpu.VMEM((TENSORS[t][1] // SB + 1, BLK, SB, LN), jnp.bfloat16) for t, _ in cuts],
            pltpu.SemaphoreType.DMA((UBUF,)), pltpu.SemaphoreType.DMA((UBUF,)),
            pltpu.SemaphoreType.DMA((len(shared), 2)), pltpu.SemaphoreType.DMA((len(cuts), BLK + 1))],
        compiler_params=pltpu.CompilerParams(vmem_limit_bytes=48 << 20),
    )(gathered.reshape(DEV * NT, SB, LN))
    outs = [from_tiles(t, x.reshape(TENSORS[t][2], TENSORS[t][1] // SB, BLK, SB, LN), shapes[t])
            for t, x in enumerate(tiles)]
    plist, _ = PIECES[DEV - 1]
    base = ((DEV - 1) * NT + plist[-1][4]) * SB
    tail = gathered[base:base + TAIL // LN].reshape(-1)
    cut = math.prod(shapes[SB])
    return outs + [tail[:cut].reshape(shapes[SB]), tail[cut:].reshape(shapes[9])]


def turn_kernel(*refs):
    count = len(CUT)
    srcs, outs, bufs, sems, done = refs[:count], refs[count:2 * count], refs[2 * count:3 * count], *refs[3 * count:]

    def take(n, c):
        t, l = CUT[n]
        c8 = TENSORS[t][1] // SB
        return pltpu.make_async_copy(srcs[n].at[pl.ds((l * c8 + c) * BLK, BLK)], bufs[n].at[:, c], sems.at[n, c])

    def give(n):
        return pltpu.make_async_copy(bufs[n], outs[n], done.at[n])

    every = [(n, c) for n, (t, _) in enumerate(CUT) for c in range(TENSORS[t][1] // SB)]
    for n, c in every:
        take(n, c).start()
    for n, c in every:
        take(n, c).wait()
        if (n, c + 1) not in every:
            give(n).start()
    for n in range(count):
        give(n).wait()


def turn(views):
    shapes = [(BLK, TENSORS[t][1] // SB, SB, LN) for t, _ in CUT]
    anywhere = pl.BlockSpec(memory_space=pltpu.HBM)
    return pl.pallas_call(
        turn_kernel,
        name="turn",
        out_shape=[jax.ShapeDtypeStruct(x, jnp.bfloat16) for x in shapes],
        in_specs=[anywhere] * len(CUT), out_specs=[anywhere] * len(CUT),
        scratch_shapes=[pltpu.VMEM(x, jnp.bfloat16) for x in shapes]
        + [pltpu.SemaphoreType.DMA((len(CUT), BLK)), pltpu.SemaphoreType.DMA((len(CUT),))],
    )(*[views[t].reshape(-1, SB, LN) for t, _ in CUT])


def sources(grads):
    views = [as_tiles(t, grads[t][0]) for t in range(len(TENSORS))]
    tail = jnp.concatenate([grads[SB].reshape(-1), grads[9].reshape(-1), jnp.zeros((-TAIL % 2048,), jnp.bfloat16)])
    return [x.reshape(-1, LN) for x in [*views, tail, *turn(views)]]


def solution(mesh):
    def local_update(*arrays):
        grads = arrays[:10]
        m, v, p, hyper = arrays[10:]
        shapes = [x.shape[1:] for x in grads]
        share, squares, _ = reduce_scatter(sources(grads))
        m, v, p, gathered = step_and_gather(hyper, share, squares, *[x.reshape(SROWS, LN) for x in (m, v, p)])
        params = unpack(gathered.reshape(DEV * NR, LN), shapes)
        return tuple(params) + tuple(x.reshape(SHARE) for x in (m, v, p))

    in_specs = tuple([P("dp")] * 10 + [P("dp"), P("dp"), P("dp"), P()])
    out_specs = tuple([P()] * 10 + [P("dp"), P("dp"), P("dp")])
    return jax.shard_map(local_update, mesh=mesh, in_specs=in_specs, out_specs=out_specs, check_vma=False)
```
